8 devices in a mesh: dp: 1 (over z), ty: 2 (over y), tx: 4 (over x, core).
Axes of the slice: x: 2, y: 2, z: 1, core: 2. Of those that a mesh axis runs over, the one named last changes fastest.
Arguments:
- x_in: bfloat16 [128, 4096], P('dp', 'tx')
- seq_lens: int32 [128], P('dp')
- k_cache: bfloat16 [128, 4096, 128], P(('dp', 'ty', 'tx'))
- v_cache: bfloat16 [128, 4096, 128], P(('dp', 'ty', 'tx'))
- ln_gamma: float32 [4096], P('tx')
- w_query: bfloat16 [4096, 4096], P('tx', 'ty')
- w_key: bfloat16 [4096, 128], P('tx')
- w_value: bfloat16 [4096, 128], P('tx')
- w_gate: bfloat16 [4096, 16384], P('tx', 'ty')
- w_up: bfloat16 [4096, 16384], P('tx', 'ty')
- w_out: bfloat16 [4096, 4096], P('ty', 'tx')
- w_down: bfloat16 [16384, 4096], P('ty', 'tx')
Outputs:
- output 1: bfloat16 [128, 4096], P('dp', 'tx')
- output 2: bfloat16 [128, 4096, 128], P(('dp', 'ty', 'tx'))
- output 3: bfloat16 [128, 4096, 128], P(('dp', 'ty', 'tx'))
All inputs are finite; a program needn't handle non-finite values.
Results may differ from the reference program's by a relative error of at most 0.0135093.
Values are sent between devices in bfloat16 or wider.
A program may use at most 1 GiB of HBM per device.

```python
import jax
import jax.numpy as jnp
from jax import lax

D_MODEL = 4096
NUM_HEADS = 32
HEAD_DIM = 128
FFN_DIM = 16384
BATCH = 128
SEQ_BLOCK = 16
CTX_LEN = 4096

EPSILON = 1e-6
ROPE_BASE = 10000.0


def setup_inputs(seed: int = 0, part: int = 0) -> dict:
    part_keys = jax.random.split(jax.random.fold_in(jax.random.key(seed), part), 6)
    shared_keys = jax.random.split(jax.random.key(seed + 1), 8)
    x_in = jax.random.normal(part_keys[0], (BATCH, D_MODEL), jnp.float32).astype(jnp.bfloat16)
    block_caps = jax.random.randint(part_keys[1], (BATCH // SEQ_BLOCK,), 1, CTX_LEN + 1)
    raw_lens = jax.random.randint(part_keys[2], (BATCH,), 0, jnp.repeat(block_caps, SEQ_BLOCK))
    pick_order = jax.random.permutation(part_keys[3], BATCH)
    seq_lens = raw_lens.at[pick_order[0]].set(CTX_LEN - 1).at[pick_order[1]].set(0).astype(jnp.int32)
    k_cache = jax.random.normal(part_keys[4], (BATCH, CTX_LEN, HEAD_DIM), jnp.float32).astype(jnp.bfloat16)
    v_cache = jax.random.normal(part_keys[5], (BATCH, CTX_LEN, HEAD_DIM), jnp.float32).astype(jnp.bfloat16)
    ln_gamma = 1.0 + 0.4 * jax.random.normal(shared_keys[0], (D_MODEL,), jnp.float32)
    w_query = (jax.random.normal(shared_keys[1], (D_MODEL, NUM_HEADS * HEAD_DIM), jnp.float32) * (2.0 * D_MODEL ** -0.5)).astype(jnp.bfloat16)
    w_key = (jax.random.normal(shared_keys[2], (D_MODEL, HEAD_DIM), jnp.float32) * D_MODEL ** -0.5).astype(jnp.bfloat16)
    w_value = (jax.random.normal(shared_keys[3], (D_MODEL, HEAD_DIM), jnp.float32) * D_MODEL ** -0.5).astype(jnp.bfloat16)
    w_gate = (jax.random.normal(shared_keys[4], (D_MODEL, FFN_DIM), jnp.float32) * D_MODEL ** -0.5).astype(jnp.bfloat16)
    w_up = (jax.random.normal(shared_keys[5], (D_MODEL, FFN_DIM), jnp.float32) * D_MODEL ** -0.5).astype(jnp.bfloat16)
    w_out = (jax.random.normal(shared_keys[6], (NUM_HEADS * HEAD_DIM, D_MODEL), jnp.float32) * (NUM_HEADS * HEAD_DIM) ** -0.5).astype(jnp.bfloat16)
    w_down = (jax.random.normal(shared_keys[7], (FFN_DIM, D_MODEL), jnp.float32) * FFN_DIM ** -0.5).astype(jnp.bfloat16)
    return {"x_in": x_in, "seq_lens": seq_lens, "k_cache": k_cache, "v_cache": v_cache, "ln_gamma": ln_gamma, "w_query": w_query, "w_key": w_key, "w_value": w_value, "w_gate": w_gate, "w_up": w_up, "w_out": w_out, "w_down": w_down}


def rope_tables(positions, head_dim):
    half_dim = head_dim // 2
    inv_freqs = ROPE_BASE ** (-(jnp.arange(half_dim, dtype=jnp.float32) * 2.0) / head_dim)
    angles = positions.astype(jnp.float32)[:, None] * inv_freqs[None, :]
    return jnp.cos(angles), jnp.sin(angles)


def rope_apply(vals, cosines, sines):
    half_dim = vals.shape[-1] // 2
    first = vals[..., :half_dim]
    second = vals[..., half_dim:]
    return jnp.concatenate([first * cosines - second * sines, second * cosines + first * sines], axis=-1)


def reference(x_in, seq_lens, k_cache, v_cache, ln_gamma, w_query, w_key, w_value, w_gate, w_up, w_out, w_down):
    x_f32 = x_in.astype(jnp.float32)
    row_mean = jnp.sum(x_f32, axis=-1) / D_MODEL
    row_var = jnp.sum(x_f32 * x_f32, axis=-1) / D_MODEL - row_mean * row_mean
    normed = ((x_f32 - row_mean[:, None]) * lax.rsqrt(row_var[:, None] + EPSILON) * ln_gamma[None, :]).astype(jnp.bfloat16)
    q_proj = jnp.dot(normed, w_query, preferred_element_type=jnp.float32).reshape(BATCH, NUM_HEADS, HEAD_DIM)
    k_proj = jnp.dot(normed, w_key, preferred_element_type=jnp.float32)
    v_new = jnp.dot(normed, w_value, preferred_element_type=jnp.float32).astype(jnp.bfloat16)
    gate = jnp.dot(normed, w_gate, preferred_element_type=jnp.float32).astype(jnp.bfloat16)
    up_proj = jnp.dot(normed, w_up, preferred_element_type=jnp.float32).astype(jnp.bfloat16)
    cosines, sines = rope_tables(seq_lens, HEAD_DIM)
    queries = rope_apply(q_proj, cosines[:, None, :], sines[:, None, :]).astype(jnp.bfloat16)
    k_new = rope_apply(k_proj, cosines, sines).astype(jnp.bfloat16)
    positions = jnp.arange(CTX_LEN)
    at_slot = positions[None, :, None] == seq_lens[:, None, None]
    k_out = jnp.where(at_slot, k_new[:, None, :], k_cache)
    v_out = jnp.where(at_slot, v_new[:, None, :], v_cache)

    def one_sequence(item):
        q_row, k_rows, v_rows, length = item
        scores = jnp.dot(q_row, k_rows.T, preferred_element_type=jnp.float32) * (HEAD_DIM ** -0.5)
        in_range = positions[None, :] <= length
        scores = jnp.where(in_range, scores, -1e30)
        att_probs = jax.nn.softmax(scores, axis=-1).astype(jnp.bfloat16)
        return jnp.dot(att_probs, v_rows, preferred_element_type=jnp.float32).astype(jnp.bfloat16)

    att_heads = lax.map(one_sequence, (queries, k_out, v_out, seq_lens))
    mlp_act = (jax.nn.silu(gate.astype(jnp.float32)) * up_proj.astype(jnp.float32)).astype(jnp.bfloat16)
    attn_part = jnp.dot(att_heads.reshape(BATCH, NUM_HEADS * HEAD_DIM), w_out, preferred_element_type=jnp.float32)
    mlp_part = jnp.dot(mlp_act, w_down, preferred_element_type=jnp.float32)
    y_out = (x_f32 + attn_part + mlp_part).astype(jnp.bfloat16)
    return (y_out, k_out, v_out)
```

```python
import functools

import jax
import jax.numpy as jnp
from jax import lax
from jax.experimental import pallas as pl
from jax.experimental.pallas import tpu as pltpu
from jax.sharding import PartitionSpec as P

EPSILON = 1e-6
ROPE_BASE = 10000.0
BF16 = jnp.bfloat16
F32 = jnp.float32
MESH = pl.DeviceIdType.MESH

VMEM = pltpu.VMEM
DMA = pltpu.SemaphoreType.DMA


def here():
    row = lax.axis_index("ty")
    col = lax.axis_index("tx")
    return row, col, col // 2, col % 2


def greet_all():
    row, col, _, _ = here()
    me = row * 4 + col
    barrier = pltpu.get_barrier_semaphore()
    for step in range(1, 8):
        peer = (me + step) % 8
        pl.semaphore_signal(barrier, inc=1, device_id={"ty": peer // 4, "tx": peer % 4}, device_id_type=MESH)
    pl.semaphore_wait(barrier, 7)


def remote(src, dst, send_sem, recv_sem, ty, tx):
    return pltpu.make_async_remote_copy(
        src_ref=src, dst_ref=dst, send_sem=send_sem, recv_sem=recv_sem,
        device_id={"ty": ty, "tx": tx}, device_id_type=MESH)


def dot(a, b):
    return jnp.dot(a, b, preferred_element_type=F32)


def project_kernel(x_ref, gamma_ref, cos_ref, sin_ref, wq_h, wk_h, wv_h, wg_h, wu_h,
                   q_out, kv_out, keep_out, xs_out,
                   wq_v, wkv_v, wg_v, wu_v, h_v, st_send, st_recv,
                   qp, qd, qx, qr, kvp, kvr, qscr, dsend, drecv, own,
                   wq_sem, wkv_sem, w_sem, st_ssem, st_rsem, qd_ssem, qd_rsem, q_ssem, q_rsem,
                   kv_ssem, kv_rsem, d_ssem, d_rsem):
    row, col, chip, core = here()
    partner = col + 1 - 2 * core
    n_chunk = dsend.shape[0]

    wq_cp = [pltpu.make_async_copy(wq_h.at[:, pl.ds(512 * p, 512)], wq_v.at[p], wq_sem.at[p]) for p in range(4)]
    kv_cp = [pltpu.make_async_copy(w.at[:, :], wkv_v.at[:, pl.ds(128 * p, 128)], wkv_sem.at[p]) for p, w in enumerate((wk_h, wv_h))]
    for cp in wq_cp + kv_cp:
        cp.start()

    def weight_copies(n):
        out = []
        for quarter in range(4):
            cols = pl.ds(pl.multiple_of(2048 * quarter + 256 * n, 256), 256)
            out.append(pltpu.make_async_copy(wg_h.at[:, cols], wg_v.at[n, quarter], w_sem.at[n, quarter, 0]))
            out.append(pltpu.make_async_copy(wu_h.at[:, cols], wu_v.at[n, quarter], w_sem.at[n, quarter, 1]))
        return out

    def start_weights(n, carry):
        for cp in weight_copies(n):
            cp.start()
        return carry

    lax.fori_loop(0, n_chunk, start_weights, 0)

    xf = x_ref[...].astype(F32)
    sum1 = jnp.sum(xf, axis=1, keepdims=True)
    sum2 = jnp.sum(xf * xf, axis=1, keepdims=True)
    rows = xf.shape[0]
    eye = lax.broadcasted_iota(jnp.int32, (rows, rows), 0) == lax.broadcasted_iota(jnp.int32, (rows, rows), 1)
    line1 = jnp.sum(jnp.where(eye, sum1, 0.0), axis=0, keepdims=True)
    line2 = jnp.sum(jnp.where(eye, sum2, 0.0), axis=0, keepdims=True)
    first = lax.broadcasted_iota(jnp.int32, (8, rows), 0) == 0
    st_send[...] = jnp.where(first, line1, line2)
    greet_all()
    st_cp = [remote(st_send, st_recv.at[d - 1], st_ssem.at[d - 1], st_rsem.at[d - 1], row, (col + d) % 4) for d in (1, 2, 3)]
    for cp in st_cp:
        cp.start()
    for cp in st_cp:
        cp.wait_recv()
    total = st_send[...] + st_recv[0] + st_recv[1] + st_recv[2]
    width = 4.0 * xf.shape[1]
    mean_line = total[0:1] / width
    var_line = total[1:2] / width - mean_line * mean_line
    rstd_line = lax.rsqrt(var_line + EPSILON)
    mean = jnp.sum(jnp.where(eye, mean_line, 0.0), axis=1, keepdims=True)
    rstd = jnp.sum(jnp.where(eye, rstd_line, 0.0), axis=1, keepdims=True)
    h_v[...] = ((xf - mean) * rstd * gamma_ref[...]).astype(BF16)

    for p in range(4):
        wq_cp[p].wait()
        part = dot(h_v[...], wq_v[p]).astype(BF16)
        for d in range(8):
            qp[d % 2, d // 2, :, 512 * p:512 * p + 512] = part[16 * d:16 * d + 16]
    qd_cp = remote(qp.at[1 - core], qd, qd_ssem, qd_rsem, row, partner)
    qd_cp.start()
    for cp in kv_cp:
        cp.wait()
    kvp[...] = dot(h_v[...], wkv_v[...]).reshape(8, 16, 256)
    kv_sends = []
    for d in (1, 2, 3):
        peer = (col + d) % 4
        cp = remote(kvp.at[row * 4 + peer], kvr.at[d - 1], kv_ssem.at[d - 1], kv_rsem.at[d - 1], row, peer)
        cp.start()
        kv_sends.append(cp)

    def pair_copy(n):
        return remote(dsend.at[n], drecv.at[n], d_ssem.at[n], d_rsem.at[n], row, partner)

    def compute_chunk(n):
        for cp in weight_copies(n):
            cp.wait()
        for xr in range(2):
            quarter = 2 * xr + (1 - core)
            dsend[n, xr, 0] = dot(h_v[...], wg_v[n, quarter]).astype(BF16)
            dsend[n, xr, 1] = dot(h_v[...], wu_v[n, quarter]).astype(BF16)
        pair_copy(n).start()
        for xr in range(2):
            quarter = 2 * xr + core
            own[n % 2, xr, 0] = dot(h_v[...], wg_v[n, quarter])
            own[n % 2, xr, 1] = dot(h_v[...], wu_v[n, quarter])

    def sum_chunk(n):
        pair_copy(n).wait_recv()
        keep_out[:, n] = (own[n % 2, chip] + drecv[n, chip].astype(F32)).astype(BF16)
        xs_out[:, n] = (own[n % 2, 1 - chip] + drecv[n, 1 - chip].astype(F32)).astype(BF16)

    compute_chunk(0)

    qd_cp.wait_recv()
    qx[...] = (qp[core].astype(F32) + qd[...].astype(F32)).astype(BF16)
    mine = row * 2 + chip
    q_sends = []
    for s, (dy, dx) in enumerate(((0, 1), (1, 0), (1, 1))):
        ty, xx = (row + dy) % 2, (chip + dx) % 2
        cp = remote(qx.at[ty * 2 + xx], qr.at[s], q_ssem.at[s], q_rsem.at[s], ty, xx * 2 + core)
        cp.start()
        q_sends.append(cp)

    def step(n, carry):
        compute_chunk(n)
        sum_chunk(n - 1)
        return carry

    lax.fori_loop(1, n_chunk, step, 0)

    me = row * 4 + col
    own_rows = pl.ds(pl.multiple_of(me * 16, 16), 16)
    cosv = cos_ref[own_rows, :]
    sinv = sin_ref[own_rows, :]

    def rotate(vals):
        return vals * cosv + pltpu.roll(vals, 64, 1) * sinv

    for cp in q_sends:
        cp.wait_recv()
    q_same = qx[mine].astype(F32) + qr[0].astype(F32)
    q_diff = qr[1].astype(F32) + qr[2].astype(F32)
    for half, vals in ((row, q_same), (1 - row, q_diff)):
        for head in range(16):
            qscr[half, :, head, :] = rotate(vals[:, 128 * head:128 * head + 128])
    q_out[...] = qscr[...].astype(BF16)
    for cp in kv_sends:
        cp.wait_recv()
    kv = kvp[me] + kvr[0] + kvr[1] + kvr[2]
    kv_out[0] = rotate(kv[:, :128]).astype(BF16).astype(F32)
    kv_out[1] = kv[:, 128:].astype(BF16).astype(F32)

    sum_chunk(n_chunk - 1)
    for cp in st_cp + [qd_cp] + kv_sends + q_sends:
        cp.wait_send()

    def drain(n, carry):
        pair_copy(n).wait_send()
        return carry

    lax.fori_loop(0, n_chunk, drain, 0)


def project(x_blk, gamma, cos2, sin2, w_query, w_key, w_value, w_gate, w_up):
    rows, width = x_blk.shape
    nc = 8
    vm = pl.BlockSpec(memory_space=VMEM)
    hbm = pl.BlockSpec(memory_space=pl.ANY)
    return pl.pallas_call(
        project_kernel,
        out_shape=(
            jax.ShapeDtypeStruct((2, 16, 16, 128), BF16),
            jax.ShapeDtypeStruct((2, 16, 128), F32),
            jax.ShapeDtypeStruct((2, nc, rows, 256), BF16),
            jax.ShapeDtypeStruct((2, nc, rows, 256), BF16),
        ),
        in_specs=[vm] * 4 + [hbm] * 5,
        out_specs=(vm,) * 4,
        scratch_shapes=[
            VMEM((4, width, 512), BF16), VMEM((width, 256), BF16),
            VMEM((nc, 4, width, 256), BF16), VMEM((nc, 4, width, 256), BF16),
            VMEM((rows, width), BF16), VMEM((8, rows), F32), VMEM((3, 8, rows), F32),
            VMEM((2, 4, 16, 2048), BF16), VMEM((4, 16, 2048), BF16), VMEM((4, 16, 2048), BF16), VMEM((3, 16, 2048), BF16),
            VMEM((8, 16, 256), F32), VMEM((3, 16, 256), F32), VMEM((2, 16, 16, 128), F32),
            VMEM((nc, 2, 2, rows, 256), BF16), VMEM((nc, 2, 2, rows, 256), BF16), VMEM((2, 2, 2, rows, 256), F32),
            DMA((4,)), DMA((2,)), DMA((nc, 4, 2)), DMA((3,)), DMA((3,)), DMA, DMA, DMA((3,)), DMA((3,)),
            DMA((3,)), DMA((3,)), DMA((nc,)), DMA((nc,)),
        ],
        compiler_params=pltpu.CompilerParams(collective_id=0, has_side_effects=True, vmem_limit_bytes=56 * 2 ** 20),
        name="project",
    )(x_blk, gamma, cos2, sin2, w_query, w_key, w_value, w_gate, w_up)


SLOTS = 8
AHEAD = 6
BLOCK = 1024
FIRST = 10


def attend_kernel(first, count, lens_ref, q_ref, kv_ref, k_in, v_in, *refs):
    if first:
        refs = refs[2:]
    k_out, v_out, att_out, kbuf, vbuf, s_scr, o_scr, in_sem, out_sem = refs
    row, col, _, _ = here()
    base = (row * 4 + col) * 16
    ctx = k_in.shape[1]

    def in_copies(t):
        slot = lax.rem(t, SLOTS)
        return (pltpu.make_async_copy(k_in.at[first + t], kbuf.at[slot], in_sem.at[slot, 0]),
                pltpu.make_async_copy(v_in.at[first + t], vbuf.at[slot], in_sem.at[slot, 1]))

    def out_copies(t):
        slot = lax.rem(t, SLOTS)
        return (pltpu.make_async_copy(kbuf.at[slot], k_out.at[first + t], out_sem.at[slot, 0]),
                pltpu.make_async_copy(vbuf.at[slot], v_out.at[first + t], out_sem.at[slot, 1]))

    for t in range(min(AHEAD, count)):
        for cp in in_copies(t):
            cp.start()

    def attend(t, slot, length, blocks):
        q = jnp.concatenate([q_ref[0, first + t], q_ref[1, first + t]], axis=0)
        scale = 128.0 ** -0.5
        peak = None
        for b in range(blocks):
            scores = lax.dot_general(q, kbuf[slot, b * BLOCK:(b + 1) * BLOCK, :], (((1,), (1,)), ((), ())),
                                     preferred_element_type=F32) * scale
            if b == blocks - 1:
                pos = lax.broadcasted_iota(jnp.int32, scores.shape, 1) + b * BLOCK
                scores = jnp.where(pos <= length, scores, -1e30)
            s_scr[:, b * BLOCK:(b + 1) * BLOCK] = scores
            for g in range(BLOCK // 128):
                piece = scores[:, g * 128:(g + 1) * 128]
                peak = piece if peak is None else jnp.maximum(peak, piece)
        peak = jnp.max(peak, axis=1, keepdims=True)
        denom = None
        for b in range(blocks):
            e = jnp.exp(s_scr[:, b * BLOCK:(b + 1) * BLOCK] - peak)
            s_scr[:, b * BLOCK:(b + 1) * BLOCK] = e
            for g in range(BLOCK // 128):
                piece = e[:, g * 128:(g + 1) * 128]
                denom = piece if denom is None else denom + piece
        inv = 1.0 / jnp.sum(denom, axis=1, keepdims=True)
        out = None
        for b in range(blocks):
            probs = (s_scr[:, b * BLOCK:(b + 1) * BLOCK] * inv).astype(BF16)
            part = dot(probs, vbuf[slot, b * BLOCK:(b + 1) * BLOCK, :])
            out = part if out is None else out + part
        o_scr[t] = out

    def body(t, carry):
        slot = lax.rem(t, SLOTS)
        for cp in in_copies(t):
            cp.wait()
        length = lens_ref[base + first + t]
        start = pl.multiple_of((length // 16) * 16, 16)
        at_row = lax.broadcasted_iota(jnp.int32, (16, 128), 0) == length - start
        for which, buf in ((0, kbuf), (1, vbuf)):
            old = buf[slot, pl.ds(start, 16), :].astype(F32)
            new = kv_ref[which, pl.ds(first + t, 1), :]
            buf[slot, pl.ds(start, 16), :] = jnp.where(at_row, new, old).astype(BF16)
        for cp in out_copies(t):
            cp.start()

        @pl.when(t + AHEAD < count)
        def _():
            @pl.when(t >= SLOTS - AHEAD)
            def _():
                for cp in out_copies(t - (SLOTS - AHEAD)):
                    cp.wait()

            for cp in in_copies(t + AHEAD):
                cp.start()

        blocks = length // BLOCK
        for b in range(ctx // BLOCK):
            @pl.when(blocks == b)
            def _():
                attend(t, slot, length, b + 1)

        return carry

    lax.fori_loop(0, count, body, 0)

    for head in range(32):
        att_out[head // 16, :, 128 * (head % 16):128 * (head % 16) + 128] = o_scr[:, head, :].astype(BF16)

    done_in_loop = max(0, count - AHEAD - (SLOTS - AHEAD)) if count > AHEAD else 0
    for t in range(done_in_loop, count):
        for cp in out_copies(t):
            cp.wait()


def attend(first, count, lens, q, kv, k_blk, v_blk, prior=()):
    vm = pl.BlockSpec(memory_space=VMEM)
    hbm = pl.BlockSpec(memory_space=pltpu.HBM)
    smem = pl.BlockSpec(memory_space=pltpu.SMEM)
    _, ctx, dim = k_blk.shape
    return pl.pallas_call(
        functools.partial(attend_kernel, first, count),
        out_shape=(
            jax.ShapeDtypeStruct(k_blk.shape, BF16),
            jax.ShapeDtypeStruct(v_blk.shape, BF16),
            jax.ShapeDtypeStruct((2, count, 2048), BF16),
        ),
        in_specs=[smem, vm, vm, hbm, hbm] + [hbm] * len(prior),
        out_specs=(hbm, hbm, vm),
        input_output_aliases={5: 0, 6: 1} if prior else {},
        scratch_shapes=[
            VMEM((SLOTS, ctx, dim), BF16), VMEM((SLOTS, ctx, dim), BF16),
            VMEM((32, ctx), F32), VMEM((count, 32, dim), F32),
            DMA((SLOTS, 2)), DMA((SLOTS, 2)),
        ],
        cost_estimate=pl.CostEstimate(flops=count * 32 * ctx * dim * 4, bytes_accessed=count * ctx * dim * 8, transcendentals=count * 32 * ctx),
        compiler_params=pltpu.CompilerParams(vmem_limit_bytes=60 * 2 ** 20),
        name="attend",
    )(lens, q, kv, k_blk, v_blk, *prior)


def output_kernel(att_ref, act_own, act_far, x_ref, wo_h, wd_h, y_out,
                  wo_v, wd_v, attf, act_r, acc, ysend, yrecv,
                  wo_sem, wd_sem, a_ssem, a_rsem, f_ssem, f_rsem, c_ssem, c_rsem, y_ssem, y_rsem):
    row, col, chip, core = here()
    partner = col + 1 - 2 * core
    far = (col + 2) % 4
    far_partner = (partner + 2) % 4
    order = (col, far, partner, far_partner)
    wd_cp = []
    for s, owner in enumerate(order):
        wd_cp.append(pltpu.make_async_copy(wd_h.at[pl.ds(pl.multiple_of(owner * 2048, 2048), 2048), :], wd_v.at[s], wd_sem.at[s]))
    wo_cp = pltpu.make_async_copy(wo_h, wo_v, wo_sem)
    for cp in wd_cp + [wo_cp]:
        cp.start()

    greet_all()
    mine = row * 2 + chip
    a_cp = []
    for s, (dy, dx) in enumerate(((0, 1), (1, 0), (1, 1))):
        ty, xx = (row + dy) % 2, (chip + dx) % 2
        cp = remote(att_ref.at[ty], attf.at[mine, core], a_ssem.at[s], a_rsem.at[s], ty, xx * 2 + core)
        cp.start()
        a_cp.append(cp)
    c_cp = [remote(src, act_r.at[s], c_ssem.at[s], c_rsem.at[s], row, partner) for s, src in enumerate((act_own, act_far))]
    for cp in c_cp:
        cp.start()
    attf[mine, core] = att_ref[row]
    f_own = remote(attf.at[mine, core], attf.at[mine, core], f_ssem.at[3], f_rsem.at[3], row, partner)
    f_own.start()

    def mlp_part(s, act, cols):
        out = None
        for n in range(8):
            part = dot(act[n], wd_v[s, 256 * n:256 * n + 256, cols])
            out = part if out is None else out + part
        return out

    for s, act in ((0, act_own), (1, act_far)):
        wd_cp[s].wait()
        for c in range(4):
            cols = slice(256 * c, 256 * c + 256)
            part = mlp_part(s, act, cols)
            acc[:, cols] = part if s == 0 else acc[:, cols] + part

    f_cp = []
    for s, (dy, dx) in enumerate(((0, 1), (1, 0), (1, 1))):
        a_cp[s].wait_recv()
        index = ((row + dy) % 2) * 2 + (chip + dx) % 2
        cp = remote(attf.at[index, core], attf.at[index, core], f_ssem.at[s], f_rsem.at[s], row, partner)
        cp.start()
        f_cp.append(cp)
    for cp in c_cp:
        cp.wait_recv()
    wd_cp[2].wait()
    wd_cp[3].wait()
    for c in range(4):
        cols = slice(256 * c, 256 * c + 256)
        acc[:, cols] = acc[:, cols] + (mlp_part(2, act_r.at[0], cols) + mlp_part(3, act_r.at[1], cols))
    wo_cp.wait()
    for cp in f_cp + [f_own]:
        cp.wait_recv()
    y_cp = []
    for c in range(4):
        cols = slice(256 * c, 256 * c + 256)
        att = attf[...].reshape(128, 2048)
        ysend[c] = (acc[:, cols] + dot(att, wo_v[:, cols])).astype(BF16)
        cp = remote(ysend.at[c], yrecv.at[c], y_ssem.at[c], y_rsem.at[c], 1 - row, col)
        cp.start()
        y_cp.append(cp)
    for c in range(4):
        cols = slice(256 * c, 256 * c + 256)
        y_cp[c].wait_recv()
        both = ysend[c].astype(F32) + yrecv[c].astype(F32)
        y_out[:, cols] = (x_ref[:, cols].astype(F32) + both).astype(BF16)
    for cp in a_cp + c_cp + f_cp + [f_own] + y_cp:
        cp.wait_send()


def output(att, act_own, act_far, x_blk, w_out, w_down):
    rows, width = x_blk.shape
    vm = pl.BlockSpec(memory_space=VMEM)
    hbm = pl.BlockSpec(memory_space=pl.ANY)
    return pl.pallas_call(
        output_kernel,
        out_shape=jax.ShapeDtypeStruct((rows, width), BF16),
        in_specs=[vm] * 4 + [hbm] * 2,
        out_specs=vm,
        scratch_shapes=[
            VMEM((2048, width), BF16), VMEM((4, 2048, width), BF16), VMEM((4, 2, 16, 2048), BF16), VMEM((2, 8, rows, 256), BF16),
            VMEM((rows, width), F32), VMEM((4, rows, 256), BF16), VMEM((4, rows, 256), BF16),
            DMA, DMA((4,)), DMA((3,)), DMA((3,)), DMA((4,)), DMA((4,)), DMA((2,)), DMA((2,)), DMA((4,)), DMA((4,)),
        ],
        compiler_params=pltpu.CompilerParams(collective_id=1, has_side_effects=True, vmem_limit_bytes=40 * 2 ** 20),
        name="output",
    )(att, act_own, act_far, x_blk, w_out, w_down)


def solution(mesh):
    cache_spec = P(("dp", "ty", "tx"), None, None)
    across = [(0, 2), (1, 3), (2, 0), (3, 1)]

    def layer_shard(x_blk, lens, k_blk, v_blk, gamma, w_query, w_key, w_value, w_gate, w_up, w_out, w_down):
        half = 64
        inv_freqs = ROPE_BASE ** (-(jnp.arange(half, dtype=F32) * 2.0) / (2 * half))
        angles = lens.astype(F32)[:, None] * inv_freqs[None, :]
        cos, sin = jnp.cos(angles), jnp.sin(angles)
        cos2 = jnp.concatenate([cos, cos], axis=1)
        sin2 = jnp.concatenate([-sin, sin], axis=1)
        q, kv, keep, xs = project(x_blk, gamma[None, :], cos2, sin2, w_query, w_key, w_value, w_gate, w_up)
        got = lax.ppermute(xs, "tx", across)
        k_half, v_half, att_a = attend(0, FIRST, lens, q, kv, k_blk, v_blk)
        got, att_a = lax.optimization_barrier((got, att_a))
        full = (keep.astype(F32) + got.astype(F32)).astype(BF16).astype(F32)
        act = (jax.nn.silu(full[0]) * full[1]).astype(BF16)
        act_far = lax.ppermute(act, "tx", across)
        lens, act = lax.optimization_barrier((lens, act))
        k_out, v_out, att_b = attend(FIRST, 16 - FIRST, lens, q, kv, k_blk, v_blk, (k_half, v_half))
        att = jnp.concatenate([att_a, att_b], axis=1)
        y = output(att, act, act_far, x_blk, w_out, w_down)
        return y, k_out, v_out

    in_specs = (P("dp", "tx"), P("dp"), cache_spec, cache_spec, P("tx"), P("tx", "ty"), P("tx", None), P("tx", None), P("tx", "ty"), P("tx", "ty"), P("ty", "tx"), P("ty", "tx"))
    out_specs = (P("dp", "tx"), cache_spec, cache_spec)
    return jax.shard_map(layer_shard, mesh=mesh, in_specs=in_specs, out_specs=out_specs, check_vma=False)
```

```python
import functools

import jax
import jax.numpy as jnp
import numpy as np
from jax import lax
from jax.experimental import pallas as pl
from jax.experimental.pallas import tpu as pltpu
from jax.sharding import PartitionSpec as P

EPSILON = 1e-6
ROPE_BASE = 10000.0
BF16 = jnp.bfloat16
F32 = jnp.float32
MESH = pl.DeviceIdType.MESH

VMEM = pltpu.VMEM
VMEM_ALL = 67043328
DMA = pltpu.SemaphoreType.DMA


def here():
    row = lax.axis_index("ty")
    col = lax.axis_index("tx")
    return row, col, col // 2, col % 2


def greet():
    row, col, _, _ = here()
    me = row * 4 + col
    barrier = pltpu.get_barrier_semaphore()
    for step in range(1, 8):
        peer = (me + step) % 8
        pl.semaphore_signal(barrier, inc=1, device_id={"ty": peer // 4, "tx": peer % 4}, device_id_type=MESH)


def greeted():
    pl.semaphore_wait(pltpu.get_barrier_semaphore(), 7)


def remote(src, dst, send_sem, recv_sem, ty, tx):
    return pltpu.make_async_remote_copy(
        src_ref=src, dst_ref=dst, send_sem=send_sem, recv_sem=recv_sem,
        device_id={"ty": ty, "tx": tx}, device_id_type=MESH)


def dot(a, b):
    return jnp.dot(a, b, preferred_element_type=F32)


CHUNKS = 8


def gated(g, u):
    return (jax.nn.silu(g.astype(BF16).astype(F32)) * u.astype(BF16).astype(F32)).astype(BF16)


def project_kernel(lens_h, x_h, gamma_h, freq_h, wq_h, wk_h, wv_h, wg_h, wu_h,
                   q_hbm, kv_hbm, keep_hbm, pay_hbm,
                   lens_ref, freq_ref, q_out, kv_out, keep_out, pay_out, res_sem, keep_sem, x_ref, gamma_ref, x_sem, wq_v, wkv_v, wg_v, wu_v, h_v, st_send, st_recv,
                   qp, qd, qx, qr, kvp, kvr, qscr, dsend, drecv, own,
                   wq_sem, wkv_sem, w_sem, st_ssem, st_rsem, qd_ssem, qd_rsem, q_ssem, q_rsem,
                   kv_ssem, kv_rsem, d_ssem, d_rsem):
    row, col, chip, core = here()
    partner = col + 1 - 2 * core
    me = row * 4 + col
    greet()

    x_cp = pltpu.make_async_copy(x_h, x_ref, x_sem.at[0])
    gamma_cp = pltpu.make_async_copy(gamma_h, gamma_ref, x_sem.at[1])
    lens_cp = pltpu.make_async_copy(lens_h, lens_ref, x_sem.at[2])
    freq_cp = pltpu.make_async_copy(freq_h, freq_ref, x_sem.at[3])
    for cp in (x_cp, gamma_cp, lens_cp, freq_cp):
        cp.start()
    wq_cp = [pltpu.make_async_copy(wq_h.at[:, pl.ds(512 * p, 512)], wq_v.at[p], wq_sem.at[p]) for p in range(4)]
    kv_cp = [pltpu.make_async_copy(w.at[:, :], wkv_v.at[:, pl.ds(128 * p, 128)], wkv_sem.at[p]) for p, w in enumerate((wk_h, wv_h))]
    for cp in wq_cp + kv_cp:
        cp.start()

    def weight_copies(n):
        out = []
        for quarter in range(4):
            cols = pl.ds(pl.multiple_of(2048 * quarter + 256 * n, 256), 256)
            out.append(pltpu.make_async_copy(wg_h.at[:, cols], wg_v.at[n, quarter], w_sem.at[n, quarter, 0]))
            out.append(pltpu.make_async_copy(wu_h.at[:, cols], wu_v.at[n, quarter], w_sem.at[n, quarter, 1]))
        return out

    def start_weights(n, carry):
        for cp in weight_copies(n):
            cp.start()
        return carry

    lax.fori_loop(0, CHUNKS, start_weights, 0)

    x_cp.wait()
    xf = x_ref[...].astype(F32)
    sum1 = jnp.sum(xf, axis=1, keepdims=True)
    sum2 = jnp.sum(xf * xf, axis=1, keepdims=True)
    rows = xf.shape[0]
    eye = lax.broadcasted_iota(jnp.int32, (rows, rows), 0) == lax.broadcasted_iota(jnp.int32, (rows, rows), 1)
    line1 = jnp.sum(jnp.where(eye, sum1, 0.0), axis=0, keepdims=True)
    line2 = jnp.sum(jnp.where(eye, sum2, 0.0), axis=0, keepdims=True)
    first = lax.broadcasted_iota(jnp.int32, (8, rows), 0) == 0
    st_send[...] = jnp.where(first, line1, line2)
    greeted()
    st_cp = [remote(st_send, st_recv.at[d - 1], st_ssem.at[d - 1], st_rsem.at[d - 1], row, (col + d) % 4) for d in (1, 2, 3)]
    for cp in st_cp:
        cp.start()
    lens_cp.wait()
    freq_cp.wait()
    seq = lax.broadcasted_iota(jnp.int32, (16, 128), 0)
    place = jnp.zeros((16, 128), F32)
    for b in range(16):
        place = jnp.where(seq == b, lens_ref[me * 16 + b].astype(F32), place)
    angle = place * freq_ref[...]
    cosv = jnp.cos(angle)
    sinv = jnp.where(lax.broadcasted_iota(jnp.int32, (16, 128), 1) < 64, -jnp.sin(angle), jnp.sin(angle))
    for cp in st_cp:
        cp.wait_recv()
    total = st_send[...] + st_recv[0] + st_recv[1] + st_recv[2]
    width = 4.0 * xf.shape[1]
    mean_line = total[0:1] / width
    var_line = total[1:2] / width - mean_line * mean_line
    rstd_line = lax.rsqrt(var_line + EPSILON)
    mean = jnp.sum(jnp.where(eye, mean_line, 0.0), axis=1, keepdims=True)
    rstd = jnp.sum(jnp.where(eye, rstd_line, 0.0), axis=1, keepdims=True)
    gamma_cp.wait()
    h_v[...] = ((xf - mean) * rstd * gamma_ref[...]).astype(BF16)

    for cp in wq_cp:
        cp.wait()
    for p in range(4):
        part = dot(h_v[...], wq_v[p]).astype(BF16)
        for d in range(8):
            qp[d % 2, d // 2, :, 512 * p:512 * p + 512] = part[16 * d:16 * d + 16]
    qd_cp = remote(qp.at[1 - core], qd, qd_ssem, qd_rsem, row, partner)
    qd_cp.start()
    for cp in kv_cp:
        cp.wait()
    kvp[...] = dot(h_v[...], wkv_v[...]).reshape(8, 16, 256)
    kv_sends = []
    for d in (1, 2, 3):
        peer = (col + d) % 4
        cp = remote(kvp.at[row * 4 + peer], kvr.at[d - 1], kv_ssem.at[d - 1], kv_rsem.at[d - 1], row, peer)
        cp.start()
        kv_sends.append(cp)

    def pair_copy(n):
        return remote(dsend.at[n], drecv.at[n], d_ssem.at[n], d_rsem.at[n], row, partner)

    def compute_chunk(n):
        for cp in weight_copies(n):
            cp.wait()
        for xr in range(2):
            quarter = 2 * xr + (1 - core)
            dsend[n, xr, 0] = dot(h_v[...], wg_v[n, quarter]).astype(BF16)
            dsend[n, xr, 1] = dot(h_v[...], wu_v[n, quarter]).astype(BF16)
        pair_copy(n).start()
        for xr in range(2):
            quarter = 2 * xr + core
            own[n % 3, xr, 0] = dot(h_v[...], wg_v[n, quarter])
            own[n % 3, xr, 1] = dot(h_v[...], wu_v[n, quarter])

    def sum_chunk(n):
        pair_copy(n).wait_recv()
        keep = own[n % 3, chip] + drecv[n, chip].astype(F32)
        give = (own[n % 3, 1 - chip] + drecv[n, 1 - chip].astype(F32)).astype(BF16)
        return keep, give

    def sum_late(n):
        keep, give = sum_chunk(n)
        for part in range(2):
            keep_out[part * CHUNKS + n] = keep[part].astype(BF16)
            pay_out[part * CHUNKS + n] = give[part]
        for cp in late_copies(n):
            cp.start()

    def late_copies(m):
        out = []
        for part in range(2):
            block = part * CHUNKS + m
            out.append(pltpu.make_async_copy(keep_out.at[block], keep_hbm.at[block], keep_sem.at[block, 0]))
            out.append(pltpu.make_async_copy(pay_out.at[block], pay_hbm.at[block], keep_sem.at[block, 1]))
        return out

    compute_chunk(0)

    qd_cp.wait_recv()
    qx[...] = (qp[core].astype(F32) + qd[...].astype(F32)).astype(BF16)
    mine = row * 2 + chip
    q_sends = []
    for s, (dy, dx) in enumerate(((0, 1), (1, 0), (1, 1))):
        ty, xx = (row + dy) % 2, (chip + dx) % 2
        cp = remote(qx.at[ty * 2 + xx], qr.at[s], q_ssem.at[s], q_rsem.at[s], ty, xx * 2 + core)
        cp.start()
        q_sends.append(cp)

    compute_chunk(1)

    def step(n, carry):
        compute_chunk(n)
        sum_late(n - 2)
        return carry

    lax.fori_loop(2, CHUNKS, step, 0)
    sum_late(CHUNKS - 2)

    def rotate(vals):
        return vals * cosv + pltpu.roll(vals, 64, 1) * sinv

    for cp in q_sends:
        cp.wait_recv()
    q_same = qx[mine].astype(F32) + qr[0].astype(F32)
    q_diff = qr[1].astype(F32) + qr[2].astype(F32)
    for half, vals in ((row, q_same), (1 - row, q_diff)):
        for head in range(16):
            qscr[half, :, head, :] = rotate(vals[:, 128 * head:128 * head + 128])
    q_out[...] = qscr[...].astype(BF16)
    q_cp = pltpu.make_async_copy(q_out, q_hbm, res_sem.at[0])
    q_cp.start()
    for cp in kv_sends:
        cp.wait_recv()
    kv = kvp[me] + kvr[0] + kvr[1] + kvr[2]
    kv_out[0] = rotate(kv[:, :128]).astype(BF16).astype(F32)
    kv_out[1] = kv[:, 128:].astype(BF16).astype(F32)

    kv_cp = pltpu.make_async_copy(kv_out, kv_hbm, res_sem.at[1])
    kv_cp.start()
    sum_late(CHUNKS - 1)
    for cp in (q_cp, kv_cp):
        cp.wait()
    for m in range(CHUNKS):
        for cp in late_copies(m):
            cp.wait()
    for cp in st_cp + [qd_cp] + kv_sends + q_sends:
        cp.wait_send()

    def drain(n, carry):
        pair_copy(n).wait_send()
        return carry

    lax.fori_loop(0, CHUNKS, drain, 0)


def project(lens, x_blk, gamma, freqs, w_query, w_key, w_value, w_gate, w_up):
    rows, width = x_blk.shape
    nc = CHUNKS
    hbm = pl.BlockSpec(memory_space=pl.ANY)
    return pl.pallas_call(
        project_kernel,
        out_shape=(
            jax.ShapeDtypeStruct((2, 16, 16, 128), BF16),
            jax.ShapeDtypeStruct((2, 16, 128), F32),
            jax.ShapeDtypeStruct((2 * CHUNKS, rows, 256), BF16),
            jax.ShapeDtypeStruct((2 * CHUNKS, rows, 256), BF16),
        ),
        in_specs=[hbm] * 9,
        out_specs=(hbm,) * 4,
        scratch_shapes=[
            pltpu.SMEM((128,), jnp.int32), VMEM((1, 128), F32), VMEM((2, 16, 16, 128), BF16), VMEM((2, 16, 128), F32),
            VMEM((2 * CHUNKS, rows, 256), BF16), VMEM((2 * CHUNKS, rows, 256), BF16),
            DMA((2,)), DMA((2 * CHUNKS, 2)),
            VMEM((rows, width), BF16), VMEM((1, width), F32), DMA((4,)),
            VMEM((4, width, 512), BF16), VMEM((width, 256), BF16),
            VMEM((nc, 4, width, 256), BF16), VMEM((nc, 4, width, 256), BF16),
            VMEM((rows, width), BF16), VMEM((8, rows), F32), VMEM((3, 8, rows), F32),
            VMEM((2, 4, 16, 2048), BF16), VMEM((4, 16, 2048), BF16), VMEM((4, 16, 2048), BF16), VMEM((3, 16, 2048), BF16),
            VMEM((8, 16, 256), F32), VMEM((3, 16, 256), F32), VMEM((2, 16, 16, 128), F32),
            VMEM((nc, 2, 2, rows, 256), BF16), VMEM((nc, 2, 2, rows, 256), BF16), VMEM((3, 2, 2, rows, 256), F32),
            DMA((4,)), DMA((2,)), DMA((nc, 4, 2)), DMA((3,)), DMA((3,)), DMA, DMA, DMA((3,)), DMA((3,)),
            DMA((3,)), DMA((3,)), DMA((nc,)), DMA((nc,)),
        ],
        compiler_params=pltpu.CompilerParams(collective_id=0, has_side_effects=True, vmem_limit_bytes=VMEM_ALL),
        name="project",
    )(lens, x_blk, gamma, freqs, w_query, w_key, w_value, w_gate, w_up)


SLOTS = 12
AHEAD = 7
BLOCK = 1024


def attend_kernel(lens_h, q_h, kv_h, k_in, v_in, k_out, v_out, att_hbm,
                  kbuf, vbuf, s_scr, in_sem, out_sem, att_out, lens_ref, q_ref, kv_ref, o_scr, small_sem):
    row, col, _, _ = here()
    base = (row * 4 + col) * 16
    count, ctx, _ = k_in.shape

    def in_copies(t):
        slot = lax.rem(t, SLOTS)
        return (pltpu.make_async_copy(k_in.at[t], kbuf.at[slot], in_sem.at[slot, 0]),
                pltpu.make_async_copy(v_in.at[t], vbuf.at[slot], in_sem.at[slot, 1]))

    def out_copies(t):
        slot = lax.rem(t, SLOTS)
        return (pltpu.make_async_copy(kbuf.at[slot], k_out.at[t], out_sem.at[slot, 0]),
                pltpu.make_async_copy(vbuf.at[slot], v_out.at[t], out_sem.at[slot, 1]))

    small = [pltpu.make_async_copy(src, dst, small_sem.at[s]) for s, (src, dst) in enumerate(((lens_h, lens_ref), (q_h, q_ref), (kv_h, kv_ref)))]
    for cp in small:
        cp.start()
    for t in range(min(AHEAD, count)):
        for cp in in_copies(t):
            cp.start()
    for cp in small:
        cp.wait()

    def attend(t, slot, length, blocks):
        q = jnp.concatenate([q_ref[0, t], q_ref[1, t]], axis=0)
        scale = 128.0 ** -0.5
        peak = None
        for b in range(blocks):
            scores = lax.dot_general(q, kbuf[slot, b * BLOCK:(b + 1) * BLOCK, :], (((1,), (1,)), ((), ())),
                                     preferred_element_type=F32) * scale
            if b == blocks - 1:
                pos = lax.broadcasted_iota(jnp.int32, scores.shape, 1) + b * BLOCK
                scores = jnp.where(pos <= length, scores, -1e30)
            s_scr[:, b * BLOCK:(b + 1) * BLOCK] = scores
            for g in range(BLOCK // 128):
                piece = scores[:, g * 128:(g + 1) * 128]
                peak = piece if peak is None else jnp.maximum(peak, piece)
        peak = jnp.max(peak, axis=1, keepdims=True)
        denom = None
        for b in range(blocks):
            e = jnp.exp(s_scr[:, b * BLOCK:(b + 1) * BLOCK] - peak)
            s_scr[:, b * BLOCK:(b + 1) * BLOCK] = e
            for g in range(BLOCK // 128):
                piece = e[:, g * 128:(g + 1) * 128]
                denom = piece if denom is None else denom + piece
        inv = 1.0 / jnp.sum(denom, axis=1, keepdims=True)
        out = None
        for b in range(blocks):
            probs = (s_scr[:, b * BLOCK:(b + 1) * BLOCK] * inv).astype(BF16)
            part = dot(probs, vbuf[slot, b * BLOCK:(b + 1) * BLOCK, :])
            out = part if out is None else out + part
        o_scr[t] = out

    def body(t, carry):
        slot = lax.rem(t, SLOTS)
        for cp in in_copies(t):
            cp.wait()
        length = lens_ref[base + t]
        start = pl.multiple_of((length // 16) * 16, 16)
        at_row = lax.broadcasted_iota(jnp.int32, (16, 128), 0) == length - start
        for which, buf in ((0, kbuf), (1, vbuf)):
            old = buf[slot, pl.ds(start, 16), :].astype(F32)
            new = kv_ref[which, pl.ds(t, 1), :]
            buf[slot, pl.ds(start, 16), :] = jnp.where(at_row, new, old).astype(BF16)
        for cp in out_copies(t):
            cp.start()

        @pl.when(t + AHEAD < count)
        def _():
            @pl.when(t >= SLOTS - AHEAD)
            def _():
                for cp in out_copies(t - (SLOTS - AHEAD)):
                    cp.wait()

            for cp in in_copies(t + AHEAD):
                cp.start()

        blocks = length // BLOCK
        for b in range(ctx // BLOCK):
            @pl.when(blocks == b)
            def _():
                attend(t, slot, length, b + 1)

        return carry

    lax.fori_loop(0, count, body, 0)

    for head in range(32):
        att_out[head // 16, :, 128 * (head % 16):128 * (head % 16) + 128] = o_scr[:, head, :].astype(BF16)
    res = pltpu.make_async_copy(att_out, att_hbm, small_sem.at[3])
    res.start()
    done_in_loop = max(0, count - AHEAD - (SLOTS - AHEAD)) if count > AHEAD else 0
    for t in range(done_in_loop, count):
        for cp in out_copies(t):
            cp.wait()
    res.wait()


def attend(lens, q, kv, k_blk, v_blk):
    hbm = pl.BlockSpec(memory_space=pltpu.HBM)
    count, ctx, dim = k_blk.shape
    return pl.pallas_call(
        attend_kernel,
        out_shape=(
            jax.ShapeDtypeStruct(k_blk.shape, BF16),
            jax.ShapeDtypeStruct(v_blk.shape, BF16),
            jax.ShapeDtypeStruct((2, count, 2048), BF16),
        ),
        in_specs=[hbm] * 5,
        out_specs=(hbm,) * 3,
        scratch_shapes=[
            VMEM((SLOTS, ctx, dim), BF16), VMEM((SLOTS, ctx, dim), BF16),
            VMEM((32, ctx), F32), DMA((SLOTS, 2)), DMA((SLOTS, 2)), VMEM((2, count, 2048), BF16),
            pltpu.SMEM((128,), jnp.int32), VMEM((2, 16, 16, 128), BF16), VMEM((2, 16, 128), F32),
            VMEM((count, 32, dim), F32), DMA((4,)),
        ],
        cost_estimate=pl.CostEstimate(flops=count * 32 * ctx * dim * 4, bytes_accessed=count * ctx * dim * 8, transcendentals=count * 32 * ctx),
        compiler_params=pltpu.CompilerParams(vmem_limit_bytes=VMEM_ALL),
        name="attend",
    )(lens, q, kv, k_blk, v_blk)


HALF = 64
PIECES = 4


def output_kernel(att_h, keep_h, got_h, x_h, wo_h, wd_h, y_hbm,
                  att_ref, keep_v, got_v, x_ref, y_out, act_v, in_sem, wo_v, wd_v, attf, acc, ysend, yrecv,
                  wo_sem, wd_sem, a_ssem, a_rsem, f_ssem, f_rsem, g_ssem, g_rsem, h_ssem, h_rsem, c_ssem, c_rsem, y_ssem, y_rsem):
    greet()
    row, col, chip, core = here()
    partner = col + 1 - 2 * core
    far = (col + 2) % 4
    far_partner = (partner + 2) % 4
    order = (col, far, partner, far_partner)
    in_cp = [pltpu.make_async_copy(src, dst, in_sem.at[s]) for s, (src, dst) in enumerate(((att_h, att_ref), (keep_h, keep_v), (got_h, got_v), (x_h, x_ref)))]
    for cp in in_cp:
        cp.start()
    wd_cp = []
    for s, owner in enumerate(order):
        wd_cp.append(pltpu.make_async_copy(wd_h.at[pl.ds(pl.multiple_of(owner * 2048, 2048), 2048), :], wd_v.at[s], wd_sem.at[s]))
    wo_cp = pltpu.make_async_copy(wo_h, wo_v, wo_sem)

    in_cp[0].wait()
    greeted()
    mine = row * 2 + chip
    around = ((0, 1), (1, 0), (1, 1))
    a_cp = []
    for s, (dy, dx) in enumerate(around):
        ty, xx = (row + dy) % 2, (chip + dx) % 2
        cp = remote(att_ref.at[ty], attf.at[mine, core], a_ssem.at[s], a_rsem.at[s], ty, xx * 2 + core)
        cp.start()
        a_cp.append(cp)
    attf[mine, core] = att_ref[row]
    f_own = remote(attf.at[mine, core], attf.at[mine, core], f_ssem.at[3], f_rsem.at[3], row, partner)
    f_own.start()

    def piece(s, r, p):
        return act_v.at[s, r, :, pl.ds(512 * p, 512)]

    in_cp[1].wait()
    in_cp[2].wait()
    for cp in (wd_cp[0], wd_cp[2], wo_cp, wd_cp[1], wd_cp[3]):
        cp.start()
    g_cp, h_cp, c_cp = {}, {}, []
    for r in range(2):
        rows = slice(HALF * r, HALF * r + HALF)
        for p in range(PIECES):
            for n in (2 * p, 2 * p + 1):
                g = keep_v[n, rows].astype(F32) + got_v[n, rows].astype(F32)
                u = keep_v[CHUNKS + n, rows].astype(F32) + got_v[CHUNKS + n, rows].astype(F32)
                act_v[0, r, :, 256 * n:256 * n + 256] = gated(g, u)
            g_cp[r, p] = remote(piece(0, r, p), piece(1, r, p), g_ssem.at[r, p], g_rsem.at[r, p], row, far)
            g_cp[r, p].start()
            h_cp[r, p] = remote(piece(1, r, p), piece(3, r, p), h_ssem.at[r, p], h_rsem.at[r, p], row, partner)
        cp = remote(act_v.at[0, r], act_v.at[2, r], c_ssem.at[r], c_rsem.at[r], row, partner)
        cp.start()
        c_cp.append(cp)

    def whole(s):
        return act_v[s].reshape(2 * HALF, 2048)

    def add(lhs, rhs, first=False):
        for c in range(2):
            cols = slice(512 * c, 512 * c + 512)
            part = dot(lhs, rhs[:, cols])
            acc[:, cols] = part if first else acc[:, cols] + part

    wd_cp[0].wait()
    add(whole(0), wd_v.at[0], True)
    for cp in c_cp:
        cp.wait_recv()
    wd_cp[2].wait()
    add(whole(2), wd_v.at[2])
    f_cp = []
    for s, (dy, dx) in enumerate(around):
        a_cp[s].wait_recv()
        index = ((row + dy) % 2) * 2 + (chip + dx) % 2
        cp = remote(attf.at[index, core], attf.at[index, core], f_ssem.at[s], f_rsem.at[s], row, partner)
        cp.start()
        f_cp.append(cp)
    wo_cp.wait()
    for cp in f_cp + [f_own]:
        cp.wait_recv()
    add(attf[...].reshape(2 * HALF, 2048), wo_v)
    wd_cp[1].wait()
    wd_cp[3].wait()
    y_cp = {}
    for r in range(2):
        rows = slice(HALF * r, HALF * r + HALF)
        for p in range(PIECES):
            g_cp[r, p].wait_recv()
            h_cp[r, p].start()
        for p in range(PIECES):
            h_cp[r, p].wait_recv()
        for c in range(2):
            cols = slice(512 * c, 512 * c + 512)
            part = dot(act_v[1, r], wd_v[1, :, cols]) + dot(act_v[3, r], wd_v[3, :, cols])
            ysend[r, c] = (acc[rows, cols] + part).astype(BF16)
            y_cp[r, c] = remote(ysend.at[r, c], yrecv.at[r, c], y_ssem.at[r, c], y_rsem.at[r, c], 1 - row, col)
            y_cp[r, c].start()
    in_cp[3].wait()
    for r in range(2):
        rows = slice(HALF * r, HALF * r + HALF)
        for c in range(2):
            cols = slice(512 * c, 512 * c + 512)
            y_cp[r, c].wait_recv()
            both = ysend[r, c].astype(F32) + yrecv[r, c].astype(F32)
            y_out[rows, cols] = (x_ref[rows, cols].astype(F32) + both).astype(BF16)
    res = pltpu.make_async_copy(y_out, y_hbm, in_sem.at[0])
    res.start()
    for cp in a_cp + c_cp + f_cp + [f_own] + list(g_cp.values()) + list(h_cp.values()) + list(y_cp.values()):
        cp.wait_send()
    res.wait()


def output(att, keep, got, x_blk, w_out, w_down):
    rows, width = x_blk.shape
    hbm = pl.BlockSpec(memory_space=pl.ANY)
    return pl.pallas_call(
        output_kernel,
        out_shape=jax.ShapeDtypeStruct((rows, width), BF16),
        in_specs=[hbm] * 6,
        out_specs=hbm,
        scratch_shapes=[
            VMEM((2, 16, 2048), BF16), VMEM((2 * CHUNKS, rows, 256), BF16), VMEM((2 * CHUNKS, rows, 256), BF16),
            VMEM((rows, width), BF16), VMEM((rows, width), BF16),
            VMEM((4, 2, HALF, 256 * CHUNKS), BF16), DMA((4,)),
            VMEM((2048, width), BF16), VMEM((4, 2048, width), BF16), VMEM((4, 2, 16, 2048), BF16),
            VMEM((rows, width), F32), VMEM((2, 2, HALF, 512), BF16), VMEM((2, 2, HALF, 512), BF16),
            DMA, DMA((4,)), DMA((3,)), DMA((3,)), DMA((4,)), DMA((4,)), DMA((2, PIECES)), DMA((2, PIECES)), DMA((2, PIECES)), DMA((2, PIECES)),
            DMA((2,)), DMA((2,)), DMA((2, 2)), DMA((2, 2)),
        ],
        compiler_params=pltpu.CompilerParams(collective_id=1, has_side_effects=True, vmem_limit_bytes=VMEM_ALL),
        name="output",
    )(att, keep, got, x_blk, w_out, w_down)


def solution(mesh):
    cache_spec = P(("dp", "ty", "tx"), None, None)
    across = [(0, 2), (1, 3), (2, 0), (3, 1)]

    def layer_shard(x_blk, lens, k_blk, v_blk, gamma, w_query, w_key, w_value, w_gate, w_up, w_out, w_down):
        freqs = np.tile(np.float32(ROPE_BASE ** (-np.arange(0, 128, 2) / 128.0)), 2)[None, :]
        q, kv, keep, pay = project(lens, x_blk, gamma[None, :], freqs, w_query, w_key, w_value, w_gate, w_up)
        got = lax.ppermute(pay, "tx", across)
        k_out, v_out, att = attend(lens, q, kv, k_blk, v_blk)
        y = output(att, keep, got, x_blk, w_out, w_down)
        return y, k_out, v_out

    in_specs = (P("dp", "tx"), P("dp"), cache_spec, cache_spec, P("tx"), P("tx", "ty"), P("tx", None), P("tx", None), P("tx", "ty"), P("tx", "ty"), P("ty", "tx"), P("ty", "tx"))
    out_specs = (P("dp", "tx"), cache_spec, cache_spec)
    return jax.shard_map(layer_shard, mesh=mesh, in_specs=in_specs, out_specs=out_specs, check_vma=False)
```

```python
import functools

import jax
import jax.numpy as jnp
import numpy as np
from jax import lax
from jax.experimental import pallas as pl
from jax.experimental.pallas import tpu as pltpu
from jax.sharding import PartitionSpec as P

EPSILON = 1e-6
ROPE_BASE = 10000.0
BF16 = jnp.bfloat16
F32 = jnp.float32
MESH = pl.DeviceIdType.MESH

VMEM = pltpu.VMEM
VMEM_ALL = 67043328
DMA = pltpu.SemaphoreType.DMA


def here():
    row = lax.axis_index("ty")
    col = lax.axis_index("tx")
    return row, col, col // 2, col % 2


def greet():
    row, col, _, _ = here()
    me = row * 4 + col
    barrier = pltpu.get_barrier_semaphore()
    for step in range(1, 8):
        peer = (me + step) % 8
        pl.semaphore_signal(barrier, inc=1, device_id={"ty": peer // 4, "tx": peer % 4}, device_id_type=MESH)


def greeted():
    pl.semaphore_wait(pltpu.get_barrier_semaphore(), 7)


def remote(src, dst, send_sem, recv_sem, ty, tx):
    return pltpu.make_async_remote_copy(
        src_ref=src, dst_ref=dst, send_sem=send_sem, recv_sem=recv_sem,
        device_id={"ty": ty, "tx": tx}, device_id_type=MESH)


def dot(a, b):
    return jnp.dot(a, b, preferred_element_type=F32)


CHUNKS = 8
EARLY = 1
LATE = CHUNKS - EARLY


def gated(g, u):
    return (jax.nn.silu(g.astype(BF16).astype(F32)) * u.astype(BF16).astype(F32)).astype(BF16)


def project_kernel(lens_h, x_h, gamma_h, freq_h, wq_h, wk_h, wv_h, wg_h, wu_h,
                   q_hbm, kv_hbm, keep_hbm, pay_hbm,
                   lens_ref, freq_ref, q_out, kv_out, keep_out, pay_out, act_out, res_sem, keep_sem, act_sem, x_ref, gamma_ref, x_sem, wq_v, wg_v, wu_v, h_v, st_send, st_recv,
                   qp, qd, qx, qr, qscr, dsend, drecv, own, xkeep, xsend, xrecv,
                   wq_sem, w_sem, st_ssem, st_rsem, qd_ssem, qd_rsem, q_ssem, q_rsem,
                   d_ssem, d_rsem, x_ssem, x_rsem):
    row, col, chip, core = here()
    partner = col + 1 - 2 * core
    far = (col + 2) % 4
    me = row * 4 + col
    greet()

    x_cp = pltpu.make_async_copy(x_h, x_ref, x_sem.at[0])
    gamma_cp = pltpu.make_async_copy(gamma_h, gamma_ref, x_sem.at[1])
    lens_cp = pltpu.make_async_copy(lens_h, lens_ref, x_sem.at[2])
    freq_cp = pltpu.make_async_copy(freq_h, freq_ref, x_sem.at[3])
    for cp in (x_cp, gamma_cp, lens_cp, freq_cp):
        cp.start()
    q_width = wq_h.shape[1]
    wq_cp = [pltpu.make_async_copy(wq_h, wq_v.at[:, pl.ds(0, q_width)], wq_sem.at[0]),
             pltpu.make_async_copy(wk_h, wq_v.at[:, pl.ds(q_width, 128)], wq_sem.at[1]),
             pltpu.make_async_copy(wv_h, wq_v.at[:, pl.ds(q_width + 128, 128)], wq_sem.at[2])]
    for cp in wq_cp:
        cp.start()

    def weight_copies(n):
        cols = pl.ds(pl.multiple_of(1024 * n, 1024), 1024)
        return (pltpu.make_async_copy(wg_h.at[:, cols], wg_v.at[n], w_sem.at[n, 0]),
                pltpu.make_async_copy(wu_h.at[:, cols], wu_v.at[n], w_sem.at[n, 1]))

    def start_weights(n, carry):
        for cp in weight_copies(n):
            cp.start()
        return carry

    lax.fori_loop(0, CHUNKS, start_weights, 0)

    x_cp.wait()
    xf = x_ref[...].astype(F32)
    sum1 = jnp.sum(xf, axis=1, keepdims=True)
    sum2 = jnp.sum(xf * xf, axis=1, keepdims=True)
    rows = xf.shape[0]
    eye = lax.broadcasted_iota(jnp.int32, (rows, rows), 0) == lax.broadcasted_iota(jnp.int32, (rows, rows), 1)
    line1 = jnp.sum(jnp.where(eye, sum1, 0.0), axis=0, keepdims=True)
    line2 = jnp.sum(jnp.where(eye, sum2, 0.0), axis=0, keepdims=True)
    first = lax.broadcasted_iota(jnp.int32, (8, rows), 0) == 0
    st_send[...] = jnp.where(first, line1, line2)
    greeted()
    st_cp = [remote(st_send, st_recv.at[d - 1], st_ssem.at[d - 1], st_rsem.at[d - 1], row, (col + d) % 4) for d in (1, 2, 3)]
    for cp in st_cp:
        cp.start()
    lens_cp.wait()
    freq_cp.wait()
    seq = lax.broadcasted_iota(jnp.int32, (16, 128), 0)
    place = jnp.zeros((16, 128), F32)
    for b in range(16):
        place = jnp.where(seq == b, lens_ref[me * 16 + b].astype(F32), place)
    angle = place * freq_ref[...]
    cosv = jnp.cos(angle)
    sinv = jnp.where(lax.broadcasted_iota(jnp.int32, (16, 128), 1) < 64, -jnp.sin(angle), jnp.sin(angle))
    for cp in st_cp:
        cp.wait_recv()
    total = st_send[...] + st_recv[0] + st_recv[1] + st_recv[2]
    width = 4.0 * xf.shape[1]
    mean_line = total[0:1] / width
    var_line = total[1:2] / width - mean_line * mean_line
    rstd_line = lax.rsqrt(var_line + EPSILON)
    mean = jnp.sum(jnp.where(eye, mean_line, 0.0), axis=1, keepdims=True)
    rstd = jnp.sum(jnp.where(eye, rstd_line, 0.0), axis=1, keepdims=True)
    gamma_cp.wait()
    h_v[...] = ((xf - mean) * rstd * gamma_ref[...]).astype(BF16)

    for cp in wq_cp:
        cp.wait()
    for lo in range(0, q_width + 256, 512):
        hi = min(lo + 512, q_width + 256)
        part = dot(h_v[...], wq_v[:, lo:hi]).astype(BF16)
        for d in range(8):
            qp[d % 2, d // 2, :, lo:hi] = part[16 * d:16 * d + 16]
    qd_cp = remote(qp.at[1 - core], qd, qd_ssem, qd_rsem, row, partner)
    qd_cp.start()

    def pair_copy(n):
        return remote(dsend.at[n], drecv.at[n], d_ssem.at[n], d_rsem.at[n], row, partner)

    def compute_chunk(n, sum_one=None):
        for cp in weight_copies(n):
            cp.wait()
        if sum_one is not None:
            pair_copy(n - 2).wait_recv()
        def products(owner):
            cols = pl.ds(pl.multiple_of(512 * owner, 512), 512)
            return dot(h_v[...], wg_v[n, :, cols]), dot(h_v[...], wu_v[n, :, cols])

        theirs, mine = products(1 - core), products(core)
        for xr in range(2):
            for part in range(2):
                dsend[n, xr, part] = theirs[part][:, 256 * xr:256 * xr + 256].astype(BF16)
                own[n % 3, xr, part] = mine[part][:, 256 * xr:256 * xr + 256]
        started = [] if sum_one is None else sum_one(n - 2)
        pair_copy(n).start()
        for cp in started:
            cp.start()

    def sum_chunk(n):
        keep = own[n % 3, chip] + drecv[n, chip].astype(F32)
        give = (own[n % 3, 1 - chip] + drecv[n, 1 - chip].astype(F32)).astype(BF16)
        return keep, give

    def far_copy(n):
        return remote(xsend.at[n], xrecv.at[n], x_ssem.at[n], x_rsem.at[n], row, far)

    def sum_early(n):
        keep, give = sum_chunk(n)
        xkeep[n] = keep
        xsend[n] = give
        return [far_copy(n)]

    def sum_late(n):
        keep, give = sum_chunk(n)
        keep_out[n - EARLY] = keep.astype(BF16)
        pay_out[n - EARLY] = give
        return late_copies(n - EARLY)

    def late_copies(m):
        return (pltpu.make_async_copy(keep_out.at[m], keep_hbm.at[m], keep_sem.at[m, 0]),
                pltpu.make_async_copy(pay_out.at[m], pay_hbm.at[pl.ds(2 * m, 2)], keep_sem.at[m, 1]))

    compute_chunk(0)

    qd_cp.wait_recv()
    qx[...] = (qp[core].astype(F32) + qd[...].astype(F32)).astype(BF16)
    mine = row * 2 + chip
    q_sends = []
    for s, (dy, dx) in enumerate(((0, 1), (1, 0), (1, 1))):
        ty, xx = (row + dy) % 2, (chip + dx) % 2
        cp = remote(qx.at[ty * 2 + xx], qr.at[s], q_ssem.at[s], q_rsem.at[s], ty, xx * 2 + core)
        cp.start()
        q_sends.append(cp)

    compute_chunk(1)

    def step(sum_one):
        def body(n, carry):
            compute_chunk(n, sum_one)
            return carry
        return body

    def last_sum(n):
        pair_copy(n).wait_recv()
        for cp in sum_late(n):
            cp.start()

    lax.fori_loop(2, EARLY + 2, step(sum_early), 0)
    lax.fori_loop(EARLY + 2, CHUNKS, step(sum_late), 0)
    last_sum(CHUNKS - 2)

    def rotate(vals):
        return vals * cosv + pltpu.roll(vals, 64, 1) * sinv

    for cp in q_sends:
        cp.wait_recv()
    q_same = qx[mine].astype(F32) + qr[0].astype(F32)
    q_diff = qr[1].astype(F32) + qr[2].astype(F32)
    for half, vals in ((row, q_same), (1 - row, q_diff)):
        for head in range(16):
            qscr[half, :, head, :] = rotate(vals[:, 128 * head:128 * head + 128])
    q_out[...] = qscr[...].astype(BF16)
    q_cp = pltpu.make_async_copy(q_out, q_hbm, res_sem.at[0])
    q_cp.start()
    kv_out[0] = rotate(q_same[:, q_width:q_width + 128]).astype(BF16).astype(F32)
    kv_out[1] = q_same[:, q_width + 128:].astype(BF16).astype(F32)
    kv_cp = pltpu.make_async_copy(kv_out, kv_hbm, res_sem.at[1])
    kv_cp.start()
    last_sum(CHUNKS - 1)
    act_cp = []
    for n in range(EARLY):
        far_copy(n).wait_recv()
        full = xkeep[n] + xrecv[n].astype(F32)
        act_out[n] = gated(full[0], full[1])
        cp = pltpu.make_async_copy(act_out.at[n], pay_hbm.at[2 * LATE + n], act_sem.at[n])
        cp.start()
        act_cp.append(cp)
        far_copy(n).wait_send()
    for cp in act_cp + [q_cp, kv_cp]:
        cp.wait()
    for m in range(LATE):
        for cp in late_copies(m):
            cp.wait()
    for cp in st_cp + [qd_cp] + q_sends:
        cp.wait_send()

    def drain(n, carry):
        pair_copy(n).wait_send()
        return carry

    lax.fori_loop(0, CHUNKS, drain, 0)


def project(lens, x_blk, gamma, freqs, w_query, w_key, w_value, w_gate, w_up):
    rows, width = x_blk.shape
    nc = CHUNKS
    q_width = w_query.shape[1] + w_key.shape[1] + w_value.shape[1]
    hbm = pl.BlockSpec(memory_space=pl.ANY)
    return pl.pallas_call(
        project_kernel,
        out_shape=(
            jax.ShapeDtypeStruct((2, 16, 16, 128), BF16),
            jax.ShapeDtypeStruct((2, 16, 128), F32),
            jax.ShapeDtypeStruct((LATE, 2, rows, 256), BF16),
            jax.ShapeDtypeStruct((2 * LATE + EARLY, rows, 256), BF16),
        ),
        in_specs=[hbm] * 9,
        out_specs=(hbm,) * 4,
        scratch_shapes=[
            pltpu.SMEM((128,), jnp.int32), VMEM((1, 128), F32), VMEM((2, 16, 16, 128), BF16), VMEM((2, 16, 128), F32),
            VMEM((LATE, 2, rows, 256), BF16), VMEM((LATE, 2, rows, 256), BF16), VMEM((EARLY, rows, 256), BF16),
            DMA((2,)), DMA((LATE, 2)), DMA((EARLY,)),
            VMEM((rows, width), BF16), VMEM((1, width), F32), DMA((4,)),
            VMEM((width, q_width), BF16), VMEM((nc, width, 1024), BF16), VMEM((nc, width, 1024), BF16),
            VMEM((rows, width), BF16), VMEM((8, rows), F32), VMEM((3, 8, rows), F32),
            VMEM((2, 4, 16, q_width), BF16), VMEM((4, 16, q_width), BF16), VMEM((4, 16, q_width), BF16), VMEM((3, 16, q_width), BF16),
            VMEM((2, 16, 16, 128), F32),
            VMEM((nc, 2, 2, rows, 256), BF16), VMEM((nc, 2, 2, rows, 256), BF16), VMEM((3, 2, 2, rows, 256), F32),
            VMEM((EARLY, 2, rows, 256), F32), VMEM((EARLY, 2, rows, 256), BF16), VMEM((EARLY, 2, rows, 256), BF16),
            DMA((3,)), DMA((nc, 2)), DMA((3,)), DMA((3,)), DMA, DMA, DMA((3,)), DMA((3,)), DMA((nc,)), DMA((nc,)), DMA((EARLY,)), DMA((EARLY,)),
        ],
        compiler_params=pltpu.CompilerParams(collective_id=0, has_side_effects=True, vmem_limit_bytes=VMEM_ALL),
        name="project",
    )(lens, x_blk, gamma, freqs, w_query, w_key, w_value, w_gate, w_up)


SLOTS = 12
AHEAD = 7
BLOCK = 1024


def attend_kernel(lens_h, q_h, kv_h, k_in, v_in, k_out, v_out, att_hbm,
                  kbuf, vbuf, s_scr, in_sem, out_sem, att_out, lens_ref, q_ref, kv_ref, o_scr, small_sem):
    row, col, _, _ = here()
    base = (row * 4 + col) * 16
    count, ctx, _ = k_in.shape

    def in_copies(t):
        slot = lax.rem(t, SLOTS)
        return (pltpu.make_async_copy(k_in.at[t], kbuf.at[slot], in_sem.at[slot, 0]),
                pltpu.make_async_copy(v_in.at[t], vbuf.at[slot], in_sem.at[slot, 1]))

    def out_copies(t):
        slot = lax.rem(t, SLOTS)
        return (pltpu.make_async_copy(kbuf.at[slot], k_out.at[t], out_sem.at[slot, 0]),
                pltpu.make_async_copy(vbuf.at[slot], v_out.at[t], out_sem.at[slot, 1]))

    small = [pltpu.make_async_copy(src, dst, small_sem.at[s]) for s, (src, dst) in enumerate(((lens_h, lens_ref), (q_h, q_ref), (kv_h, kv_ref)))]
    for cp in small:
        cp.start()
    for t in range(min(AHEAD, count)):
        for cp in in_copies(t):
            cp.start()
    for cp in small:
        cp.wait()

    def attend(t, slot, length, blocks):
        q = jnp.concatenate([q_ref[0, t], q_ref[1, t]], axis=0)
        scale = 128.0 ** -0.5
        peak = None
        for b in range(blocks):
            scores = lax.dot_general(q, kbuf[slot, b * BLOCK:(b + 1) * BLOCK, :], (((1,), (1,)), ((), ())),
                                     preferred_element_type=F32) * scale
            if b == blocks - 1:
                pos = lax.broadcasted_iota(jnp.int32, scores.shape, 1) + b * BLOCK
                scores = jnp.where(pos <= length, scores, -1e30)
            s_scr[:, b * BLOCK:(b + 1) * BLOCK] = scores
            for g in range(BLOCK // 128):
                piece = scores[:, g * 128:(g + 1) * 128]
                peak = piece if peak is None else jnp.maximum(peak, piece)
        peak = jnp.max(peak, axis=1, keepdims=True)
        denom = None
        for b in range(blocks):
            e = jnp.exp(s_scr[:, b * BLOCK:(b + 1) * BLOCK] - peak)
            s_scr[:, b * BLOCK:(b + 1) * BLOCK] = e
            for g in range(BLOCK // 128):
                piece = e[:, g * 128:(g + 1) * 128]
                denom = piece if denom is None else denom + piece
        inv = 1.0 / jnp.sum(denom, axis=1, keepdims=True)
        out = None
        for b in range(blocks):
            probs = (s_scr[:, b * BLOCK:(b + 1) * BLOCK] * inv).astype(BF16)
            part = dot(probs, vbuf[slot, b * BLOCK:(b + 1) * BLOCK, :])
            out = part if out is None else out + part
        o_scr[t] = out

    def body(t, carry):
        slot = lax.rem(t, SLOTS)
        for cp in in_copies(t):
            cp.wait()
        length = lens_ref[base + t]
        start = pl.multiple_of((length // 16) * 16, 16)
        at_row = lax.broadcasted_iota(jnp.int32, (16, 128), 0) == length - start
        for which, buf in ((0, kbuf), (1, vbuf)):
            old = buf[slot, pl.ds(start, 16), :].astype(F32)
            new = kv_ref[which, pl.ds(t, 1), :]
            buf[slot, pl.ds(start, 16), :] = jnp.where(at_row, new, old).astype(BF16)
        for cp in out_copies(t):
            cp.start()

        @pl.when(t + AHEAD < count)
        def _():
            @pl.when(t >= SLOTS - AHEAD)
            def _():
                for cp in out_copies(t - (SLOTS - AHEAD)):
                    cp.wait()

            for cp in in_copies(t + AHEAD):
                cp.start()

        blocks = length // BLOCK
        for b in range(ctx // BLOCK):
            @pl.when(blocks == b)
            def _():
                attend(t, slot, length, b + 1)

        return carry

    lax.fori_loop(0, count, body, 0)

    for head in range(32):
        att_out[head // 16, :, 128 * (head % 16):128 * (head % 16) + 128] = o_scr[:, head, :].astype(BF16)
    res = pltpu.make_async_copy(att_out, att_hbm, small_sem.at[3])
    res.start()
    done_in_loop = max(0, count - AHEAD - (SLOTS - AHEAD)) if count > AHEAD else 0
    for t in range(done_in_loop, count):
        for cp in out_copies(t):
            cp.wait()
    res.wait()


def attend(lens, q, kv, k_blk, v_blk):
    hbm = pl.BlockSpec(memory_space=pltpu.HBM)
    count, ctx, dim = k_blk.shape
    return pl.pallas_call(
        attend_kernel,
        out_shape=(
            jax.ShapeDtypeStruct(k_blk.shape, BF16),
            jax.ShapeDtypeStruct(v_blk.shape, BF16),
            jax.ShapeDtypeStruct((2, count, 2048), BF16),
        ),
        in_specs=[hbm] * 5,
        out_specs=(hbm,) * 3,
        scratch_shapes=[
            VMEM((SLOTS, ctx, dim), BF16), VMEM((SLOTS, ctx, dim), BF16),
            VMEM((32, ctx), F32), DMA((SLOTS, 2)), DMA((SLOTS, 2)), VMEM((2, count, 2048), BF16),
            pltpu.SMEM((128,), jnp.int32), VMEM((2, 16, 16, 128), BF16), VMEM((2, 16, 128), F32),
            VMEM((count, 32, dim), F32), DMA((4,)),
        ],
        cost_estimate=pl.CostEstimate(flops=count * 32 * ctx * dim * 4, bytes_accessed=count * ctx * dim * 8, transcendentals=count * 32 * ctx),
        compiler_params=pltpu.CompilerParams(vmem_limit_bytes=VMEM_ALL),
        name="attend",
    )(lens, q, kv, k_blk, v_blk)


GROUPS = ((0, 64), (64, 96), (96, 128))
WIDE = 256 * CHUNKS
EDGES = (0, 256 * EARLY, 256 * (EARLY + 4), WIDE)


def output_kernel(att_h, keep_h, pay_h, got_h, x_h, wo_h, wd_h, y_out,
                  att_ref, keep_v, got_v, x_ref, act_v, in_sem, wo_v, wd_v, attf, acc, ysend, yrecv,
                  wo_sem, wd_sem, a_ssem, a_rsem, f_ssem, f_rsem, g_ssem, g_rsem, h_ssem, h_rsem, c_ssem, c_rsem, y_ssem, y_rsem):
    greet()
    row, col, chip, core = here()
    partner = col + 1 - 2 * core
    far = (col + 2) % 4
    order = (2 * core + chip, 2 * (1 - core) + chip, 2 * core + 1 - chip, 2 * (1 - core) + 1 - chip)
    rs = pl.ds(0, 2 * LATE)
    moves = [(att_h, att_ref), (keep_h, keep_v), (got_h.at[rs], got_v), (x_h, x_ref)]
    for s, src in ((0, pay_h), (2, got_h)):
        for n in range(EARLY):
            moves.append((src.at[2 * LATE + n], act_v.at[:, pl.ds(WIDE * s + 256 * n, 256)]))
    in_cp = [pltpu.make_async_copy(src, dst, in_sem.at[s]) for s, (src, dst) in enumerate(moves)]
    for cp in in_cp:
        cp.start()
    wd_cp = []
    for s, owner in enumerate(order):
        wd_cp.append(pltpu.make_async_copy(wd_h.at[:, owner], wd_v.at[s], wd_sem.at[s]))
    wo_cp = pltpu.make_async_copy(wo_h, wo_v, wo_sem)

    in_cp[0].wait()
    greeted()
    mine = row * 2 + chip
    around = ((0, 1), (1, 0), (1, 1))
    a_cp = []
    for s, (dy, dx) in enumerate(around):
        ty, xx = (row + dy) % 2, (chip + dx) % 2
        cp = remote(att_ref.at[ty], attf.at[mine, core], a_ssem.at[s], a_rsem.at[s], ty, xx * 2 + core)
        cp.start()
        a_cp.append(cp)
    attf[mine, core] = att_ref[row]
    f_own = remote(attf.at[mine, core], attf.at[mine, core], f_ssem.at[3], f_rsem.at[3], row, partner)
    f_own.start()

    def piece(s, r, p):
        lo, hi = GROUPS[r]
        return act_v.at[pl.ds(lo, hi - lo), pl.ds(WIDE * s + EDGES[p], EDGES[p + 1] - EDGES[p])]

    in_cp[1].wait()
    in_cp[2].wait()
    for cp in (wd_cp[0], wd_cp[1], wo_cp, wd_cp[2], wd_cp[3]):
        cp.start()
    g_cp, h_cp = {}, {}
    for r, (lo, hi) in enumerate(GROUPS):
        rows = slice(lo, hi)
        for p in (1, 2):
            for n in range(EDGES[p] // 256 - EARLY, EDGES[p + 1] // 256 - EARLY):
                g = keep_v[n, 0, rows].astype(F32) + got_v[2 * n, rows].astype(F32)
                u = keep_v[n, 1, rows].astype(F32) + got_v[2 * n + 1, rows].astype(F32)
                at = 256 * (EARLY + n)
                act_v[rows, at:at + 256] = gated(g, u)
            g_cp[r, p] = remote(piece(0, r, p), piece(2, r, p), g_ssem.at[r, p - 1], g_rsem.at[r, p - 1], row, far)
            g_cp[r, p].start()
            h_cp[r, p] = remote(piece(2, r, p), piece(3, r, p), h_ssem.at[r, p - 1], h_rsem.at[r, p - 1], row, partner)
    for cp in in_cp[4:]:
        cp.wait()
    every = pl.ds(0, 128)
    first = pl.ds(2 * WIDE, EDGES[1])
    c_cp = [remote(act_v.at[every, pl.ds(0, WIDE)], act_v.at[every, pl.ds(WIDE, WIDE)], c_ssem.at[0], c_rsem.at[0], row, partner),
            remote(act_v.at[every, first], act_v.at[every, pl.ds(3 * WIDE, EDGES[1])], c_ssem.at[1], c_rsem.at[1], row, partner)]
    for cp in c_cp:
        cp.start()

    def down(rows, s, k0, k1):
        return dot(act_v[rows, WIDE * s + k0:WIDE * s + k1], wd_v[s, k0 // 256:k1 // 256].reshape(k1 - k0, -1))

    f_cp = []
    for s, (dy, dx) in enumerate(around):
        a_cp[s].wait_recv()
        index = ((row + dy) % 2) * 2 + (chip + dx) % 2
        cp = remote(attf.at[index, core], attf.at[index, core], f_ssem.at[s], f_rsem.at[s], row, partner)
        cp.start()
        f_cp.append(cp)
    for cp in c_cp:
        cp.wait_recv()
    wd_cp[0].wait()
    wd_cp[1].wait()
    acc[...] = down(slice(0, 128), 0, 0, WIDE) + down(slice(0, 128), 1, 0, WIDE)
    wo_cp.wait()
    for cp in f_cp + [f_own]:
        cp.wait_recv()
    acc[...] += dot(attf[...].reshape(128, 2048), wo_v[...])
    wd_cp[2].wait()
    wd_cp[3].wait()
    y_cp = {}

    def finish(r, p):
        lo, hi = GROUPS[r]
        rows, window = slice(lo, hi), pl.ds(lo, hi - lo)
        k0, k1 = (0, EDGES[2]) if p == 1 else (EDGES[2], WIDE)
        h_cp[r, p].wait_recv()
        part = acc[rows] + (down(rows, 2, k0, k1) + down(rows, 3, k0, k1))
        if p == 1:
            acc[rows] = part
        else:
            ysend[rows] = part.astype(BF16)
            y_cp[r] = remote(ysend.at[window], yrecv.at[window], y_ssem.at[r], y_rsem.at[r], 1 - row, col)
            y_cp[r].start()

    last = None
    for r in range(len(GROUPS)):
        for p in (1, 2):
            g_cp[r, p].wait_recv()
            h_cp[r, p].start()
            if last is not None:
                finish(*last)
            last = (r, p)
    finish(*last)
    in_cp[3].wait()
    for r, (lo, hi) in enumerate(GROUPS):
        rows = slice(lo, hi)
        y_cp[r].wait_recv()
        both = ysend[rows].astype(F32) + yrecv[rows].astype(F32)
        y_out[rows] = (x_ref[rows].astype(F32) + both).astype(BF16)
    for cp in a_cp + c_cp + f_cp + [f_own] + list(g_cp.values()) + list(h_cp.values()) + list(y_cp.values()):
        cp.wait_send()


def output(att, keep, pay, got, x_blk, w_out, w_down):
    rows, width = x_blk.shape
    hbm = pl.BlockSpec(memory_space=pl.ANY)
    groups = len(GROUPS)
    return pl.pallas_call(
        output_kernel,
        out_shape=pltpu.VMEM((rows, width), BF16),
        in_specs=[hbm] * 7,
        out_specs=pl.BlockSpec(memory_space=VMEM),
        scratch_shapes=[
            VMEM((2, 16, 2048), BF16), VMEM((LATE, 2, rows, 256), BF16), VMEM((2 * LATE, rows, 256), BF16),
            VMEM((rows, width), BF16), VMEM((rows, 4 * WIDE), BF16), DMA((4 + 2 * EARLY,)),
            VMEM((2048, width), BF16), VMEM((4, CHUNKS, 256, width), BF16), VMEM((4, 2, 16, 2048), BF16),
            VMEM((rows, width), F32), VMEM((rows, width), BF16), VMEM((rows, width), BF16),
            DMA, DMA((4,)), DMA((3,)), DMA((3,)), DMA((4,)), DMA((4,)), DMA((groups, 2)), DMA((groups, 2)), DMA((groups, 2)), DMA((groups, 2)),
            DMA((2,)), DMA((2,)), DMA((groups,)), DMA((groups,)),
        ],
        compiler_params=pltpu.CompilerParams(collective_id=1, has_side_effects=True, vmem_limit_bytes=48 * 2 ** 20),
        name="output",
    )(*[pltpu.with_memory_space_constraint(v, pltpu.HBM) for v in (att, keep, pay, got, x_blk, w_out, w_down.reshape(CHUNKS, 4, 256, width))])


def solution(mesh):
    cache_spec = P(("dp", "ty", "tx"), None, None)
    across = [(0, 2), (1, 3), (2, 0), (3, 1)]

    def layer_shard(x_blk, lens, k_blk, v_blk, gamma, w_query, w_key, w_value, w_gate, w_up, w_out, w_down):
        freqs = np.tile(np.float32(ROPE_BASE ** (-np.arange(0, 128, 2) / 128.0)), 2)[None, :]
        q, kv, keep, pay = project(lens, x_blk, gamma[None, :], freqs, w_query, w_key, w_value, w_gate, w_up)
        got = lax.ppermute(pay, "tx", across)
        k_out, v_out, att = attend(lens, q, kv, k_blk, v_blk)
        y = output(att, keep, pay, got, x_blk, w_out, w_down)
        return y, k_out, v_out

    in_specs = (P("dp", "tx"), P("dp"), cache_spec, cache_spec, P("tx"), P("tx", "ty"), P("tx", None), P("tx", None), P("tx", "ty"), P("tx", "ty"), P("ty", "tx"), P("ty", "tx"))
    out_specs = (P("dp", "tx"), cache_spec, cache_spec)
    return jax.shard_map(layer_shard, mesh=mesh, in_specs=in_specs, out_specs=out_specs, check_vma=False)
```

```python
import functools

import jax
import jax.numpy as jnp
import numpy as np
from jax import lax
from jax.experimental import pallas as pl
from jax.experimental.pallas import tpu as pltpu
from jax.sharding import PartitionSpec as P

EPSILON = 1e-6
ROPE_BASE = 10000.0
BF16 = jnp.bfloat16
F32 = jnp.float32
MESH = pl.DeviceIdType.MESH

VMEM = pltpu.VMEM
VMEM_ALL = 67043328
DMA = pltpu.SemaphoreType.DMA


def here():
    row = lax.axis_index("ty")
    col = lax.axis_index("tx")
    return row, col, col // 2, col % 2


def greet():
    row, col, _, _ = here()
    me = row * 4 + col
    barrier = pltpu.get_barrier_semaphore()
    for step in range(1, 8):
        peer = (me + step) % 8
        pl.semaphore_signal(barrier, inc=1, device_id={"ty": peer // 4, "tx": peer % 4}, device_id_type=MESH)


def greeted():
    pl.semaphore_wait(pltpu.get_barrier_semaphore(), 7)


def remote(src, dst, send_sem, recv_sem, ty, tx):
    return pltpu.make_async_remote_copy(
        src_ref=src, dst_ref=dst, send_sem=send_sem, recv_sem=recv_sem,
        device_id={"ty": ty, "tx": tx}, device_id_type=MESH)


def keep_in(space, *arrays):
    return [pltpu.with_memory_space_constraint(v, space) for v in arrays]


def dot(a, b):
    return jnp.dot(a, b, preferred_element_type=F32)


CHUNKS = 8
READY = 5
EARLY = 2
LATE = CHUNKS - EARLY


def gated(g, u):
    return (jax.nn.silu(g.astype(BF16).astype(F32)) * u.astype(BF16).astype(F32)).astype(BF16)


def project_kernel(lens_h, x_h, gamma_h, freq_h, wq_h, wk_h, wv_h, wg_h, wu_h, k_h, v_h,
                   q_out, kv_out, keep_out, pay_out, pre_out,
                   lens_ref, freq_ref, pre_sem, x_ref, gamma_ref, x_sem, wq_v, wg_v, wu_v, h_v, st_send, st_recv,
                   qp, qd, qx, qr, qscr, dsend, drecv, own, xkeep, xsend, xrecv,
                   wq_sem, w_sem, st_ssem, st_rsem, qd_ssem, qd_rsem, q_ssem, q_rsem,
                   d_ssem, d_rsem, x_ssem, x_rsem):
    row, col, chip, core = here()
    partner = col + 1 - 2 * core
    far = (col + 2) % 4
    me = row * 4 + col
    greet()

    x_cp = pltpu.make_async_copy(x_h, x_ref, x_sem.at[0])
    gamma_cp = pltpu.make_async_copy(gamma_h, gamma_ref, x_sem.at[1])
    lens_cp = pltpu.make_async_copy(lens_h, lens_ref, x_sem.at[2])
    freq_cp = pltpu.make_async_copy(freq_h, freq_ref, x_sem.at[3])
    for cp in (x_cp, gamma_cp, lens_cp, freq_cp):
        cp.start()
    q_width = wq_h.shape[1]
    wq_cp = [pltpu.make_async_copy(wq_h, wq_v.at[:, pl.ds(0, q_width)], wq_sem.at[0]),
             pltpu.make_async_copy(wk_h, wq_v.at[:, pl.ds(q_width, 128)], wq_sem.at[1]),
             pltpu.make_async_copy(wv_h, wq_v.at[:, pl.ds(q_width + 128, 128)], wq_sem.at[2])]
    for cp in wq_cp:
        cp.start()

    def weight_copies(n):
        cols = pl.ds(pl.multiple_of(1024 * n, 1024), 1024)
        return (pltpu.make_async_copy(wg_h.at[:, cols], wg_v.at[n], w_sem.at[n, 0]),
                pltpu.make_async_copy(wu_h.at[:, cols], wu_v.at[n], w_sem.at[n, 1]))

    def start_weights(n, carry):
        for cp in weight_copies(n):
            cp.start()
        return carry

    lax.fori_loop(0, CHUNKS, start_weights, 0)

    x_cp.wait()
    xf = x_ref[...].astype(F32)
    sum1 = jnp.sum(xf, axis=1, keepdims=True)
    sum2 = jnp.sum(xf * xf, axis=1, keepdims=True)
    rows = xf.shape[0]
    eye = lax.broadcasted_iota(jnp.int32, (rows, rows), 0) == lax.broadcasted_iota(jnp.int32, (rows, rows), 1)
    line1 = jnp.sum(jnp.where(eye, sum1, 0.0), axis=0, keepdims=True)
    line2 = jnp.sum(jnp.where(eye, sum2, 0.0), axis=0, keepdims=True)
    first = lax.broadcasted_iota(jnp.int32, (8, rows), 0) == 0
    st_send[...] = jnp.where(first, line1, line2)
    greeted()
    st_cp = [remote(st_send, st_recv.at[d - 1], st_ssem.at[d - 1], st_rsem.at[d - 1], row, (col + d) % 4) for d in (1, 2, 3)]
    for cp in st_cp:
        cp.start()
    lens_cp.wait()
    freq_cp.wait()
    seq = lax.broadcasted_iota(jnp.int32, (16, 128), 0)
    place = jnp.zeros((16, 128), F32)
    for b in range(16):
        place = jnp.where(seq == b, lens_ref[me * 16 + b].astype(F32), place)
    angle = place * freq_ref[...]
    cosv = jnp.cos(angle)
    sinv = jnp.where(lax.broadcasted_iota(jnp.int32, (16, 128), 1) < 64, -jnp.sin(angle), jnp.sin(angle))
    for cp in st_cp:
        cp.wait_recv()
    total = st_send[...] + st_recv[0] + st_recv[1] + st_recv[2]
    width = 4.0 * xf.shape[1]
    mean_line = total[0:1] / width
    var_line = total[1:2] / width - mean_line * mean_line
    rstd_line = lax.rsqrt(var_line + EPSILON)
    mean = jnp.sum(jnp.where(eye, mean_line, 0.0), axis=1, keepdims=True)
    rstd = jnp.sum(jnp.where(eye, rstd_line, 0.0), axis=1, keepdims=True)
    gamma_cp.wait()
    h_v[...] = ((xf - mean) * rstd * gamma_ref[...]).astype(BF16)

    for cp in wq_cp:
        cp.wait()
    for lo in range(0, q_width + 256, 512):
        hi = min(lo + 512, q_width + 256)
        part = dot(h_v[...], wq_v[:, lo:hi]).astype(BF16)
        for d in range(8):
            qp[d % 2, d // 2, :, lo:hi] = part[16 * d:16 * d + 16]
    qd_cp = remote(qp.at[1 - core], qd, qd_ssem, qd_rsem, row, partner)
    qd_cp.start()

    def pair_copy(n):
        return remote(dsend.at[n], drecv.at[n], d_ssem.at[n], d_rsem.at[n], row, partner)

    def compute_chunk(n, sum_one=None):
        for cp in weight_copies(n):
            cp.wait()
        if sum_one is not None:
            pair_copy(n - 2).wait_recv()
        def products(owner):
            cols = pl.ds(pl.multiple_of(512 * owner, 512), 512)
            return dot(h_v[...], wg_v[n, :, cols]), dot(h_v[...], wu_v[n, :, cols])

        theirs, mine = products(1 - core), products(core)
        for xr in range(2):
            for part in range(2):
                dsend[n, xr, part] = theirs[part][:, 256 * xr:256 * xr + 256].astype(BF16)
                own[n % 3, xr, part] = mine[part][:, 256 * xr:256 * xr + 256]
        started = [] if sum_one is None else sum_one(n - 2)
        pair_copy(n).start()
        for cp in started:
            cp.start()

    def sum_chunk(n):
        keep = own[n % 3, chip] + drecv[n, chip].astype(F32)
        give = (own[n % 3, 1 - chip] + drecv[n, 1 - chip].astype(F32)).astype(BF16)
        return keep, give

    def far_copy(n):
        return remote(xsend.at[n], xrecv.at[n], x_ssem.at[n], x_rsem.at[n], row, far)

    def sum_early(n):
        keep, give = sum_chunk(n)
        xkeep[n] = keep
        xsend[n] = give
        return [far_copy(n)]

    def sum_late(n):
        keep, give = sum_chunk(n)
        keep_out[n - EARLY] = keep.astype(BF16)
        pay_out[2 * (n - EARLY)] = give[0]
        pay_out[2 * (n - EARLY) + 1] = give[1]
        return []

    compute_chunk(0)

    qd_cp.wait_recv()
    qx[...] = (qp[core].astype(F32) + qd[...].astype(F32)).astype(BF16)
    mine = row * 2 + chip
    q_sends = []
    for s, (dy, dx) in enumerate(((0, 1), (1, 0), (1, 1))):
        ty, xx = (row + dy) % 2, (chip + dx) % 2
        cp = remote(qx.at[ty * 2 + xx], qr.at[s], q_ssem.at[s], q_rsem.at[s], ty, xx * 2 + core)
        cp.start()
        q_sends.append(cp)

    compute_chunk(1)

    def step(sum_one):
        def body(n, carry):
            compute_chunk(n, sum_one)
            return carry
        return body

    def last_sum(n):
        pair_copy(n).wait_recv()
        sum_late(n)

    lax.fori_loop(2, EARLY + 2, step(sum_early), 0)
    lax.fori_loop(EARLY + 2, CHUNKS - 1, step(sum_late), 0)
    pre_cp = []
    for t in range(READY):
        for part, src in enumerate((k_h, v_h)):
            pre_cp.append(pltpu.make_async_copy(src.at[t], pre_out.at[part, t], pre_sem.at[part, t]))
    for cp in pre_cp:
        cp.start()
    lax.fori_loop(CHUNKS - 1, CHUNKS, step(sum_late), 0)
    last_sum(CHUNKS - 2)

    def rotate(vals):
        return vals * cosv + pltpu.roll(vals, 64, 1) * sinv

    for cp in q_sends:
        cp.wait_recv()
    q_same = qx[mine].astype(F32) + qr[0].astype(F32)
    q_diff = qr[1].astype(F32) + qr[2].astype(F32)
    for half, vals in ((row, q_same), (1 - row, q_diff)):
        for head in range(16):
            qscr[half, :, head, :] = rotate(vals[:, 128 * head:128 * head + 128])
    q_out[...] = qscr[...].astype(BF16)
    kv_out[0] = rotate(q_same[:, q_width:q_width + 128]).astype(BF16).astype(F32)
    kv_out[1] = q_same[:, q_width + 128:].astype(BF16).astype(F32)
    last_sum(CHUNKS - 1)
    for n in range(EARLY):
        far_copy(n).wait_recv()
        full = xkeep[n] + xrecv[n].astype(F32)
        pay_out[2 * LATE + n] = gated(full[0], full[1])
        far_copy(n).wait_send()
    for cp in pre_cp:
        cp.wait()
    for cp in st_cp + [qd_cp] + q_sends:
        cp.wait_send()

    def drain(n, carry):
        pair_copy(n).wait_send()
        return carry

    lax.fori_loop(0, CHUNKS, drain, 0)


def project(lens, x_blk, gamma, freqs, w_query, w_key, w_value, w_gate, w_up, k_blk, v_blk):
    rows, width = x_blk.shape
    nc = CHUNKS
    q_width = w_query.shape[1] + w_key.shape[1] + w_value.shape[1]
    hbm = pl.BlockSpec(memory_space=pl.ANY)
    return pl.pallas_call(
        project_kernel,
        out_shape=(
            VMEM((2, 16, 16, 128), BF16),
            VMEM((2, 16, 128), F32),
            VMEM((LATE, 2, rows, 256), BF16),
            VMEM((2 * LATE + EARLY, rows, 256), BF16),
            VMEM((2, READY, *k_blk.shape[1:]), BF16),
        ),
        in_specs=[hbm] * 11,
        out_specs=(pl.BlockSpec(memory_space=VMEM),) * 5,
        scratch_shapes=[
            pltpu.SMEM((128,), jnp.int32), VMEM((1, 128), F32), DMA((2, READY)),
            VMEM((rows, width), BF16), VMEM((1, width), F32), DMA((4,)),
            VMEM((width, q_width), BF16), VMEM((nc, width, 1024), BF16), VMEM((nc, width, 1024), BF16),
            VMEM((rows, width), BF16), VMEM((8, rows), F32), VMEM((3, 8, rows), F32),
            VMEM((2, 4, 16, q_width), BF16), VMEM((4, 16, q_width), BF16), VMEM((4, 16, q_width), BF16), VMEM((3, 16, q_width), BF16),
            VMEM((2, 16, 16, 128), F32),
            VMEM((nc, 2, 2, rows, 256), BF16), VMEM((nc, 2, 2, rows, 256), BF16), VMEM((3, 2, 2, rows, 256), F32),
            VMEM((EARLY, 2, rows, 256), F32), VMEM((EARLY, 2, rows, 256), BF16), VMEM((EARLY, 2, rows, 256), BF16),
            DMA((3,)), DMA((nc, 2)), DMA((3,)), DMA((3,)), DMA, DMA, DMA((3,)), DMA((3,)), DMA((nc,)), DMA((nc,)), DMA((EARLY,)), DMA((EARLY,)),
        ],
        compiler_params=pltpu.CompilerParams(collective_id=0, has_side_effects=True, vmem_limit_bytes=47 * 2 ** 20),
        name="project",
    )(*keep_in(pltpu.HBM, lens, x_blk, gamma, freqs, w_query, w_key, w_value, w_gate, w_up, k_blk, v_blk))


SLOTS = 12
AHEAD = 7
BLOCK = 1024


def attend_kernel(lens_h, q_ref, kv_ref, pre_ref, k_in, v_in, k_out, v_out, att_out,
                  kbuf, vbuf, s_scr, in_sem, out_sem, lens_ref, o_scr, small_sem):
    row, col, _, _ = here()
    base = (row * 4 + col) * 16
    count, ctx, _ = k_in.shape

    def in_copies(t):
        slot = lax.rem(t, SLOTS)
        return (pltpu.make_async_copy(k_in.at[t], kbuf.at[slot], in_sem.at[slot, 0]),
                pltpu.make_async_copy(v_in.at[t], vbuf.at[slot], in_sem.at[slot, 1]))

    def out_copies(t):
        slot = lax.rem(t, SLOTS)
        return (pltpu.make_async_copy(kbuf.at[slot], k_out.at[t], out_sem.at[slot, 0]),
                pltpu.make_async_copy(vbuf.at[slot], v_out.at[t], out_sem.at[slot, 1]))

    lens_cp = pltpu.make_async_copy(lens_h, lens_ref, small_sem)
    lens_cp.start()
    for t in range(READY, AHEAD):
        for cp in in_copies(t):
            cp.start()
    lens_cp.wait()

    def take(t, slot):
        def move(b, carry):
            rows = pl.ds(pl.multiple_of(b * 512, 512), 512)
            kbuf[slot, rows] = pre_ref[0, t, rows]
            vbuf[slot, rows] = pre_ref[1, t, rows]
            return carry

        lax.fori_loop(0, ctx // 512, move, 0)

    def attend(t, slot, length, blocks):
        q = jnp.concatenate([q_ref[0, t], q_ref[1, t]], axis=0)
        scale = 128.0 ** -0.5
        peak = None
        for b in range(blocks):
            scores = lax.dot_general(q, kbuf[slot, b * BLOCK:(b + 1) * BLOCK, :], (((1,), (1,)), ((), ())),
                                     preferred_element_type=F32) * scale
            if b == blocks - 1:
                pos = lax.broadcasted_iota(jnp.int32, scores.shape, 1) + b * BLOCK
                scores = jnp.where(pos <= length, scores, -1e30)
            s_scr[:, b * BLOCK:(b + 1) * BLOCK] = scores
            for g in range(BLOCK // 128):
                piece = scores[:, g * 128:(g + 1) * 128]
                peak = piece if peak is None else jnp.maximum(peak, piece)
        peak = jnp.max(peak, axis=1, keepdims=True)
        denom = None
        for b in range(blocks):
            e = jnp.exp(s_scr[:, b * BLOCK:(b + 1) * BLOCK] - peak)
            s_scr[:, b * BLOCK:(b + 1) * BLOCK] = e
            for g in range(BLOCK // 128):
                piece = e[:, g * 128:(g + 1) * 128]
                denom = piece if denom is None else denom + piece
        inv = 1.0 / jnp.sum(denom, axis=1, keepdims=True)
        out = None
        for b in range(blocks):
            probs = (s_scr[:, b * BLOCK:(b + 1) * BLOCK] * inv).astype(BF16)
            part = dot(probs, vbuf[slot, b * BLOCK:(b + 1) * BLOCK, :])
            out = part if out is None else out + part
        o_scr[t] = out

    def body(t, carry):
        slot = lax.rem(t, SLOTS)
        @pl.when(t < READY)
        def _():
            take(t, slot)

        @pl.when(t >= READY)
        def _():
            for cp in in_copies(t):
                cp.wait()

        length = lens_ref[base + t]
        start = pl.multiple_of((length // 16) * 16, 16)
        at_row = lax.broadcasted_iota(jnp.int32, (16, 128), 0) == length - start
        for which, buf in ((0, kbuf), (1, vbuf)):
            old = buf[slot, pl.ds(start, 16), :].astype(F32)
            new = kv_ref[which, pl.ds(t, 1), :]
            buf[slot, pl.ds(start, 16), :] = jnp.where(at_row, new, old).astype(BF16)
        for cp in out_copies(t):
            cp.start()

        @pl.when(t + AHEAD < count)
        def _():
            @pl.when(t >= SLOTS - AHEAD)
            def _():
                for cp in out_copies(t - (SLOTS - AHEAD)):
                    cp.wait()

            for cp in in_copies(t + AHEAD):
                cp.start()

        blocks = length // BLOCK
        for b in range(ctx // BLOCK):
            @pl.when(blocks == b)
            def _():
                attend(t, slot, length, b + 1)

        return carry

    lax.fori_loop(0, count, body, 0)

    for head in range(32):
        att_out[head // 16, :, 128 * (head % 16):128 * (head % 16) + 128] = o_scr[:, head, :].astype(BF16)
    done_in_loop = max(0, count - AHEAD - (SLOTS - AHEAD)) if count > AHEAD else 0
    for t in range(done_in_loop, count):
        for cp in out_copies(t):
            cp.wait()


def attend(lens, q, kv, pre, k_blk, v_blk):
    hbm = pl.BlockSpec(memory_space=pltpu.HBM)
    vm = pl.BlockSpec(memory_space=VMEM)
    count, ctx, dim = k_blk.shape
    return pl.pallas_call(
        attend_kernel,
        out_shape=(
            jax.ShapeDtypeStruct(k_blk.shape, BF16),
            jax.ShapeDtypeStruct(v_blk.shape, BF16),
            VMEM((2, count, 2048), BF16),
        ),
        in_specs=[hbm, vm, vm, vm, hbm, hbm],
        out_specs=(hbm, hbm, vm),
        scratch_shapes=[
            VMEM((SLOTS, ctx, dim), BF16), VMEM((SLOTS, ctx, dim), BF16),
            VMEM((32, ctx), F32), DMA((SLOTS, 2)), DMA((SLOTS, 2)),
            pltpu.SMEM((128,), jnp.int32), VMEM((count, 32, dim), F32), DMA,
        ],
        cost_estimate=pl.CostEstimate(flops=count * 32 * ctx * dim * 4, bytes_accessed=count * ctx * dim * 8, transcendentals=count * 32 * ctx),
        compiler_params=pltpu.CompilerParams(vmem_limit_bytes=30 * 2 ** 20),
        name="attend",
    )(*keep_in(pltpu.HBM, lens), *keep_in(VMEM, q, kv, pre), *keep_in(pltpu.HBM, k_blk, v_blk))


WIDE = 256 * CHUNKS
EDGE = 256 * (EARLY + 4)
ITEMS = ((0, 64, False), (0, 64, True), (64, 96, False), (64, 96, True), (96, 128, False), (96, 128, True))


def output_kernel(att_ref, keep_v, pay_v, got_v, x_h, wo_h, wd_h, y_out,
                  x_ref, act_v, in_sem, wo_v, wd_v, attf, acc, ysend, yrecv,
                  wo_sem, wd_sem, a_ssem, a_rsem, f_ssem, f_rsem, g_ssem, g_rsem, h_ssem, h_rsem, c_ssem, c_rsem, y_ssem, y_rsem):
    greet()
    row, col, chip, core = here()
    partner = col + 1 - 2 * core
    far = (col + 2) % 4
    order = (2 * core + chip, 2 * (1 - core) + chip, 2 * core + 1 - chip, 2 * (1 - core) + 1 - chip)
    x_cp = pltpu.make_async_copy(x_h, x_ref, in_sem)
    x_cp.start()
    wd_cp = []
    for s, owner in enumerate(order):
        wd_cp.append(pltpu.make_async_copy(wd_h.at[:, owner], wd_v.at[s], wd_sem.at[s]))
    wo_cp = pltpu.make_async_copy(wo_h, wo_v, wo_sem)

    for cp in (wd_cp[0], wd_cp[1], wo_cp, wd_cp[2], wd_cp[3]):
        cp.start()
    greeted()
    mine = row * 2 + chip
    around = ((0, 1), (1, 0), (1, 1))
    a_cp = []
    for s, (dy, dx) in enumerate(around):
        ty, xx = (row + dy) % 2, (chip + dx) % 2
        cp = remote(att_ref.at[ty], attf.at[mine, core], a_ssem.at[s], a_rsem.at[s], ty, xx * 2 + core)
        cp.start()
        a_cp.append(cp)
    attf[mine, core] = att_ref[row]
    f_own = remote(attf.at[mine, core], attf.at[mine, core], f_ssem.at[3], f_rsem.at[3], row, partner)
    f_own.start()

    def piece(s, item):
        lo, hi, last = ITEMS[item]
        c0, c1 = (EDGE, WIDE) if last else (256 * EARLY, EDGE)
        return act_v.at[pl.ds(lo, hi - lo), pl.ds(WIDE * s + c0, c1 - c0)]

    g_cp, h_cp = [], []
    for item, (lo, hi, last) in enumerate(ITEMS):
        rows = slice(lo, hi)
        for n in range(4, LATE) if last else range(4):
            g = keep_v[n, 0, rows].astype(F32) + got_v[2 * n, rows].astype(F32)
            u = keep_v[n, 1, rows].astype(F32) + got_v[2 * n + 1, rows].astype(F32)
            at = 256 * (EARLY + n)
            act_v[rows, at:at + 256] = gated(g, u)
        g_cp.append(remote(piece(0, item), piece(2, item), g_ssem.at[item], g_rsem.at[item], row, far))
        g_cp[item].start()
        h_cp.append(remote(piece(2, item), piece(3, item), h_ssem.at[item], h_rsem.at[item], row, partner))
    for s, src in ((0, pay_v), (2, got_v)):
        for n in range(EARLY):
            act_v[:, WIDE * s + 256 * n:WIDE * s + 256 * n + 256] = src[2 * LATE + n]
    every = pl.ds(0, 128)
    first = pl.ds(2 * WIDE, 256 * EARLY)
    c_cp = [remote(act_v.at[every, pl.ds(0, WIDE)], act_v.at[every, pl.ds(WIDE, WIDE)], c_ssem.at[0], c_rsem.at[0], row, partner),
            remote(act_v.at[every, first], act_v.at[every, pl.ds(3 * WIDE, 256 * EARLY)], c_ssem.at[1], c_rsem.at[1], row, partner)]
    for cp in c_cp:
        cp.start()

    def down(rows, s, k0, k1):
        return dot(act_v[rows, WIDE * s + k0:WIDE * s + k1], wd_v[s, k0 // 256:k1 // 256].reshape(k1 - k0, -1))

    for cp in c_cp:
        cp.wait_recv()
    wd_cp[0].wait()
    wd_cp[1].wait()
    acc[...] = down(slice(0, 128), 0, 0, WIDE) + down(slice(0, 128), 1, 0, WIDE)
    f_cp = []
    for s, (dy, dx) in enumerate(around):
        a_cp[s].wait_recv()
        index = ((row + dy) % 2) * 2 + (chip + dx) % 2
        cp = remote(attf.at[index, core], attf.at[index, core], f_ssem.at[s], f_rsem.at[s], row, partner)
        cp.start()
        f_cp.append(cp)
    def attention_part():
        wo_cp.wait()
        for cp in f_cp + [f_own]:
            cp.wait_recv()
        acc[...] += dot(attf[...].reshape(128, 2048), wo_v[...])
        wd_cp[2].wait()
        wd_cp[3].wait()

    y_cp = []

    def finish(item):
        lo, hi, last = ITEMS[item]
        rows, window = slice(lo, hi), pl.ds(lo, hi - lo)
        k0, k1 = (EDGE, WIDE) if last else (0, EDGE)
        h_cp[item].wait_recv()
        part = acc[rows] + (down(rows, 2, k0, k1) + down(rows, 3, k0, k1))
        if last:
            ysend[rows] = part.astype(BF16)
            cp = remote(ysend.at[window], yrecv.at[window], y_ssem.at[item], y_rsem.at[item], 1 - row, col)
            cp.start()
            y_cp.append((rows, cp))
        else:
            acc[rows] = part

    for item in range(len(ITEMS)):
        g_cp[item].wait_recv()
        h_cp[item].start()
        if item:
            finish(item - 1)
        else:
            attention_part()
    finish(len(ITEMS) - 1)
    x_cp.wait()
    for rows, cp in y_cp:
        cp.wait_recv()
        both = ysend[rows].astype(F32) + yrecv[rows].astype(F32)
        y_out[rows] = (x_ref[rows].astype(F32) + both).astype(BF16)
    for cp in a_cp + c_cp + f_cp + [f_own] + g_cp + h_cp + [cp for _, cp in y_cp]:
        cp.wait_send()


def output(att, keep, pay, got, x_blk, w_out, w_down):
    rows, width = x_blk.shape
    hbm = pl.BlockSpec(memory_space=pl.ANY)
    vm = pl.BlockSpec(memory_space=VMEM)
    items = len(ITEMS)
    return pl.pallas_call(
        output_kernel,
        out_shape=pltpu.VMEM((rows, width), BF16),
        in_specs=[vm] * 4 + [hbm] * 3,
        out_specs=vm,
        scratch_shapes=[
            VMEM((rows, width), BF16), VMEM((rows, 4 * WIDE), BF16), DMA,
            VMEM((2048, width), BF16), VMEM((4, CHUNKS, 256, width), BF16), VMEM((4, 2, 16, 2048), BF16),
            VMEM((rows, width), F32), VMEM((rows, width), BF16), VMEM((rows, width), BF16),
            DMA, DMA((4,)), DMA((3,)), DMA((3,)), DMA((4,)), DMA((4,)), DMA((items,)), DMA((items,)), DMA((items,)), DMA((items,)),
            DMA((2,)), DMA((2,)), DMA((items,)), DMA((items,)),
        ],
        compiler_params=pltpu.CompilerParams(collective_id=1, has_side_effects=True, vmem_limit_bytes=32 * 2 ** 20),
        name="output",
    )(*keep_in(VMEM, att, keep, pay, got), *keep_in(pltpu.HBM, x_blk, w_out, w_down.reshape(CHUNKS, 4, 256, width)))


def solution(mesh):
    cache_spec = P(("dp", "ty", "tx"), None, None)
    across = [(0, 2), (1, 3), (2, 0), (3, 1)]

    def layer_shard(x_blk, lens, k_blk, v_blk, gamma, w_query, w_key, w_value, w_gate, w_up, w_out, w_down):
        freqs = np.tile(np.float32(ROPE_BASE ** (-np.arange(0, 128, 2) / 128.0)), 2)[None, :]
        q, kv, keep, pay, pre = project(lens, x_blk, gamma[None, :], freqs, w_query, w_key, w_value, w_gate, w_up, k_blk, v_blk)
        got = lax.ppermute(pay, "tx", across)
        k_out, v_out, att = attend(lens, q, kv, pre, k_blk, v_blk)
        y = output(att, keep, pay, got, x_blk, w_out, w_down)
        return y, k_out, v_out

    in_specs = (P("dp", "tx"), P("dp"), cache_spec, cache_spec, P("tx"), P("tx", "ty"), P("tx", None), P("tx", None), P("tx", "ty"), P("tx", "ty"), P("ty", "tx"), P("ty", "tx"))
    out_specs = (P("dp", "tx"), cache_spec, cache_spec)
    return jax.shard_map(layer_shard, mesh=mesh, in_specs=in_specs, out_specs=out_specs, check_vma=False)
```

```python
import functools

import jax
import jax.numpy as jnp
import numpy as np
from jax import lax
from jax.experimental import pallas as pl
from jax.experimental.pallas import tpu as pltpu
from jax.sharding import PartitionSpec as P

EPSILON = 1e-6
ROPE_BASE = 10000.0
BF16 = jnp.bfloat16
F32 = jnp.float32
MESH = pl.DeviceIdType.MESH

VMEM = pltpu.VMEM
VMEM_ALL = 67043328
DMA = pltpu.SemaphoreType.DMA


def here():
    row = lax.axis_index("ty")
    col = lax.axis_index("tx")
    return row, col, col // 2, col % 2


def greet(offsets):
    row, _, chip, core = here()
    barrier = pltpu.get_barrier_semaphore()
    for dy, dx, dc in offsets:
        peer = {"ty": (row + dy) % 2, "tx": ((chip + dx) % 2) * 2 + (core + dc) % 2}
        pl.semaphore_signal(barrier, inc=1, device_id=peer, device_id_type=MESH)


def greeted(offsets):
    pl.semaphore_wait(pltpu.get_barrier_semaphore(), len(offsets))


MET_EARLY = ((0, 0, 1), (0, 1, 0), (0, 1, 1), (1, 0, 0), (1, 1, 0))
MET_LATE = ((0, 0, 1), (0, 1, 0), (1, 0, 0), (1, 1, 0))


def remote(src, dst, send_sem, recv_sem, ty, tx):
    return pltpu.make_async_remote_copy(
        src_ref=src, dst_ref=dst, send_sem=send_sem, recv_sem=recv_sem,
        device_id={"ty": ty, "tx": tx}, device_id_type=MESH)


def keep_in(space, *arrays):
    return [pltpu.with_memory_space_constraint(v, space) for v in arrays]


def dot(a, b):
    return jnp.dot(a, b, preferred_element_type=F32)


CHUNKS = 8
READY = 5
EARLY = 2
LATE = CHUNKS - EARLY


def gated(g, u):
    return (jax.nn.silu(g.astype(BF16).astype(F32)) * u.astype(BF16).astype(F32)).astype(BF16)


def project_kernel(lens_h, x_h, gamma_h, freq_h, wq_h, wk_h, wv_h, wg_h, wu_h, k_h, v_h,
                   q_out, kv_out, keep_out, pay_out, pre_out,
                   lens_ref, freq_ref, pre_sem, x_ref, gamma_ref, x_sem, wq_v, wg_v, wu_v, h_v, st_send, st_recv,
                   qp, qd, qx, qr, qscr, dsend, drecv, own, xkeep, xsend, xrecv,
                   wq_sem, w_sem, st_ssem, st_rsem, qd_ssem, qd_rsem, q_ssem, q_rsem,
                   d_ssem, d_rsem, x_ssem, x_rsem):
    row, col, chip, core = here()
    partner = col + 1 - 2 * core
    far = (col + 2) % 4
    me = row * 4 + col
    greet(MET_EARLY)

    x_cp = pltpu.make_async_copy(x_h, x_ref, x_sem.at[0])
    gamma_cp = pltpu.make_async_copy(gamma_h, gamma_ref, x_sem.at[1])
    lens_cp = pltpu.make_async_copy(lens_h, lens_ref, x_sem.at[2])
    freq_cp = pltpu.make_async_copy(freq_h, freq_ref, x_sem.at[3])
    for cp in (x_cp, gamma_cp, lens_cp, freq_cp):
        cp.start()
    q_width = wq_h.shape[1]
    wq_cp = [pltpu.make_async_copy(wq_h, wq_v.at[:, pl.ds(0, q_width)], wq_sem.at[0]),
             pltpu.make_async_copy(wk_h, wq_v.at[:, pl.ds(q_width, 128)], wq_sem.at[1]),
             pltpu.make_async_copy(wv_h, wq_v.at[:, pl.ds(q_width + 128, 128)], wq_sem.at[2])]
    for cp in wq_cp:
        cp.start()

    def weight_copies(n):
        cols = pl.ds(pl.multiple_of(1024 * n, 1024), 1024)
        return (pltpu.make_async_copy(wg_h.at[:, cols], wg_v.at[n], w_sem.at[n, 0]),
                pltpu.make_async_copy(wu_h.at[:, cols], wu_v.at[n], w_sem.at[n, 1]))

    def start_weights(n, carry):
        for cp in weight_copies(n):
            cp.start()
        return carry

    lax.fori_loop(0, CHUNKS, start_weights, 0)

    x_cp.wait()
    xf = x_ref[...].astype(F32)
    sum1 = jnp.sum(xf, axis=1, keepdims=True)
    sum2 = jnp.sum(xf * xf, axis=1, keepdims=True)
    rows = xf.shape[0]
    eye = lax.broadcasted_iota(jnp.int32, (rows, rows), 0) == lax.broadcasted_iota(jnp.int32, (rows, rows), 1)
    line1 = jnp.sum(jnp.where(eye, sum1, 0.0), axis=0, keepdims=True)
    line2 = jnp.sum(jnp.where(eye, sum2, 0.0), axis=0, keepdims=True)
    first = lax.broadcasted_iota(jnp.int32, (8, rows), 0) == 0
    st_send[...] = jnp.where(first, line1, line2)
    greeted(MET_EARLY)
    st_cp = [remote(st_send, st_recv.at[d - 1], st_ssem.at[d - 1], st_rsem.at[d - 1], row, (col + d) % 4) for d in (1, 2, 3)]
    for cp in st_cp:
        cp.start()
    lens_cp.wait()
    freq_cp.wait()
    seq = lax.broadcasted_iota(jnp.int32, (16, 128), 0)
    place = jnp.zeros((16, 128), F32)
    for b in range(16):
        place = jnp.where(seq == b, lens_ref[me * 16 + b].astype(F32), place)
    angle = place * freq_ref[...]
    cosv = jnp.cos(angle)
    sinv = jnp.where(lax.broadcasted_iota(jnp.int32, (16, 128), 1) < 64, -jnp.sin(angle), jnp.sin(angle))
    for cp in st_cp:
        cp.wait_recv()
    total = st_send[...] + st_recv[0] + st_recv[1] + st_recv[2]
    width = 4.0 * xf.shape[1]
    mean_line = total[0:1] / width
    var_line = total[1:2] / width - mean_line * mean_line
    rstd_line = lax.rsqrt(var_line + EPSILON)
    mean = jnp.sum(jnp.where(eye, mean_line, 0.0), axis=1, keepdims=True)
    rstd = jnp.sum(jnp.where(eye, rstd_line, 0.0), axis=1, keepdims=True)
    gamma_cp.wait()
    h_v[...] = ((xf - mean) * rstd * gamma_ref[...]).astype(BF16)

    for cp in wq_cp:
        cp.wait()
    q_parts = ((0, 1024), (1024, q_width + 256))
    qd_cp = []
    for k, (lo, hi) in enumerate(q_parts):
        part = dot(h_v[...], wq_v[:, lo:hi]).astype(BF16)
        for d in range(8):
            qp[d % 2, d // 2, :, lo:hi] = part[16 * d:16 * d + 16]
        cols = pl.ds(lo, hi - lo)
        qd_cp.append(remote(qp.at[1 - core, :, :, cols], qd.at[:, :, cols], qd_ssem.at[k], qd_rsem.at[k], row, partner))
        qd_cp[k].start()

    def pair_copy(n):
        return remote(dsend.at[n], drecv.at[n], d_ssem.at[n], d_rsem.at[n], row, partner)

    def compute_chunk(n, sum_one=None):
        for cp in weight_copies(n):
            cp.wait()
        if sum_one is not None:
            pair_copy(n - 2).wait_recv()
        def products(owner):
            cols = pl.ds(pl.multiple_of(512 * owner, 512), 512)
            return dot(h_v[...], wg_v[n, :, cols]), dot(h_v[...], wu_v[n, :, cols])

        theirs, mine = products(1 - core), products(core)
        for xr in range(2):
            for part in range(2):
                dsend[n, xr, part] = theirs[part][:, 256 * xr:256 * xr + 256].astype(BF16)
                own[n % 3, xr, part] = mine[part][:, 256 * xr:256 * xr + 256]
        started = [] if sum_one is None else sum_one(n - 2)
        pair_copy(n).start()
        for cp in started:
            cp.start()

    def sum_chunk(n):
        keep = own[n % 3, chip] + drecv[n, chip].astype(F32)
        give = (own[n % 3, 1 - chip] + drecv[n, 1 - chip].astype(F32)).astype(BF16)
        return keep, give

    def far_copy(n):
        return remote(xsend.at[n], xrecv.at[n], x_ssem.at[n], x_rsem.at[n], row, far)

    def sum_early(n):
        keep, give = sum_chunk(n)
        xkeep[n] = keep
        xsend[n] = give
        return [far_copy(n)]

    def sum_late(n):
        keep, give = sum_chunk(n)
        keep_out[n - EARLY] = keep.astype(BF16)
        pay_out[2 * (n - EARLY)] = give[0]
        pay_out[2 * (n - EARLY) + 1] = give[1]
        return []

    compute_chunk(0)

    mine = row * 2 + chip
    q_sends = []
    for k, (lo, hi) in enumerate(q_parts):
        qd_cp[k].wait_recv()
        qx[:, :, lo:hi] = (qp[core, :, :, lo:hi].astype(F32) + qd[:, :, lo:hi].astype(F32)).astype(BF16)
        for s, (dy, dx) in enumerate(((0, 1), (1, 0), (1, 1))):
            ty, xx = (row + dy) % 2, (chip + dx) % 2
            cols = pl.ds(lo, min(hi, q_width) - lo if dy else hi - lo)
            cp = remote(qx.at[ty * 2 + xx, :, cols], qr.at[s, :, cols], q_ssem.at[k, s], q_rsem.at[k, s], ty, xx * 2 + core)
            cp.start()
            q_sends.append(cp)

    compute_chunk(1)

    def step(sum_one):
        def body(n, carry):
            compute_chunk(n, sum_one)
            return carry
        return body

    def last_sum(n):
        pair_copy(n).wait_recv()
        sum_late(n)

    lax.fori_loop(2, EARLY + 2, step(sum_early), 0)
    lax.fori_loop(EARLY + 2, CHUNKS - 1, step(sum_late), 0)
    pre_cp = []
    for t in range(READY):
        for part, src in enumerate((k_h, v_h)):
            pre_cp.append(pltpu.make_async_copy(src.at[t], pre_out.at[part, t], pre_sem.at[part, t]))
    for cp in pre_cp:
        cp.start()
    lax.fori_loop(CHUNKS - 1, CHUNKS, step(sum_late), 0)
    last_sum(CHUNKS - 2)

    def rotate(vals):
        return vals * cosv + pltpu.roll(vals, 64, 1) * sinv

    for cp in q_sends:
        cp.wait_recv()
    q_same = qx[mine].astype(F32) + qr[0].astype(F32)
    q_diff = qr[1, :, 0:q_width].astype(F32) + qr[2, :, 0:q_width].astype(F32)
    for half, vals in ((row, q_same), (1 - row, q_diff)):
        for head in range(16):
            qscr[half, :, head, :] = rotate(vals[:, 128 * head:128 * head + 128])
    q_out[...] = qscr[...].astype(BF16)
    kv_out[0] = rotate(q_same[:, q_width:q_width + 128]).astype(BF16).astype(F32)
    kv_out[1] = q_same[:, q_width + 128:].astype(BF16).astype(F32)
    last_sum(CHUNKS - 1)
    for n in range(EARLY):
        far_copy(n).wait_recv()
        full = xkeep[n] + xrecv[n].astype(F32)
        pay_out[2 * LATE + n] = gated(full[0], full[1])
        far_copy(n).wait_send()
    for cp in pre_cp:
        cp.wait()
    for cp in st_cp + qd_cp + q_sends:
        cp.wait_send()

    def drain(n, carry):
        pair_copy(n).wait_send()
        return carry

    lax.fori_loop(0, CHUNKS, drain, 0)


def project(lens, x_blk, gamma, freqs, w_query, w_key, w_value, w_gate, w_up, k_blk, v_blk):
    rows, width = x_blk.shape
    nc = CHUNKS
    q_width = w_query.shape[1] + w_key.shape[1] + w_value.shape[1]
    hbm = pl.BlockSpec(memory_space=pl.ANY)
    return pl.pallas_call(
        project_kernel,
        out_shape=(
            VMEM((2, 16, 16, 128), BF16),
            VMEM((2, 16, 128), F32),
            VMEM((LATE, 2, rows, 256), BF16),
            VMEM((2 * LATE + EARLY, rows, 256), BF16),
            VMEM((2, READY, *k_blk.shape[1:]), BF16),
        ),
        in_specs=[hbm] * 11,
        out_specs=(pl.BlockSpec(memory_space=VMEM),) * 5,
        scratch_shapes=[
            pltpu.SMEM((128,), jnp.int32), VMEM((1, 128), F32), DMA((2, READY)),
            VMEM((rows, width), BF16), VMEM((1, width), F32), DMA((4,)),
            VMEM((width, q_width), BF16), VMEM((nc, width, 1024), BF16), VMEM((nc, width, 1024), BF16),
            VMEM((rows, width), BF16), VMEM((8, rows), F32), VMEM((3, 8, rows), F32),
            VMEM((2, 4, 16, q_width), BF16), VMEM((4, 16, q_width), BF16), VMEM((4, 16, q_width), BF16), VMEM((3, 16, q_width), BF16),
            VMEM((2, 16, 16, 128), F32),
            VMEM((nc, 2, 2, rows, 256), BF16), VMEM((nc, 2, 2, rows, 256), BF16), VMEM((3, 2, 2, rows, 256), F32),
            VMEM((EARLY, 2, rows, 256), F32), VMEM((EARLY, 2, rows, 256), BF16), VMEM((EARLY, 2, rows, 256), BF16),
            DMA((3,)), DMA((nc, 2)), DMA((3,)), DMA((3,)), DMA((2,)), DMA((2,)), DMA((2, 3)), DMA((2, 3)), DMA((nc,)), DMA((nc,)), DMA((EARLY,)), DMA((EARLY,)),
        ],
        compiler_params=pltpu.CompilerParams(collective_id=0, has_side_effects=True, vmem_limit_bytes=47 * 2 ** 20),
        name="project",
    )(*keep_in(pltpu.HBM, lens, x_blk, gamma, freqs, w_query, w_key, w_value, w_gate, w_up, k_blk, v_blk))


SLOTS = 12
AHEAD = 7
BLOCK = 1024


def attend_kernel(lens_h, q_ref, kv_ref, pre_ref, k_in, v_in, k_out, v_out, att_out,
                  kbuf, vbuf, s_scr, in_sem, out_sem, lens_ref, o_scr, small_sem):
    row, col, _, _ = here()
    base = (row * 4 + col) * 16
    count, ctx, _ = k_in.shape

    def in_copies(t):
        slot = lax.rem(t, SLOTS)
        return (pltpu.make_async_copy(k_in.at[t], kbuf.at[slot], in_sem.at[slot, 0]),
                pltpu.make_async_copy(v_in.at[t], vbuf.at[slot], in_sem.at[slot, 1]))

    def out_copies(t):
        slot = lax.rem(t, SLOTS)
        return (pltpu.make_async_copy(kbuf.at[slot], k_out.at[t], out_sem.at[slot, 0]),
                pltpu.make_async_copy(vbuf.at[slot], v_out.at[t], out_sem.at[slot, 1]))

    lens_cp = pltpu.make_async_copy(lens_h, lens_ref, small_sem)
    lens_cp.start()
    for t in range(READY, AHEAD):
        for cp in in_copies(t):
            cp.start()
    lens_cp.wait()

    def take(t, slot):
        def move(b, carry):
            rows = pl.ds(pl.multiple_of(b * 512, 512), 512)
            kbuf[slot, rows] = pre_ref[0, t, rows]
            vbuf[slot, rows] = pre_ref[1, t, rows]
            return carry

        lax.fori_loop(0, ctx // 512, move, 0)

    def attend(t, slot, length, blocks):
        q = jnp.concatenate([q_ref[0, t], q_ref[1, t]], axis=0)
        scale = 128.0 ** -0.5
        peak = None
        for b in range(blocks):
            scores = lax.dot_general(q, kbuf[slot, b * BLOCK:(b + 1) * BLOCK, :], (((1,), (1,)), ((), ())),
                                     preferred_element_type=F32) * scale
            if b == blocks - 1:
                pos = lax.broadcasted_iota(jnp.int32, scores.shape, 1) + b * BLOCK
                scores = jnp.where(pos <= length, scores, -1e30)
            s_scr[:, b * BLOCK:(b + 1) * BLOCK] = scores
            for g in range(BLOCK // 128):
                piece = scores[:, g * 128:(g + 1) * 128]
                peak = piece if peak is None else jnp.maximum(peak, piece)
        peak = jnp.max(peak, axis=1, keepdims=True)
        denom = None
        for b in range(blocks):
            e = jnp.exp(s_scr[:, b * BLOCK:(b + 1) * BLOCK] - peak)
            s_scr[:, b * BLOCK:(b + 1) * BLOCK] = e
            for g in range(BLOCK // 128):
                piece = e[:, g * 128:(g + 1) * 128]
                denom = piece if denom is None else denom + piece
        inv = 1.0 / jnp.sum(denom, axis=1, keepdims=True)
        out = None
        for b in range(blocks):
            probs = (s_scr[:, b * BLOCK:(b + 1) * BLOCK] * inv).astype(BF16)
            part = dot(probs, vbuf[slot, b * BLOCK:(b + 1) * BLOCK, :])
            out = part if out is None else out + part
        o_scr[t] = out

    def body(t, carry):
        slot = lax.rem(t, SLOTS)
        @pl.when(t < READY)
        def _():
            take(t, slot)

        @pl.when(t >= READY)
        def _():
            for cp in in_copies(t):
                cp.wait()

        length = lens_ref[base + t]
        start = pl.multiple_of((length // 16) * 16, 16)
        at_row = lax.broadcasted_iota(jnp.int32, (16, 128), 0) == length - start
        for which, buf in ((0, kbuf), (1, vbuf)):
            old = buf[slot, pl.ds(start, 16), :].astype(F32)
            new = kv_ref[which, pl.ds(t, 1), :]
            buf[slot, pl.ds(start, 16), :] = jnp.where(at_row, new, old).astype(BF16)
        for cp in out_copies(t):
            cp.start()

        @pl.when(t + AHEAD < count)
        def _():
            @pl.when(t >= SLOTS - AHEAD)
            def _():
                for cp in out_copies(t - (SLOTS - AHEAD)):
                    cp.wait()

            for cp in in_copies(t + AHEAD):
                cp.start()

        blocks = length // BLOCK
        for b in range(ctx // BLOCK):
            @pl.when(blocks == b)
            def _():
                attend(t, slot, length, b + 1)

        return carry

    lax.fori_loop(0, count, body, 0)

    for head in range(32):
        att_out[head // 16, :, 128 * (head % 16):128 * (head % 16) + 128] = o_scr[:, head, :].astype(BF16)
    done_in_loop = max(0, count - AHEAD - (SLOTS - AHEAD)) if count > AHEAD else 0
    for t in range(done_in_loop, count):
        for cp in out_copies(t):
            cp.wait()


def attend(lens, q, kv, pre, k_blk, v_blk):
    hbm = pl.BlockSpec(memory_space=pltpu.HBM)
    vm = pl.BlockSpec(memory_space=VMEM)
    count, ctx, dim = k_blk.shape
    return pl.pallas_call(
        attend_kernel,
        out_shape=(
            jax.ShapeDtypeStruct(k_blk.shape, BF16),
            jax.ShapeDtypeStruct(v_blk.shape, BF16),
            VMEM((2, count, 2048), BF16),
        ),
        in_specs=[hbm, vm, vm, vm, hbm, hbm],
        out_specs=(hbm, hbm, vm),
        scratch_shapes=[
            VMEM((SLOTS, ctx, dim), BF16), VMEM((SLOTS, ctx, dim), BF16),
            VMEM((32, ctx), F32), DMA((SLOTS, 2)), DMA((SLOTS, 2)),
            pltpu.SMEM((128,), jnp.int32), VMEM((count, 32, dim), F32), DMA,
        ],
        cost_estimate=pl.CostEstimate(flops=count * 32 * ctx * dim * 4, bytes_accessed=count * ctx * dim * 8, transcendentals=count * 32 * ctx),
        compiler_params=pltpu.CompilerParams(vmem_limit_bytes=30 * 2 ** 20),
        name="attend",
    )(*keep_in(pltpu.HBM, lens), *keep_in(VMEM, q, kv, pre), *keep_in(pltpu.HBM, k_blk, v_blk))


WIDE = 256 * CHUNKS
EDGE = 256 * (EARLY + 3)
ITEMS = tuple((32 * r, 32 * r + 32, last) for r in range(4) for last in (False, True))


def output_kernel(att_ref, keep_v, pay_v, got_v, x_h, wo_h, wd_h, y_out,
                  x_ref, act_v, in_sem, wo_v, wd_v, attf, acc, ysend, yrecv,
                  wo_sem, wd_sem, a_ssem, a_rsem, f_ssem, f_rsem, g_ssem, g_rsem, h_ssem, h_rsem, c_ssem, c_rsem, y_ssem, y_rsem):
    greet(MET_LATE)
    row, col, chip, core = here()
    partner = col + 1 - 2 * core
    far = (col + 2) % 4
    order = (2 * core + chip, 2 * (1 - core) + chip, 2 * core + 1 - chip, 2 * (1 - core) + 1 - chip)
    x_cp = pltpu.make_async_copy(x_h, x_ref, in_sem)
    x_cp.start()
    wd_cp = []
    for s, owner in enumerate(order):
        wd_cp.append(pltpu.make_async_copy(wd_h.at[:, owner], wd_v.at[s], wd_sem.at[s]))
    wo_cp = pltpu.make_async_copy(wo_h, wo_v, wo_sem)

    for cp in (wd_cp[0], wd_cp[1], wo_cp, wd_cp[2], wd_cp[3]):
        cp.start()
    greeted(MET_LATE)
    mine = row * 2 + chip
    around = ((0, 1), (1, 0), (1, 1))
    a_cp = []
    for s, (dy, dx) in enumerate(around):
        ty, xx = (row + dy) % 2, (chip + dx) % 2
        cp = remote(att_ref.at[ty], attf.at[mine, core], a_ssem.at[s], a_rsem.at[s], ty, xx * 2 + core)
        cp.start()
        a_cp.append(cp)
    attf[mine, core] = att_ref[row]
    f_own = remote(attf.at[mine, core], attf.at[mine, core], f_ssem.at[3], f_rsem.at[3], row, partner)
    f_own.start()

    def piece(s, item):
        lo, hi, last = ITEMS[item]
        c0, c1 = (EDGE, WIDE) if last else (256 * EARLY, EDGE)
        return act_v.at[pl.ds(lo, hi - lo), pl.ds(WIDE * s + c0, c1 - c0)]

    g_cp, h_cp = [], []
    for item, (lo, hi, last) in enumerate(ITEMS):
        rows = slice(lo, hi)
        for n in range(3, LATE) if last else range(3):
            g = keep_v[n, 0, rows].astype(F32) + got_v[2 * n, rows].astype(F32)
            u = keep_v[n, 1, rows].astype(F32) + got_v[2 * n + 1, rows].astype(F32)
            at = 256 * (EARLY + n)
            act_v[rows, at:at + 256] = gated(g, u)
        g_cp.append(remote(piece(0, item), piece(2, item), g_ssem.at[item], g_rsem.at[item], row, far))
        g_cp[item].start()
        h_cp.append(remote(piece(2, item), piece(3, item), h_ssem.at[item], h_rsem.at[item], row, partner))
    for s, src in ((0, pay_v), (2, got_v)):
        for n in range(EARLY):
            act_v[:, WIDE * s + 256 * n:WIDE * s + 256 * n + 256] = src[2 * LATE + n]
    every = pl.ds(0, 128)
    first = pl.ds(2 * WIDE, 256 * EARLY)
    c_cp = [remote(act_v.at[every, pl.ds(0, WIDE)], act_v.at[every, pl.ds(WIDE, WIDE)], c_ssem.at[0], c_rsem.at[0], row, partner),
            remote(act_v.at[every, first], act_v.at[every, pl.ds(3 * WIDE, 256 * EARLY)], c_ssem.at[1], c_rsem.at[1], row, partner)]
    for cp in c_cp:
        cp.start()

    def down(rows, s, k0, k1):
        return dot(act_v[rows, WIDE * s + k0:WIDE * s + k1], wd_v[s, k0 // 256:k1 // 256].reshape(k1 - k0, -1))

    for cp in c_cp:
        cp.wait_recv()
    wd_cp[0].wait()
    wd_cp[1].wait()
    acc[...] = down(slice(0, 128), 0, 0, WIDE) + down(slice(0, 128), 1, 0, WIDE)
    f_cp = []
    for s, (dy, dx) in enumerate(around):
        a_cp[s].wait_recv()
        index = ((row + dy) % 2) * 2 + (chip + dx) % 2
        cp = remote(attf.at[index, core], attf.at[index, core], f_ssem.at[s], f_rsem.at[s], row, partner)
        cp.start()
        f_cp.append(cp)
    def attention_part():
        wo_cp.wait()
        for cp in f_cp + [f_own]:
            cp.wait_recv()
        wd_cp[2].wait()
        wd_cp[3].wait()
        every_row = slice(0, 128)
        early = down(every_row, 2, 0, 256 * EARLY) + down(every_row, 3, 0, 256 * EARLY)
        acc[...] += dot(attf[...].reshape(128, 2048), wo_v[...]) + early

    y_cp = []

    def finish(item):
        lo, hi, last = ITEMS[item]
        rows, window = slice(lo, hi), pl.ds(lo, hi - lo)
        k0, k1 = (EDGE, WIDE) if last else (256 * EARLY, EDGE)
        h_cp[item].wait_recv()
        part = acc[rows] + (down(rows, 2, k0, k1) + down(rows, 3, k0, k1))
        if last:
            ysend[rows] = part.astype(BF16)
            cp = remote(ysend.at[window], yrecv.at[window], y_ssem.at[item], y_rsem.at[item], 1 - row, col)
            cp.start()
            y_cp.append((rows, cp))
        else:
            acc[rows] = part

    for item in range(len(ITEMS)):
        g_cp[item].wait_recv()
        h_cp[item].start()
        if item:
            finish(item - 1)
        else:
            attention_part()
    finish(len(ITEMS) - 1)
    x_cp.wait()
    for rows, cp in y_cp:
        cp.wait_recv()
        both = ysend[rows].astype(F32) + yrecv[rows].astype(F32)
        y_out[rows] = (x_ref[rows].astype(F32) + both).astype(BF16)
    for cp in a_cp + c_cp + f_cp + [f_own] + g_cp + h_cp + [cp for _, cp in y_cp]:
        cp.wait_send()


def output(att, keep, pay, got, x_blk, w_out, w_down):
    rows, width = x_blk.shape
    hbm = pl.BlockSpec(memory_space=pl.ANY)
    vm = pl.BlockSpec(memory_space=VMEM)
    items = len(ITEMS)
    return pl.pallas_call(
        output_kernel,
        out_shape=pltpu.VMEM((rows, width), BF16),
        in_specs=[vm] * 4 + [hbm] * 3,
        out_specs=vm,
        scratch_shapes=[
            VMEM((rows, width), BF16), VMEM((rows, 4 * WIDE), BF16), DMA,
            VMEM((2048, width), BF16), VMEM((4, CHUNKS, 256, width), BF16), VMEM((4, 2, 16, 2048), BF16),
            VMEM((rows, width), F32), VMEM((rows, width), BF16), VMEM((rows, width), BF16),
            DMA, DMA((4,)), DMA((3,)), DMA((3,)), DMA((4,)), DMA((4,)), DMA((items,)), DMA((items,)), DMA((items,)), DMA((items,)),
            DMA((2,)), DMA((2,)), DMA((items,)), DMA((items,)),
        ],
        compiler_params=pltpu.CompilerParams(collective_id=1, has_side_effects=True, vmem_limit_bytes=32 * 2 ** 20),
        name="output",
    )(*keep_in(VMEM, att, keep, pay, got), *keep_in(pltpu.HBM, x_blk, w_out, w_down.reshape(CHUNKS, 4, 256, width)))


def solution(mesh):
    cache_spec = P(("dp", "ty", "tx"), None, None)
    across = [(0, 2), (1, 3), (2, 0), (3, 1)]

    def layer_shard(x_blk, lens, k_blk, v_blk, gamma, w_query, w_key, w_value, w_gate, w_up, w_out, w_down):
        freqs = np.tile(np.float32(ROPE_BASE ** (-np.arange(0, 128, 2) / 128.0)), 2)[None, :]
        q, kv, keep, pay, pre = project(lens, x_blk, gamma[None, :], freqs, w_query, w_key, w_value, w_gate, w_up, k_blk, v_blk)
        got = lax.ppermute(pay, "tx", across)
        k_out, v_out, att = attend(lens, q, kv, pre, k_blk, v_blk)
        y = output(att, keep, pay, got, x_blk, w_out, w_down)
        return y, k_out, v_out

    in_specs = (P("dp", "tx"), P("dp"), cache_spec, cache_spec, P("tx"), P("tx", "ty"), P("tx", None), P("tx", None), P("tx", "ty"), P("tx", "ty"), P("ty", "tx"), P("ty", "tx"))
    out_specs = (P("dp", "tx"), cache_spec, cache_spec)
    return jax.shard_map(layer_shard, mesh=mesh, in_specs=in_specs, out_specs=out_specs, check_vma=False)
```

```python
import functools

import jax
import jax.numpy as jnp
import numpy as np
from jax import lax
from jax.experimental import pallas as pl
from jax.experimental.pallas import tpu as pltpu
from jax.sharding import PartitionSpec as P

EPSILON = 1e-6
ROPE_BASE = 10000.0
BF16 = jnp.bfloat16
F32 = jnp.float32
MESH = pl.DeviceIdType.MESH

VMEM = pltpu.VMEM
VMEM_ALL = 67043328
DMA = pltpu.SemaphoreType.DMA


def here():
    row = lax.axis_index("ty")
    col = lax.axis_index("tx")
    return row, col, col // 2, col % 2


def greet(offsets):
    row, _, chip, core = here()
    barrier = pltpu.get_barrier_semaphore()
    for dy, dx, dc in offsets:
        peer = {"ty": (row + dy) % 2, "tx": ((chip + dx) % 2) * 2 + (core + dc) % 2}
        pl.semaphore_signal(barrier, inc=1, device_id=peer, device_id_type=MESH)


def greeted(offsets):
    pl.semaphore_wait(pltpu.get_barrier_semaphore(), len(offsets))


MET_EARLY = ((0, 0, 1), (0, 1, 0), (0, 1, 1), (1, 0, 0), (1, 1, 0))
MET_LATE = ((0, 0, 1), (0, 1, 0), (1, 0, 0), (1, 1, 0))


def remote(src, dst, send_sem, recv_sem, ty, tx):
    return pltpu.make_async_remote_copy(
        src_ref=src, dst_ref=dst, send_sem=send_sem, recv_sem=recv_sem,
        device_id={"ty": ty, "tx": tx}, device_id_type=MESH)


def keep_in(space, *arrays):
    return [pltpu.with_memory_space_constraint(v, space) for v in arrays]


def dot(a, b):
    return jnp.dot(a, b, preferred_element_type=F32)


CHUNKS = 8
READY = 5
EARLY = 2
LATE = CHUNKS - EARLY


def gated(g, u):
    return (jax.nn.silu(g.astype(BF16).astype(F32)) * u.astype(BF16).astype(F32)).astype(BF16)


def project_kernel(lens_h, x_h, gamma_h, freq_h, wq_h, wk_h, wv_h, wg_h, wu_h, k_h, v_h,
                   q_out, kv_out, keep_out, pay_out, pre_out,
                   lens_ref, freq_ref, pre_sem, x_ref, gamma_ref, x_sem, wq_v, wg_v, wu_v, h_v, st_send, st_recv,
                   qp, qd, qx, qr, qscr, dsend, drecv, own, xkeep, xsend, xrecv,
                   wq_sem, w_sem, st_ssem, st_rsem, qd_ssem, qd_rsem, q_ssem, q_rsem,
                   d_ssem, d_rsem, x_ssem, x_rsem):
    row, col, chip, core = here()
    partner = col + 1 - 2 * core
    far = (col + 2) % 4
    me = row * 4 + col
    greet(MET_EARLY)

    x_cp = pltpu.make_async_copy(x_h, x_ref, x_sem.at[0])
    gamma_cp = pltpu.make_async_copy(gamma_h, gamma_ref, x_sem.at[1])
    lens_cp = pltpu.make_async_copy(lens_h, lens_ref, x_sem.at[2])
    freq_cp = pltpu.make_async_copy(freq_h, freq_ref, x_sem.at[3])
    for cp in (x_cp, gamma_cp, lens_cp, freq_cp):
        cp.start()
    q_width = wq_h.shape[1]
    wq_cp = [pltpu.make_async_copy(wq_h, wq_v.at[:, pl.ds(0, q_width)], wq_sem.at[0]),
             pltpu.make_async_copy(wk_h, wq_v.at[:, pl.ds(q_width, 128)], wq_sem.at[1]),
             pltpu.make_async_copy(wv_h, wq_v.at[:, pl.ds(q_width + 128, 128)], wq_sem.at[2])]
    for cp in wq_cp:
        cp.start()

    def weight_copies(n):
        cols = pl.ds(pl.multiple_of(1024 * n, 1024), 1024)
        return (pltpu.make_async_copy(wg_h.at[:, cols], wg_v.at[n], w_sem.at[n, 0]),
                pltpu.make_async_copy(wu_h.at[:, cols], wu_v.at[n], w_sem.at[n, 1]))

    def start_weights(n, carry):
        for cp in weight_copies(n):
            cp.start()
        return carry

    lax.fori_loop(0, CHUNKS, start_weights, 0)

    x_cp.wait()
    xf = x_ref[...].astype(F32)
    sum1 = jnp.sum(xf, axis=1, keepdims=True)
    sum2 = jnp.sum(xf * xf, axis=1, keepdims=True)
    rows = xf.shape[0]
    eye = lax.broadcasted_iota(jnp.int32, (rows, rows), 0) == lax.broadcasted_iota(jnp.int32, (rows, rows), 1)
    line1 = jnp.sum(jnp.where(eye, sum1, 0.0), axis=0, keepdims=True)
    line2 = jnp.sum(jnp.where(eye, sum2, 0.0), axis=0, keepdims=True)
    first = lax.broadcasted_iota(jnp.int32, (8, rows), 0) == 0
    st_send[...] = jnp.where(first, line1, line2)
    greeted(MET_EARLY)
    st_cp = [remote(st_send, st_recv.at[d - 1], st_ssem.at[d - 1], st_rsem.at[d - 1], row, (col + d) % 4) for d in (1, 2, 3)]
    for cp in st_cp:
        cp.start()
    lens_cp.wait()
    freq_cp.wait()
    seq = lax.broadcasted_iota(jnp.int32, (16, 128), 0)
    place = jnp.zeros((16, 128), F32)
    for b in range(16):
        place = jnp.where(seq == b, lens_ref[me * 16 + b].astype(F32), place)
    angle = place * freq_ref[...]
    cosv = jnp.cos(angle)
    sinv = jnp.where(lax.broadcasted_iota(jnp.int32, (16, 128), 1) < 64, -jnp.sin(angle), jnp.sin(angle))
    for cp in st_cp:
        cp.wait_recv()
    total = st_send[...] + st_recv[0] + st_recv[1] + st_recv[2]
    width = 4.0 * xf.shape[1]
    mean_line = total[0:1] / width
    var_line = total[1:2] / width - mean_line * mean_line
    rstd_line = lax.rsqrt(var_line + EPSILON)
    mean = jnp.sum(jnp.where(eye, mean_line, 0.0), axis=1, keepdims=True)
    rstd = jnp.sum(jnp.where(eye, rstd_line, 0.0), axis=1, keepdims=True)
    gamma_cp.wait()
    h_v[...] = ((xf - mean) * rstd * gamma_ref[...]).astype(BF16)

    for cp in wq_cp:
        cp.wait()
    q_parts = ((0, 1024), (1024, q_width + 256))
    qd_cp = []
    for k, (lo, hi) in enumerate(q_parts):
        part = dot(h_v[...], wq_v[:, lo:hi]).astype(BF16)
        for d in range(8):
            qp[d % 2, d // 2, :, lo:hi] = part[16 * d:16 * d + 16]
        cols = pl.ds(lo, hi - lo)
        qd_cp.append(remote(qp.at[1 - core, :, :, cols], qd.at[:, :, cols], qd_ssem.at[k], qd_rsem.at[k], row, partner))
        qd_cp[k].start()

    def pair_copy(n):
        return remote(dsend.at[n], drecv.at[n], d_ssem.at[n], d_rsem.at[n], row, partner)

    def compute_chunk(n, sum_one=None):
        for cp in weight_copies(n):
            cp.wait()
        if sum_one is not None:
            pair_copy(n - 2).wait_recv()
        def products(owner):
            cols = pl.ds(pl.multiple_of(512 * owner, 512), 512)
            return dot(h_v[...], wg_v[n, :, cols]), dot(h_v[...], wu_v[n, :, cols])

        theirs, mine = products(1 - core), products(core)
        for xr in range(2):
            for part in range(2):
                dsend[n, xr, part] = theirs[part][:, 256 * xr:256 * xr + 256].astype(BF16)
                own[n % 3, xr, part] = mine[part][:, 256 * xr:256 * xr + 256]
        started = [] if sum_one is None else sum_one(n - 2)
        pair_copy(n).start()
        for cp in started:
            cp.start()

    def sum_chunk(n):
        keep = own[n % 3, chip] + drecv[n, chip].astype(F32)
        give = (own[n % 3, 1 - chip] + drecv[n, 1 - chip].astype(F32)).astype(BF16)
        return keep, give

    def far_copy(n):
        return remote(xsend.at[n], xrecv.at[n], x_ssem.at[n], x_rsem.at[n], row, far)

    def sum_early(n):
        keep, give = sum_chunk(n)
        xkeep[n] = keep
        xsend[n] = give
        return [far_copy(n)]

    def sum_late(n):
        keep, give = sum_chunk(n)
        keep_out[n - EARLY] = keep.astype(BF16)
        pay_out[2 * (n - EARLY)] = give[0]
        pay_out[2 * (n - EARLY) + 1] = give[1]
        return []

    compute_chunk(0)

    mine = row * 2 + chip
    q_sends = []
    for k, (lo, hi) in enumerate(q_parts):
        qd_cp[k].wait_recv()
        qx[:, :, lo:hi] = (qp[core, :, :, lo:hi].astype(F32) + qd[:, :, lo:hi].astype(F32)).astype(BF16)
        for s, (dy, dx) in enumerate(((0, 1), (1, 0), (1, 1))):
            ty, xx = (row + dy) % 2, (chip + dx) % 2
            cols = pl.ds(lo, min(hi, q_width) - lo if dy else hi - lo)
            cp = remote(qx.at[ty * 2 + xx, :, cols], qr.at[s, :, cols], q_ssem.at[k, s], q_rsem.at[k, s], ty, xx * 2 + core)
            cp.start()
            q_sends.append(cp)

    compute_chunk(1)

    def step(sum_one):
        def body(n, carry):
            compute_chunk(n, sum_one)
            return carry
        return body

    def last_sum(n):
        pair_copy(n).wait_recv()
        sum_late(n)

    lax.fori_loop(2, EARLY + 2, step(sum_early), 0)
    lax.fori_loop(EARLY + 2, CHUNKS - 1, step(sum_late), 0)
    pre_cp = []
    for t in range(READY):
        for part, src in enumerate((k_h, v_h)):
            pre_cp.append(pltpu.make_async_copy(src.at[t], pre_out.at[part, t], pre_sem.at[part, t]))
    for cp in pre_cp:
        cp.start()
    lax.fori_loop(CHUNKS - 1, CHUNKS, step(sum_late), 0)
    last_sum(CHUNKS - 2)

    def rotate(vals):
        return vals * cosv + pltpu.roll(vals, 64, 1) * sinv

    for cp in q_sends:
        cp.wait_recv()
    q_same = qx[mine].astype(F32) + qr[0].astype(F32)
    q_diff = qr[1, :, 0:q_width].astype(F32) + qr[2, :, 0:q_width].astype(F32)
    for half, vals in ((row, q_same), (1 - row, q_diff)):
        for head in range(16):
            qscr[half, :, head, :] = rotate(vals[:, 128 * head:128 * head + 128])
    q_out[...] = qscr[...].astype(BF16)
    kv_out[0] = rotate(q_same[:, q_width:q_width + 128]).astype(BF16).astype(F32)
    kv_out[1] = q_same[:, q_width + 128:].astype(BF16).astype(F32)
    last_sum(CHUNKS - 1)
    for n in range(EARLY):
        far_copy(n).wait_recv()
        full = xkeep[n] + xrecv[n].astype(F32)
        pay_out[2 * LATE + n] = gated(full[0], full[1])
        far_copy(n).wait_send()
    for cp in pre_cp:
        cp.wait()
    for cp in st_cp + qd_cp + q_sends:
        cp.wait_send()

    def drain(n, carry):
        pair_copy(n).wait_send()
        return carry

    lax.fori_loop(0, CHUNKS, drain, 0)


def project(lens, x_blk, gamma, freqs, w_query, w_key, w_value, w_gate, w_up, k_blk, v_blk):
    rows, width = x_blk.shape
    nc = CHUNKS
    q_width = w_query.shape[1] + w_key.shape[1] + w_value.shape[1]
    hbm = pl.BlockSpec(memory_space=pl.ANY)
    return pl.pallas_call(
        project_kernel,
        out_shape=(
            VMEM((2, 16, 16, 128), BF16),
            VMEM((2, 16, 128), F32),
            VMEM((LATE, 2, rows, 256), BF16),
            VMEM((2 * LATE + EARLY, rows, 256), BF16),
            VMEM((2, READY, *k_blk.shape[1:]), BF16),
        ),
        in_specs=[hbm] * 11,
        out_specs=(pl.BlockSpec(memory_space=VMEM),) * 5,
        scratch_shapes=[
            pltpu.SMEM((128,), jnp.int32), VMEM((1, 128), F32), DMA((2, READY)),
            VMEM((rows, width), BF16), VMEM((1, width), F32), DMA((4,)),
            VMEM((width, q_width), BF16), VMEM((nc, width, 1024), BF16), VMEM((nc, width, 1024), BF16),
            VMEM((rows, width), BF16), VMEM((8, rows), F32), VMEM((3, 8, rows), F32),
            VMEM((2, 4, 16, q_width), BF16), VMEM((4, 16, q_width), BF16), VMEM((4, 16, q_width), BF16), VMEM((3, 16, q_width), BF16),
            VMEM((2, 16, 16, 128), F32),
            VMEM((nc, 2, 2, rows, 256), BF16), VMEM((nc, 2, 2, rows, 256), BF16), VMEM((3, 2, 2, rows, 256), F32),
            VMEM((EARLY, 2, rows, 256), F32), VMEM((EARLY, 2, rows, 256), BF16), VMEM((EARLY, 2, rows, 256), BF16),
            DMA((3,)), DMA((nc, 2)), DMA((3,)), DMA((3,)), DMA((2,)), DMA((2,)), DMA((2, 3)), DMA((2, 3)), DMA((nc,)), DMA((nc,)), DMA((EARLY,)), DMA((EARLY,)),
        ],
        compiler_params=pltpu.CompilerParams(collective_id=0, has_side_effects=True, vmem_limit_bytes=47 * 2 ** 20),
        name="project",
    )(*keep_in(pltpu.HBM, lens, x_blk, gamma, freqs, w_query, w_key, w_value, w_gate, w_up, k_blk, v_blk))


SLOTS = 12
AHEAD = 7
BLOCK = 1024


def attend_kernel(lens_h, q_ref, kv_ref, pre_ref, k_in, v_in, k_out, v_out, att_out,
                  kbuf, vbuf, s_scr, in_sem, out_sem, lens_ref, o_scr, small_sem):
    row, col, _, _ = here()
    base = (row * 4 + col) * 16
    count, ctx, _ = k_in.shape

    def in_copies(t):
        slot = lax.rem(t, SLOTS)
        return (pltpu.make_async_copy(k_in.at[t], kbuf.at[slot], in_sem.at[slot, 0]),
                pltpu.make_async_copy(v_in.at[t], vbuf.at[slot], in_sem.at[slot, 1]))

    def out_copies(t):
        slot = lax.rem(t, SLOTS)
        return (pltpu.make_async_copy(kbuf.at[slot], k_out.at[t], out_sem.at[slot, 0]),
                pltpu.make_async_copy(vbuf.at[slot], v_out.at[t], out_sem.at[slot, 1]))

    lens_cp = pltpu.make_async_copy(lens_h, lens_ref, small_sem)
    lens_cp.start()
    for t in range(READY, AHEAD):
        for cp in in_copies(t):
            cp.start()
    lens_cp.wait()

    def take(t, slot):
        def move(b, carry):
            rows = pl.ds(pl.multiple_of(b * 512, 512), 512)
            kbuf[slot, rows] = pre_ref[0, t, rows]
            vbuf[slot, rows] = pre_ref[1, t, rows]
            return carry

        lax.fori_loop(0, ctx // 512, move, 0)

    def attend(t, slot, length, blocks):
        q = jnp.concatenate([q_ref[0, t], q_ref[1, t]], axis=0)
        scale = 128.0 ** -0.5
        peak = None
        for b in range(blocks):
            scores = lax.dot_general(q, kbuf[slot, b * BLOCK:(b + 1) * BLOCK, :], (((1,), (1,)), ((), ())),
                                     preferred_element_type=F32) * scale
            if b == blocks - 1:
                pos = lax.broadcasted_iota(jnp.int32, scores.shape, 1) + b * BLOCK
                scores = jnp.where(pos <= length, scores, -1e30)
            s_scr[:, b * BLOCK:(b + 1) * BLOCK] = scores
            for g in range(BLOCK // 128):
                piece = scores[:, g * 128:(g + 1) * 128]
                peak = piece if peak is None else jnp.maximum(peak, piece)
        peak = jnp.max(peak, axis=1, keepdims=True)
        denom = None
        for b in range(blocks):
            e = jnp.exp(s_scr[:, b * BLOCK:(b + 1) * BLOCK] - peak)
            s_scr[:, b * BLOCK:(b + 1) * BLOCK] = e
            for g in range(BLOCK // 128):
                piece = e[:, g * 128:(g + 1) * 128]
                denom = piece if denom is None else denom + piece
        inv = 1.0 / jnp.sum(denom, axis=1, keepdims=True)
        out = None
        for b in range(blocks):
            probs = (s_scr[:, b * BLOCK:(b + 1) * BLOCK] * inv).astype(BF16)
            part = dot(probs, vbuf[slot, b * BLOCK:(b + 1) * BLOCK, :])
            out = part if out is None else out + part
        o_scr[t] = out

    def body(t, carry):
        slot = lax.rem(t, SLOTS)
        @pl.when(t < READY)
        def _():
            take(t, slot)

        @pl.when(t >= READY)
        def _():
            for cp in in_copies(t):
                cp.wait()

        length = lens_ref[base + t]
        start = pl.multiple_of((length // 16) * 16, 16)
        at_row = lax.broadcasted_iota(jnp.int32, (16, 128), 0) == length - start
        for which, buf in ((0, kbuf), (1, vbuf)):
            old = buf[slot, pl.ds(start, 16), :].astype(F32)
            new = kv_ref[which, pl.ds(t, 1), :]
            buf[slot, pl.ds(start, 16), :] = jnp.where(at_row, new, old).astype(BF16)
        for cp in out_copies(t):
            cp.start()

        @pl.when(t + AHEAD < count)
        def _():
            @pl.when(t >= SLOTS - AHEAD)
            def _():
                for cp in out_copies(t - (SLOTS - AHEAD)):
                    cp.wait()

            for cp in in_copies(t + AHEAD):
                cp.start()

        blocks = length // BLOCK
        for b in range(ctx // BLOCK):
            @pl.when(blocks == b)
            def _():
                attend(t, slot, length, b + 1)

        return carry

    lax.fori_loop(0, count, body, 0)

    for head in range(32):
        att_out[head // 16, :, 128 * (head % 16):128 * (head % 16) + 128] = o_scr[:, head, :].astype(BF16)
    done_in_loop = max(0, count - AHEAD - (SLOTS - AHEAD)) if count > AHEAD else 0
    for t in range(done_in_loop, count):
        for cp in out_copies(t):
            cp.wait()


def attend(lens, q, kv, pre, k_blk, v_blk):
    hbm = pl.BlockSpec(memory_space=pltpu.HBM)
    vm = pl.BlockSpec(memory_space=VMEM)
    count, ctx, dim = k_blk.shape
    return pl.pallas_call(
        attend_kernel,
        out_shape=(
            jax.ShapeDtypeStruct(k_blk.shape, BF16),
            jax.ShapeDtypeStruct(v_blk.shape, BF16),
            VMEM((2, count, 2048), BF16),
        ),
        in_specs=[hbm, vm, vm, vm, hbm, hbm],
        out_specs=(hbm, hbm, vm),
        scratch_shapes=[
            VMEM((SLOTS, ctx, dim), BF16), VMEM((SLOTS, ctx, dim), BF16),
            VMEM((32, ctx), F32), DMA((SLOTS, 2)), DMA((SLOTS, 2)),
            pltpu.SMEM((128,), jnp.int32), VMEM((count, 32, dim), F32), DMA,
        ],
        cost_estimate=pl.CostEstimate(flops=count * 32 * ctx * dim * 4, bytes_accessed=count * ctx * dim * 8, transcendentals=count * 32 * ctx),
        compiler_params=pltpu.CompilerParams(vmem_limit_bytes=30 * 2 ** 20),
        name="attend",
    )(*keep_in(pltpu.HBM, lens), *keep_in(VMEM, q, kv, pre), *keep_in(pltpu.HBM, k_blk, v_blk))


WIDE = 256 * CHUNKS
EDGE = 256 * (EARLY + 3)
ITEMS = tuple((lo, hi, last) for lo, hi in ((0, 48), (48, 80), (80, 112), (112, 128)) for last in (False, True))


def output_kernel(att_ref, keep_v, pay_v, got_v, x_h, wo_h, wd_h, y_out,
                  x_ref, act_v, in_sem, wo_v, wd_v, attf, acc, ysend, yrecv,
                  wo_sem, wd_sem, a_ssem, a_rsem, f_ssem, f_rsem, g_ssem, g_rsem, h_ssem, h_rsem, c_ssem, c_rsem, y_ssem, y_rsem):
    greet(MET_LATE)
    row, col, chip, core = here()
    partner = col + 1 - 2 * core
    far = (col + 2) % 4
    order = (2 * core + chip, 2 * (1 - core) + chip, 2 * core + 1 - chip, 2 * (1 - core) + 1 - chip)
    x_cp = pltpu.make_async_copy(x_h, x_ref, in_sem)
    x_cp.start()
    wd_cp = []
    for s, owner in enumerate(order):
        wd_cp.append(pltpu.make_async_copy(wd_h.at[:, owner], wd_v.at[s], wd_sem.at[s]))
    wo_cp = pltpu.make_async_copy(wo_h, wo_v, wo_sem)

    for cp in (wd_cp[0], wd_cp[1], wo_cp, wd_cp[2], wd_cp[3]):
        cp.start()
    greeted(MET_LATE)
    mine = row * 2 + chip
    around = ((0, 1), (1, 0), (1, 1))
    a_cp = []
    for s, (dy, dx) in enumerate(around):
        ty, xx = (row + dy) % 2, (chip + dx) % 2
        cp = remote(att_ref.at[ty], attf.at[mine, core], a_ssem.at[s], a_rsem.at[s], ty, xx * 2 + core)
        cp.start()
        a_cp.append(cp)
    attf[mine, core] = att_ref[row]
    f_own = remote(attf.at[mine, core], attf.at[mine, core], f_ssem.at[3], f_rsem.at[3], row, partner)
    f_own.start()

    def piece(s, item):
        lo, hi, last = ITEMS[item]
        c0, c1 = (EDGE, WIDE) if last else (256 * EARLY, EDGE)
        return act_v.at[pl.ds(lo, hi - lo), pl.ds(WIDE * s + c0, c1 - c0)]

    g_cp, h_cp = [], []
    for item, (lo, hi, last) in enumerate(ITEMS):
        rows = slice(lo, hi)
        for n in range(3, LATE) if last else range(3):
            g = keep_v[n, 0, rows].astype(F32) + got_v[2 * n, rows].astype(F32)
            u = keep_v[n, 1, rows].astype(F32) + got_v[2 * n + 1, rows].astype(F32)
            at = 256 * (EARLY + n)
            act_v[rows, at:at + 256] = gated(g, u)
        g_cp.append(remote(piece(0, item), piece(2, item), g_ssem.at[item], g_rsem.at[item], row, far))
        g_cp[item].start()
        h_cp.append(remote(piece(2, item), piece(3, item), h_ssem.at[item], h_rsem.at[item], row, partner))
    for s, src in ((0, pay_v), (2, got_v)):
        for n in range(EARLY):
            act_v[:, WIDE * s + 256 * n:WIDE * s + 256 * n + 256] = src[2 * LATE + n]
    every = pl.ds(0, 128)
    first = pl.ds(2 * WIDE, 256 * EARLY)
    c_cp = [remote(act_v.at[every, pl.ds(0, WIDE)], act_v.at[every, pl.ds(WIDE, WIDE)], c_ssem.at[0], c_rsem.at[0], row, partner),
            remote(act_v.at[every, first], act_v.at[every, pl.ds(3 * WIDE, 256 * EARLY)], c_ssem.at[1], c_rsem.at[1], row, partner)]
    for cp in c_cp:
        cp.start()

    def down(rows, s, k0, k1):
        return dot(act_v[rows, WIDE * s + k0:WIDE * s + k1], wd_v[s, k0 // 256:k1 // 256].reshape(k1 - k0, -1))

    for cp in c_cp:
        cp.wait_recv()
    wd_cp[0].wait()
    wd_cp[1].wait()
    acc[...] = down(slice(0, 128), 0, 0, WIDE) + down(slice(0, 128), 1, 0, WIDE)
    f_cp = []
    for s, (dy, dx) in enumerate(around):
        a_cp[s].wait_recv()
        index = ((row + dy) % 2) * 2 + (chip + dx) % 2
        cp = remote(attf.at[index, core], attf.at[index, core], f_ssem.at[s], f_rsem.at[s], row, partner)
        cp.start()
        f_cp.append(cp)
    def attention_part():
        wo_cp.wait()
        for cp in f_cp + [f_own]:
            cp.wait_recv()
        wd_cp[2].wait()
        wd_cp[3].wait()
        every_row = slice(0, 128)
        early = down(every_row, 2, 0, 256 * EARLY) + down(every_row, 3, 0, 256 * EARLY)
        acc[...] += dot(attf[...].reshape(128, 2048), wo_v[...]) + early

    y_cp = []

    def finish(item):
        lo, hi, last = ITEMS[item]
        rows, window = slice(lo, hi), pl.ds(lo, hi - lo)
        k0, k1 = (EDGE, WIDE) if last else (256 * EARLY, EDGE)
        h_cp[item].wait_recv()
        part = acc[rows] + (down(rows, 2, k0, k1) + down(rows, 3, k0, k1))
        if last:
            ysend[rows] = part.astype(BF16)
            cp = remote(ysend.at[window], yrecv.at[window], y_ssem.at[item], y_rsem.at[item], 1 - row, col)
            cp.start()
            y_cp.append((rows, cp))
        else:
            acc[rows] = part

    for item in range(len(ITEMS)):
        g_cp[item].wait_recv()
        h_cp[item].start()
        if item:
            finish(item - 1)
        else:
            attention_part()
    finish(len(ITEMS) - 1)
    x_cp.wait()
    for rows, cp in y_cp:
        cp.wait_recv()
        both = ysend[rows].astype(F32) + yrecv[rows].astype(F32)
        y_out[rows] = (x_ref[rows].astype(F32) + both).astype(BF16)
    for cp in a_cp + c_cp + f_cp + [f_own] + g_cp + h_cp + [cp for _, cp in y_cp]:
        cp.wait_send()


def output(att, keep, pay, got, x_blk, w_out, w_down):
    rows, width = x_blk.shape
    hbm = pl.BlockSpec(memory_space=pl.ANY)
    vm = pl.BlockSpec(memory_space=VMEM)
    items = len(ITEMS)
    return pl.pallas_call(
        output_kernel,
        out_shape=pltpu.VMEM((rows, width), BF16),
        in_specs=[vm] * 4 + [hbm] * 3,
        out_specs=vm,
        scratch_shapes=[
            VMEM((rows, width), BF16), VMEM((rows, 4 * WIDE), BF16), DMA,
            VMEM((2048, width), BF16), VMEM((4, CHUNKS, 256, width), BF16), VMEM((4, 2, 16, 2048), BF16),
            VMEM((rows, width), F32), VMEM((rows, width), BF16), VMEM((rows, width), BF16),
            DMA, DMA((4,)), DMA((3,)), DMA((3,)), DMA((4,)), DMA((4,)), DMA((items,)), DMA((items,)), DMA((items,)), DMA((items,)),
            DMA((2,)), DMA((2,)), DMA((items,)), DMA((items,)),
        ],
        compiler_params=pltpu.CompilerParams(collective_id=1, has_side_effects=True, vmem_limit_bytes=32 * 2 ** 20),
        name="output",
    )(*keep_in(VMEM, att, keep, pay, got), *keep_in(pltpu.HBM, x_blk, w_out, w_down.reshape(CHUNKS, 4, 256, width)))


def solution(mesh):
    cache_spec = P(("dp", "ty", "tx"), None, None)
    across = [(0, 2), (1, 3), (2, 0), (3, 1)]

    def layer_shard(x_blk, lens, k_blk, v_blk, gamma, w_query, w_key, w_value, w_gate, w_up, w_out, w_down):
        freqs = np.tile(np.float32(ROPE_BASE ** (-np.arange(0, 128, 2) / 128.0)), 2)[None, :]
        q, kv, keep, pay, pre = project(lens, x_blk, gamma[None, :], freqs, w_query, w_key, w_value, w_gate, w_up, k_blk, v_blk)
        got = lax.ppermute(pay, "tx", across)
        k_out, v_out, att = attend(lens, q, kv, pre, k_blk, v_blk)
        y = output(att, keep, pay, got, x_blk, w_out, w_down)
        return y, k_out, v_out

    in_specs = (P("dp", "tx"), P("dp"), cache_spec, cache_spec, P("tx"), P("tx", "ty"), P("tx", None), P("tx", None), P("tx", "ty"), P("tx", "ty"), P("ty", "tx"), P("ty", "tx"))
    out_specs = (P("dp", "tx"), cache_spec, cache_spec)
    return jax.shard_map(layer_shard, mesh=mesh, in_specs=in_specs, out_specs=out_specs, check_vma=False)
```

```python
import functools

import jax
import jax.numpy as jnp
import numpy as np
from jax import lax
from jax.experimental import pallas as pl
from jax.experimental.pallas import tpu as pltpu
from jax.sharding import PartitionSpec as P

EPSILON = 1e-6
ROPE_BASE = 10000.0
BF16 = jnp.bfloat16
F32 = jnp.float32
MESH = pl.DeviceIdType.MESH

VMEM = pltpu.VMEM
VMEM_ALL = 67043328
DMA = pltpu.SemaphoreType.DMA


def here():
    row = lax.axis_index("ty")
    col = lax.axis_index("tx")
    return row, col, col // 2, col % 2


def greet(offsets):
    row, _, chip, core = here()
    barrier = pltpu.get_barrier_semaphore()
    for dy, dx, dc in offsets:
        peer = {"ty": (row + dy) % 2, "tx": ((chip + dx) % 2) * 2 + (core + dc) % 2}
        pl.semaphore_signal(barrier, inc=1, device_id=peer, device_id_type=MESH)


def greeted(offsets):
    pl.semaphore_wait(pltpu.get_barrier_semaphore(), len(offsets))


MET_EARLY = ((0, 0, 1), (0, 1, 0), (0, 1, 1), (1, 0, 0), (1, 1, 0))
MET_LATE = ((0, 0, 1), (0, 1, 0), (1, 0, 0), (1, 1, 0))


def remote(src, dst, send_sem, recv_sem, ty, tx):
    return pltpu.make_async_remote_copy(
        src_ref=src, dst_ref=dst, send_sem=send_sem, recv_sem=recv_sem,
        device_id={"ty": ty, "tx": tx}, device_id_type=MESH)


def keep_in(space, *arrays):
    return [pltpu.with_memory_space_constraint(v, space) for v in arrays]


def dot(a, b):
    return jnp.dot(a, b, preferred_element_type=F32)


CHUNKS = 8
READY = 5
EARLY = 2
LATE = CHUNKS - EARLY


def gated(g, u):
    return (jax.nn.silu(g.astype(BF16).astype(F32)) * u.astype(BF16).astype(F32)).astype(BF16)


def project_kernel(lens_h, x_h, gamma_h, freq_h, wq_h, wk_h, wv_h, wg_h, wu_h, k_h, v_h,
                   q_out, kv_out, keep_out, pay_out, pre_out,
                   lens_ref, freq_ref, pre_sem, x_ref, gamma_ref, x_sem, wq_v, wg_v, wu_v, h_v, st_send, st_recv,
                   qp, qd, qx, qr, qscr, dsend, drecv, own, xkeep, xsend, xrecv,
                   wq_sem, w_sem, st_ssem, st_rsem, qd_ssem, qd_rsem, q_ssem, q_rsem,
                   d_ssem, d_rsem, x_ssem, x_rsem):
    row, col, chip, core = here()
    partner = col + 1 - 2 * core
    far = (col + 2) % 4
    me = row * 4 + col
    greet(MET_EARLY)

    x_cp = pltpu.make_async_copy(x_h, x_ref, x_sem.at[0])
    gamma_cp = pltpu.make_async_copy(gamma_h, gamma_ref, x_sem.at[1])
    lens_cp = pltpu.make_async_copy(lens_h, lens_ref, x_sem.at[2])
    freq_cp = pltpu.make_async_copy(freq_h, freq_ref, x_sem.at[3])
    for cp in (x_cp, gamma_cp, lens_cp, freq_cp):
        cp.start()
    q_width = wq_h.shape[1]
    wq_cp = [pltpu.make_async_copy(wq_h, wq_v.at[:, pl.ds(0, q_width)], wq_sem.at[0]),
             pltpu.make_async_copy(wk_h, wq_v.at[:, pl.ds(q_width, 128)], wq_sem.at[1]),
             pltpu.make_async_copy(wv_h, wq_v.at[:, pl.ds(q_width + 128, 128)], wq_sem.at[2])]
    for cp in wq_cp:
        cp.start()

    def weight_copies(n):
        cols = pl.ds(pl.multiple_of(1024 * n, 1024), 1024)
        return (pltpu.make_async_copy(wg_h.at[:, cols], wg_v.at[n], w_sem.at[n, 0]),
                pltpu.make_async_copy(wu_h.at[:, cols], wu_v.at[n], w_sem.at[n, 1]))

    def start_weights(n, carry):
        for cp in weight_copies(n):
            cp.start()
        return carry

    lax.fori_loop(0, CHUNKS, start_weights, 0)

    x_cp.wait()
    xf = x_ref[...].astype(F32)
    sum1 = jnp.sum(xf, axis=1, keepdims=True)
    sum2 = jnp.sum(xf * xf, axis=1, keepdims=True)
    rows = xf.shape[0]
    eye = lax.broadcasted_iota(jnp.int32, (rows, rows), 0) == lax.broadcasted_iota(jnp.int32, (rows, rows), 1)
    line1 = jnp.sum(jnp.where(eye, sum1, 0.0), axis=0, keepdims=True)
    line2 = jnp.sum(jnp.where(eye, sum2, 0.0), axis=0, keepdims=True)
    first = lax.broadcasted_iota(jnp.int32, (8, rows), 0) == 0
    st_send[...] = jnp.where(first, line1, line2)
    greeted(MET_EARLY)
    st_cp = [remote(st_send, st_recv.at[d - 1], st_ssem.at[d - 1], st_rsem.at[d - 1], row, (col + d) % 4) for d in (1, 2, 3)]
    for cp in st_cp:
        cp.start()
    lens_cp.wait()
    freq_cp.wait()
    seq = lax.broadcasted_iota(jnp.int32, (16, 128), 0)
    place = jnp.zeros((16, 128), F32)
    for b in range(16):
        place = jnp.where(seq == b, lens_ref[me * 16 + b].astype(F32), place)
    angle = place * freq_ref[...]
    cosv = jnp.cos(angle)
    sinv = jnp.where(lax.broadcasted_iota(jnp.int32, (16, 128), 1) < 64, -jnp.sin(angle), jnp.sin(angle))
    for cp in st_cp:
        cp.wait_recv()
    total = st_send[...] + st_recv[0] + st_recv[1] + st_recv[2]
    width = 4.0 * xf.shape[1]
    mean_line = total[0:1] / width
    var_line = total[1:2] / width - mean_line * mean_line
    rstd_line = lax.rsqrt(var_line + EPSILON)
    mean = jnp.sum(jnp.where(eye, mean_line, 0.0), axis=1, keepdims=True)
    rstd = jnp.sum(jnp.where(eye, rstd_line, 0.0), axis=1, keepdims=True)
    gamma_cp.wait()
    h_v[...] = ((xf - mean) * rstd * gamma_ref[...]).astype(BF16)

    for cp in wq_cp:
        cp.wait()
    q_parts = ((0, 1024), (1024, q_width + 256))
    qd_cp = []
    for k, (lo, hi) in enumerate(q_parts):
        part = dot(h_v[...], wq_v[:, lo:hi]).astype(BF16)
        for d in range(8):
            qp[d % 2, d // 2, :, lo:hi] = part[16 * d:16 * d + 16]
        cols = pl.ds(lo, hi - lo)
        qd_cp.append(remote(qp.at[1 - core, :, :, cols], qd.at[:, :, cols], qd_ssem.at[k], qd_rsem.at[k], row, partner))
        qd_cp[k].start()

    def pair_copy(n):
        return remote(dsend.at[n], drecv.at[n], d_ssem.at[n], d_rsem.at[n], row, partner)

    def compute_chunk(n, sum_one=None):
        for cp in weight_copies(n):
            cp.wait()
        if sum_one is not None:
            pair_copy(n - 2).wait_recv()
        def products(owner):
            cols = pl.ds(pl.multiple_of(512 * owner, 512), 512)
            return dot(h_v[...], wg_v[n, :, cols]), dot(h_v[...], wu_v[n, :, cols])

        theirs, mine = products(1 - core), products(core)
        for xr in range(2):
            for part in range(2):
                dsend[n, xr, part] = theirs[part][:, 256 * xr:256 * xr + 256].astype(BF16)
                own[n % 3, xr, part] = mine[part][:, 256 * xr:256 * xr + 256]
        started = [] if sum_one is None else sum_one(n - 2)
        pair_copy(n).start()
        for cp in started:
            cp.start()

    def sum_chunk(n):
        keep = own[n % 3, chip] + drecv[n, chip].astype(F32)
        give = (own[n % 3, 1 - chip] + drecv[n, 1 - chip].astype(F32)).astype(BF16)
        return keep, give

    def far_copy(n):
        return remote(xsend.at[n], xrecv.at[n], x_ssem.at[n], x_rsem.at[n], row, far)

    def sum_early(n):
        keep, give = sum_chunk(n)
        xkeep[n] = keep
        xsend[n] = give
        return [far_copy(n)]

    def sum_late(n):
        keep, give = sum_chunk(n)
        keep_out[n - EARLY] = keep.astype(BF16)
        pay_out[2 * (n - EARLY)] = give[0]
        pay_out[2 * (n - EARLY) + 1] = give[1]
        return []

    compute_chunk(0)

    mine = row * 2 + chip
    q_sends = []
    for k, (lo, hi) in enumerate(q_parts):
        qd_cp[k].wait_recv()
        qx[:, :, lo:hi] = (qp[core, :, :, lo:hi].astype(F32) + qd[:, :, lo:hi].astype(F32)).astype(BF16)
        for s, (dy, dx) in enumerate(((0, 1), (1, 0), (1, 1))):
            ty, xx = (row + dy) % 2, (chip + dx) % 2
            cols = pl.ds(lo, min(hi, q_width) - lo if dy else hi - lo)
            cp = remote(qx.at[ty * 2 + xx, :, cols], qr.at[s, :, cols], q_ssem.at[k, s], q_rsem.at[k, s], ty, xx * 2 + core)
            cp.start()
            q_sends.append(cp)

    compute_chunk(1)

    def step(sum_one):
        def body(n, carry):
            compute_chunk(n, sum_one)
            return carry
        return body

    def last_sum(n):
        pair_copy(n).wait_recv()
        sum_late(n)

    lax.fori_loop(2, EARLY + 2, step(sum_early), 0)
    lax.fori_loop(EARLY + 2, CHUNKS - 1, step(sum_late), 0)
    pre_cp = []
    for t in range(READY):
        for part, src in enumerate((k_h, v_h)):
            pre_cp.append(pltpu.make_async_copy(src.at[t], pre_out.at[part, t], pre_sem.at[part, t]))
    for cp in pre_cp:
        cp.start()
    lax.fori_loop(CHUNKS - 1, CHUNKS, step(sum_late), 0)
    last_sum(CHUNKS - 2)

    def rotate(vals):
        return vals * cosv + pltpu.roll(vals, 64, 1) * sinv

    for cp in q_sends:
        cp.wait_recv()
    q_same = qx[mine].astype(F32) + qr[0].astype(F32)
    q_diff = qr[1, :, 0:q_width].astype(F32) + qr[2, :, 0:q_width].astype(F32)
    for half, vals in ((row, q_same), (1 - row, q_diff)):
        for head in range(16):
            qscr[half, :, head, :] = rotate(vals[:, 128 * head:128 * head + 128])
    q_out[...] = qscr[...].astype(BF16)
    kv_out[0] = rotate(q_same[:, q_width:q_width + 128]).astype(BF16).astype(F32)
    kv_out[1] = q_same[:, q_width + 128:].astype(BF16).astype(F32)
    last_sum(CHUNKS - 1)
    for n in range(EARLY):
        far_copy(n).wait_recv()
        full = xkeep[n] + xrecv[n].astype(F32)
        pay_out[2 * LATE + n] = gated(full[0], full[1])
        far_copy(n).wait_send()
    for cp in pre_cp:
        cp.wait()
    for cp in st_cp + qd_cp + q_sends:
        cp.wait_send()

    def drain(n, carry):
        pair_copy(n).wait_send()
        return carry

    lax.fori_loop(0, CHUNKS, drain, 0)


def project(lens, x_blk, gamma, freqs, w_query, w_key, w_value, w_gate, w_up, k_blk, v_blk):
    rows, width = x_blk.shape
    nc = CHUNKS
    q_width = w_query.shape[1] + w_key.shape[1] + w_value.shape[1]
    hbm = pl.BlockSpec(memory_space=pl.ANY)
    return pl.pallas_call(
        project_kernel,
        out_shape=(
            VMEM((2, 16, 16, 128), BF16),
            VMEM((2, 16, 128), F32),
            VMEM((LATE, 2, rows, 256), BF16),
            VMEM((2 * LATE + EARLY, rows, 256), BF16),
            VMEM((2, READY, *k_blk.shape[1:]), BF16),
        ),
        in_specs=[hbm] * 11,
        out_specs=(pl.BlockSpec(memory_space=VMEM),) * 5,
        scratch_shapes=[
            pltpu.SMEM((128,), jnp.int32), VMEM((1, 128), F32), DMA((2, READY)),
            VMEM((rows, width), BF16), VMEM((1, width), F32), DMA((4,)),
            VMEM((width, q_width), BF16), VMEM((nc, width, 1024), BF16), VMEM((nc, width, 1024), BF16),
            VMEM((rows, width), BF16), VMEM((8, rows), F32), VMEM((3, 8, rows), F32),
            VMEM((2, 4, 16, q_width), BF16), VMEM((4, 16, q_width), BF16), VMEM((4, 16, q_width), BF16), VMEM((3, 16, q_width), BF16),
            VMEM((2, 16, 16, 128), F32),
            VMEM((nc, 2, 2, rows, 256), BF16), VMEM((nc, 2, 2, rows, 256), BF16), VMEM((3, 2, 2, rows, 256), F32),
            VMEM((EARLY, 2, rows, 256), F32), VMEM((EARLY, 2, rows, 256), BF16), VMEM((EARLY, 2, rows, 256), BF16),
            DMA((3,)), DMA((nc, 2)), DMA((3,)), DMA((3,)), DMA((2,)), DMA((2,)), DMA((2, 3)), DMA((2, 3)), DMA((nc,)), DMA((nc,)), DMA((EARLY,)), DMA((EARLY,)),
        ],
        compiler_params=pltpu.CompilerParams(collective_id=0, has_side_effects=True, vmem_limit_bytes=47 * 2 ** 20),
        name="project",
    )(*keep_in(pltpu.HBM, lens, x_blk, gamma, freqs, w_query, w_key, w_value, w_gate, w_up, k_blk, v_blk))


SLOTS = 12
AHEAD = 7
BLOCK = 1024


def attend_kernel(lens_h, q_ref, kv_ref, pre_ref, k_in, v_in, k_out, v_out, att_out,
                  kbuf, vbuf, s_scr, in_sem, out_sem, lens_ref, o_scr, small_sem):
    row, col, _, _ = here()
    base = (row * 4 + col) * 16
    count, ctx, _ = k_in.shape

    def in_copies(t):
        slot = lax.rem(t, SLOTS)
        return (pltpu.make_async_copy(k_in.at[t], kbuf.at[slot], in_sem.at[slot, 0]),
                pltpu.make_async_copy(v_in.at[t], vbuf.at[slot], in_sem.at[slot, 1]))

    def out_copies(t):
        slot = lax.rem(t, SLOTS)
        return (pltpu.make_async_copy(kbuf.at[slot], k_out.at[t], out_sem.at[slot, 0]),
                pltpu.make_async_copy(vbuf.at[slot], v_out.at[t], out_sem.at[slot, 1]))

    lens_cp = pltpu.make_async_copy(lens_h, lens_ref, small_sem)
    lens_cp.start()
    for t in range(READY, AHEAD):
        for cp in in_copies(t):
            cp.start()
    lens_cp.wait()

    def take(t, slot):
        def move(b, carry):
            rows = pl.ds(pl.multiple_of(b * 512, 512), 512)
            kbuf[slot, rows] = pre_ref[0, t, rows]
            vbuf[slot, rows] = pre_ref[1, t, rows]
            return carry

        lax.fori_loop(0, ctx // 512, move, 0)

    def attend(t, slot, length, blocks):
        q = jnp.concatenate([q_ref[0, t], q_ref[1, t]], axis=0)
        scale = 128.0 ** -0.5
        peak = None
        for b in range(blocks):
            scores = lax.dot_general(q, kbuf[slot, b * BLOCK:(b + 1) * BLOCK, :], (((1,), (1,)), ((), ())),
                                     preferred_element_type=F32) * scale
            if b == blocks - 1:
                pos = lax.broadcasted_iota(jnp.int32, scores.shape, 1) + b * BLOCK
                scores = jnp.where(pos <= length, scores, -1e30)
            s_scr[:, b * BLOCK:(b + 1) * BLOCK] = scores
            for g in range(BLOCK // 128):
                piece = scores[:, g * 128:(g + 1) * 128]
                peak = piece if peak is None else jnp.maximum(peak, piece)
        peak = jnp.max(peak, axis=1, keepdims=True)
        denom = None
        for b in range(blocks):
            e = jnp.exp(s_scr[:, b * BLOCK:(b + 1) * BLOCK] - peak)
            s_scr[:, b * BLOCK:(b + 1) * BLOCK] = e
            for g in range(BLOCK // 128):
                piece = e[:, g * 128:(g + 1) * 128]
                denom = piece if denom is None else denom + piece
        inv = 1.0 / jnp.sum(denom, axis=1, keepdims=True)
        out = None
        for b in range(blocks):
            probs = (s_scr[:, b * BLOCK:(b + 1) * BLOCK] * inv).astype(BF16)
            part = dot(probs, vbuf[slot, b * BLOCK:(b + 1) * BLOCK, :])
            out = part if out is None else out + part
        o_scr[t] = out

    def body(t, carry):
        slot = lax.rem(t, SLOTS)
        @pl.when(t < READY)
        def _():
            take(t, slot)

        @pl.when(t >= READY)
        def _():
            for cp in in_copies(t):
                cp.wait()

        length = lens_ref[base + t]
        start = pl.multiple_of((length // 16) * 16, 16)
        at_row = lax.broadcasted_iota(jnp.int32, (16, 128), 0) == length - start
        for which, buf in ((0, kbuf), (1, vbuf)):
            old = buf[slot, pl.ds(start, 16), :].astype(F32)
            new = kv_ref[which, pl.ds(t, 1), :]
            buf[slot, pl.ds(start, 16), :] = jnp.where(at_row, new, old).astype(BF16)
        for cp in out_copies(t):
            cp.start()

        @pl.when(t + AHEAD < count)
        def _():
            @pl.when(t >= SLOTS - AHEAD)
            def _():
                for cp in out_copies(t - (SLOTS - AHEAD)):
                    cp.wait()

            for cp in in_copies(t + AHEAD):
                cp.start()

        blocks = length // BLOCK
        for b in range(ctx // BLOCK):
            @pl.when(blocks == b)
            def _():
                attend(t, slot, length, b + 1)

        return carry

    lax.fori_loop(0, count, body, 0)

    for head in range(32):
        att_out[head // 16, :, 128 * (head % 16):128 * (head % 16) + 128] = o_scr[:, head, :].astype(BF16)
    done_in_loop = max(0, count - AHEAD - (SLOTS - AHEAD)) if count > AHEAD else 0
    for t in range(done_in_loop, count):
        for cp in out_copies(t):
            cp.wait()


def attend(lens, q, kv, pre, k_blk, v_blk):
    hbm = pl.BlockSpec(memory_space=pltpu.HBM)
    vm = pl.BlockSpec(memory_space=VMEM)
    count, ctx, dim = k_blk.shape
    return pl.pallas_call(
        attend_kernel,
        out_shape=(
            jax.ShapeDtypeStruct(k_blk.shape, BF16),
            jax.ShapeDtypeStruct(v_blk.shape, BF16),
            VMEM((2, count, 2048), BF16),
        ),
        in_specs=[hbm, vm, vm, vm, hbm, hbm],
        out_specs=(hbm, hbm, vm),
        scratch_shapes=[
            VMEM((SLOTS, ctx, dim), BF16), VMEM((SLOTS, ctx, dim), BF16),
            VMEM((32, ctx), F32), DMA((SLOTS, 2)), DMA((SLOTS, 2)),
            pltpu.SMEM((128,), jnp.int32), VMEM((count, 32, dim), F32), DMA,
        ],
        cost_estimate=pl.CostEstimate(flops=count * 32 * ctx * dim * 4, bytes_accessed=count * ctx * dim * 8, transcendentals=count * 32 * ctx),
        compiler_params=pltpu.CompilerParams(vmem_limit_bytes=30 * 2 ** 20),
        name="attend",
    )(*keep_in(pltpu.HBM, lens), *keep_in(VMEM, q, kv, pre), *keep_in(pltpu.HBM, k_blk, v_blk))


WIDE = 256 * CHUNKS
EDGE = 256 * (EARLY + 3)
ITEMS = tuple((lo, hi, last) for lo, hi in ((0, 48), (48, 96), (96, 112), (112, 128)) for last in (False, True))


def output_kernel(att_ref, keep_v, pay_v, got_v, x_h, wo_h, wd_h, y_out,
                  x_ref, act_v, in_sem, wo_v, wd_v, attf, acc, ysend, yrecv,
                  wo_sem, wd_sem, a_ssem, a_rsem, f_ssem, f_rsem, g_ssem, g_rsem, h_ssem, h_rsem, c_ssem, c_rsem, y_ssem, y_rsem):
    greet(MET_LATE)
    row, col, chip, core = here()
    partner = col + 1 - 2 * core
    far = (col + 2) % 4
    order = (2 * core + chip, 2 * (1 - core) + chip, 2 * core + 1 - chip, 2 * (1 - core) + 1 - chip)
    x_cp = pltpu.make_async_copy(x_h, x_ref, in_sem)
    x_cp.start()
    wd_cp = []
    for s, owner in enumerate(order):
        wd_cp.append(pltpu.make_async_copy(wd_h.at[:, owner], wd_v.at[s], wd_sem.at[s]))
    wo_cp = pltpu.make_async_copy(wo_h, wo_v, wo_sem)

    for cp in (wd_cp[0], wd_cp[1], wo_cp, wd_cp[2], wd_cp[3]):
        cp.start()
    greeted(MET_LATE)
    mine = row * 2 + chip
    around = ((0, 1), (1, 0), (1, 1))
    a_cp = []
    for s, (dy, dx) in enumerate(around):
        ty, xx = (row + dy) % 2, (chip + dx) % 2
        cp = remote(att_ref.at[ty], attf.at[mine, core], a_ssem.at[s], a_rsem.at[s], ty, xx * 2 + core)
        cp.start()
        a_cp.append(cp)
    attf[mine, core] = att_ref[row]
    f_own = remote(attf.at[mine, core], attf.at[mine, core], f_ssem.at[3], f_rsem.at[3], row, partner)
    f_own.start()

    def piece(s, item):
        lo, hi, last = ITEMS[item]
        c0, c1 = (EDGE, WIDE) if last else (256 * EARLY, EDGE)
        return act_v.at[pl.ds(lo, hi - lo), pl.ds(WIDE * s + c0, c1 - c0)]

    g_cp, h_cp = [], []
    for item, (lo, hi, last) in enumerate(ITEMS):
        rows = slice(lo, hi)
        for n in range(3, LATE) if last else range(3):
            g = keep_v[n, 0, rows].astype(F32) + got_v[2 * n, rows].astype(F32)
            u = keep_v[n, 1, rows].astype(F32) + got_v[2 * n + 1, rows].astype(F32)
            at = 256 * (EARLY + n)
            act_v[rows, at:at + 256] = gated(g, u)
        g_cp.append(remote(piece(0, item), piece(2, item), g_ssem.at[item], g_rsem.at[item], row, far))
        g_cp[item].start()
        h_cp.append(remote(piece(2, item), piece(3, item), h_ssem.at[item], h_rsem.at[item], row, partner))
    for s, src in ((0, pay_v), (2, got_v)):
        for n in range(EARLY):
            act_v[:, WIDE * s + 256 * n:WIDE * s + 256 * n + 256] = src[2 * LATE + n]
    every = pl.ds(0, 128)
    first = pl.ds(2 * WIDE, 256 * EARLY)
    c_cp = [remote(act_v.at[every, pl.ds(0, WIDE)], act_v.at[every, pl.ds(WIDE, WIDE)], c_ssem.at[0], c_rsem.at[0], row, partner),
            remote(act_v.at[every, first], act_v.at[every, pl.ds(3 * WIDE, 256 * EARLY)], c_ssem.at[1], c_rsem.at[1], row, partner)]
    for cp in c_cp:
        cp.start()

    def down(rows, s, k0, k1):
        return dot(act_v[rows, WIDE * s + k0:WIDE * s + k1], wd_v[s, k0 // 256:k1 // 256].reshape(k1 - k0, -1))

    for cp in c_cp:
        cp.wait_recv()
    wd_cp[0].wait()
    wd_cp[1].wait()
    acc[...] = down(slice(0, 128), 0, 0, WIDE) + down(slice(0, 128), 1, 0, WIDE)
    f_cp = []
    for s, (dy, dx) in enumerate(around):
        a_cp[s].wait_recv()
        index = ((row + dy) % 2) * 2 + (chip + dx) % 2
        cp = remote(attf.at[index, core], attf.at[index, core], f_ssem.at[s], f_rsem.at[s], row, partner)
        cp.start()
        f_cp.append(cp)
    def attention_part():
        wo_cp.wait()
        for cp in f_cp + [f_own]:
            cp.wait_recv()
        wd_cp[2].wait()
        wd_cp[3].wait()
        every_row = slice(0, 128)
        early = down(every_row, 2, 0, 256 * EARLY) + down(every_row, 3, 0, 256 * EARLY)
        acc[...] += dot(attf[...].reshape(128, 2048), wo_v[...]) + early

    y_cp = []

    def finish(item):
        lo, hi, last = ITEMS[item]
        rows, window = slice(lo, hi), pl.ds(lo, hi - lo)
        k0, k1 = (EDGE, WIDE) if last else (256 * EARLY, EDGE)
        h_cp[item].wait_recv()
        part = acc[rows] + (down(rows, 2, k0, k1) + down(rows, 3, k0, k1))
        if last:
            ysend[rows] = part.astype(BF16)
            cp = remote(ysend.at[window], yrecv.at[window], y_ssem.at[item], y_rsem.at[item], 1 - row, col)
            cp.start()
            y_cp.append((rows, cp))
        else:
            acc[rows] = part

    for item in range(len(ITEMS)):
        g_cp[item].wait_recv()
        h_cp[item].start()
        if item:
            finish(item - 1)
        else:
            attention_part()
    finish(len(ITEMS) - 1)
    x_cp.wait()
    for rows, cp in y_cp:
        cp.wait_recv()
        both = ysend[rows].astype(F32) + yrecv[rows].astype(F32)
        y_out[rows] = (x_ref[rows].astype(F32) + both).astype(BF16)
    for cp in a_cp + c_cp + f_cp + [f_own] + g_cp + h_cp + [cp for _, cp in y_cp]:
        cp.wait_send()


def output(att, keep, pay, got, x_blk, w_out, w_down):
    rows, width = x_blk.shape
    hbm = pl.BlockSpec(memory_space=pl.ANY)
    vm = pl.BlockSpec(memory_space=VMEM)
    items = len(ITEMS)
    return pl.pallas_call(
        output_kernel,
        out_shape=pltpu.VMEM((rows, width), BF16),
        in_specs=[vm] * 4 + [hbm] * 3,
        out_specs=vm,
        scratch_shapes=[
            VMEM((rows, width), BF16), VMEM((rows, 4 * WIDE), BF16), DMA,
            VMEM((2048, width), BF16), VMEM((4, CHUNKS, 256, width), BF16), VMEM((4, 2, 16, 2048), BF16),
            VMEM((rows, width), F32), VMEM((rows, width), BF16), VMEM((rows, width), BF16),
            DMA, DMA((4,)), DMA((3,)), DMA((3,)), DMA((4,)), DMA((4,)), DMA((items,)), DMA((items,)), DMA((items,)), DMA((items,)),
            DMA((2,)), DMA((2,)), DMA((items,)), DMA((items,)),
        ],
        compiler_params=pltpu.CompilerParams(collective_id=1, has_side_effects=True, vmem_limit_bytes=32 * 2 ** 20),
        name="output",
    )(*keep_in(VMEM, att, keep, pay, got), *keep_in(pltpu.HBM, x_blk, w_out, w_down.reshape(CHUNKS, 4, 256, width)))


def solution(mesh):
    cache_spec = P(("dp", "ty", "tx"), None, None)
    across = [(0, 2), (1, 3), (2, 0), (3, 1)]

    def layer_shard(x_blk, lens, k_blk, v_blk, gamma, w_query, w_key, w_value, w_gate, w_up, w_out, w_down):
        freqs = np.tile(np.float32(ROPE_BASE ** (-np.arange(0, 128, 2) / 128.0)), 2)[None, :]
        q, kv, keep, pay, pre = project(lens, x_blk, gamma[None, :], freqs, w_query, w_key, w_value, w_gate, w_up, k_blk, v_blk)
        got = lax.ppermute(pay, "tx", across)
        k_out, v_out, att = attend(lens, q, kv, pre, k_blk, v_blk)
        y = output(att, keep, pay, got, x_blk, w_out, w_down)
        return y, k_out, v_out

    in_specs = (P("dp", "tx"), P("dp"), cache_spec, cache_spec, P("tx"), P("tx", "ty"), P("tx", None), P("tx", None), P("tx", "ty"), P("tx", "ty"), P("ty", "tx"), P("ty", "tx"))
    out_specs = (P("dp", "tx"), cache_spec, cache_spec)
    return jax.shard_map(layer_shard, mesh=mesh, in_specs=in_specs, out_specs=out_specs, check_vma=False)
```
